64 devices in a mesh: dp: 4 (over x, y), cp: 16 (over z, core).
Axes of the slice: x: 2, y: 2, z: 8, core: 2. Of those that a mesh axis runs over, the one named last changes fastest.
The devices are a block of a 4x4x8 slice.
Arguments:
- x_in: bfloat16 [12288, 8192], P(('dp', 'cp')), parts along dimension 0
- dy_in: bfloat16 [12288, 8192], P(('dp', 'cp')), parts along dimension 0
- doc_id: int32 [12288], P(('dp', 'cp')), parts along dimension 0
- w_q: bfloat16 [8192, 16, 128], replicated
- w_k: bfloat16 [8192, 2, 128], replicated
- w_v: bfloat16 [8192, 2, 128], replicated
- w_o: bfloat16 [16, 128, 8192], replicated
Outputs:
- output 1: bfloat16 [12288, 8192], P(('dp', 'cp')), parts along dimension 0
- output 2: bfloat16 [12288, 8192], P(('dp', 'cp')), parts along dimension 0
There are 4 independent parts. The reference program is written for one: setup_inputs(seed, part) draws one part's arguments, and reference() takes and returns one part's arrays. A program takes and returns all parts, laid end to end along the dimension named above; an argument that names none is the same for every part.
All inputs are finite; a program needn't handle non-finite values.
Results may differ from the reference program's by a relative error of at most 0.00987741.
Values are sent between devices in bfloat16 or wider.
A program may use at most 768 MiB of HBM per device.

```python
import jax
import jax.numpy as jnp
from jax import lax

D_MODEL = 8192
Q_HEADS = 16
KV_HEADS = 2
HEAD_DIM = 128
TOK_DEV = 192
GROUP_DEVS = 16
SEQ_LEN = GROUP_DEVS * TOK_DEV
PIECE_LEN = TOK_DEV // 2
QUERY_GROUP = Q_HEADS // KV_HEADS
DOC_CUTS = max(1, GROUP_DEVS // 2)
NEG_BIG = -1.0e30


def stored_positions():
    row_idx = jnp.arange(SEQ_LEN, dtype=jnp.int32)
    owner_dev = row_idx // TOK_DEV
    offset = row_idx % TOK_DEV
    piece_idx = jnp.where(offset < PIECE_LEN, owner_dev, 2 * GROUP_DEVS - 1 - owner_dev)
    return piece_idx * PIECE_LEN + offset % PIECE_LEN


def setup_inputs(seed: int = 0, part: int = 0) -> dict:
    part_key = jax.random.fold_in(jax.random.key(seed), part)
    key_x, key_dy, key_doc = jax.random.split(part_key, 3)
    key_q, key_k, key_v, key_o = jax.random.split(jax.random.key(seed + 1), 4)
    in_scale = D_MODEL ** -0.5
    out_scale = (Q_HEADS * HEAD_DIM) ** -0.5
    x_in = jax.random.normal(key_x, (SEQ_LEN, D_MODEL), jnp.float32).astype(jnp.bfloat16)
    dy_in = jax.random.normal(key_dy, (SEQ_LEN, D_MODEL), jnp.float32).astype(jnp.bfloat16)
    cut_pos = jax.random.randint(key_doc, (DOC_CUTS,), 1, SEQ_LEN, dtype=jnp.int32)
    doc_id = jnp.sum((stored_positions()[:, None] >= cut_pos[None, :]).astype(jnp.int32), axis=1)
    w_q = (jax.random.normal(key_q, (D_MODEL, Q_HEADS, HEAD_DIM), jnp.float32) * in_scale).astype(jnp.bfloat16)
    w_k = (jax.random.normal(key_k, (D_MODEL, KV_HEADS, HEAD_DIM), jnp.float32) * in_scale).astype(jnp.bfloat16)
    w_v = (jax.random.normal(key_v, (D_MODEL, KV_HEADS, HEAD_DIM), jnp.float32) * in_scale).astype(jnp.bfloat16)
    w_o = (jax.random.normal(key_o, (Q_HEADS, HEAD_DIM, D_MODEL), jnp.float32) * out_scale).astype(jnp.bfloat16)
    return {'x_in': x_in, 'dy_in': dy_in, 'doc_id': doc_id, 'w_q': w_q, 'w_k': w_k, 'w_v': w_v, 'w_o': w_o}


def reference(x_in, dy_in, doc_id, w_q, w_k, w_v, w_o):
    score_scale = HEAD_DIM ** -0.5
    all_pos = stored_positions()
    wq_flat = w_q.reshape(D_MODEL, Q_HEADS * HEAD_DIM)
    wk_flat = w_k.reshape(D_MODEL, KV_HEADS * HEAD_DIM)
    wv_flat = w_v.reshape(D_MODEL, KV_HEADS * HEAD_DIM)
    wo_flat = w_o.reshape(Q_HEADS * HEAD_DIM, D_MODEL)
    q_all = jnp.dot(x_in, wq_flat, preferred_element_type=jnp.float32).astype(jnp.bfloat16)
    q_all = q_all.reshape(SEQ_LEN, KV_HEADS, QUERY_GROUP, HEAD_DIM)
    k_all = jnp.dot(x_in, wk_flat, preferred_element_type=jnp.float32).astype(jnp.bfloat16)
    v_all = jnp.dot(x_in, wv_flat, preferred_element_type=jnp.float32).astype(jnp.bfloat16)
    k_wide = k_all.reshape(SEQ_LEN, KV_HEADS, HEAD_DIM).astype(jnp.float32)
    v_wide = v_all.reshape(SEQ_LEN, KV_HEADS, HEAD_DIM).astype(jnp.float32)
    do_all = jnp.dot(dy_in, wo_flat.T, preferred_element_type=jnp.float32).astype(jnp.bfloat16)
    do_all = do_all.reshape(SEQ_LEN, KV_HEADS, QUERY_GROUP, HEAD_DIM)

    def block_step(grad_acc, block_idx):
        dk_acc, dv_acc = grad_acc
        row_start = block_idx * TOK_DEV
        q_blk = lax.dynamic_slice_in_dim(q_all, row_start, TOK_DEV, 0).astype(jnp.float32)
        do_blk = lax.dynamic_slice_in_dim(do_all, row_start, TOK_DEV, 0).astype(jnp.float32)
        pos_blk = lax.dynamic_slice_in_dim(all_pos, row_start, TOK_DEV, 0)
        doc_blk = lax.dynamic_slice_in_dim(doc_id, row_start, TOK_DEV, 0)
        visible = (all_pos[None, :] <= pos_blk[:, None]) & (doc_id[None, :] == doc_blk[:, None])
        scores = jnp.einsum('tkge,ske->tkgs', q_blk, k_wide) * score_scale
        scores = jnp.where(visible[:, None, None, :], scores, NEG_BIG)
        log_norm = jax.nn.logsumexp(scores, axis=-1, keepdims=True)
        prob_blk = jnp.exp(scores - log_norm).astype(jnp.bfloat16).astype(jnp.float32)
        out_blk = jnp.einsum('tkgs,ske->tkge', prob_blk, v_wide).astype(jnp.bfloat16).astype(jnp.float32)
        delta_row = jnp.sum(do_blk * out_blk, axis=-1, keepdims=True)
        d_prob = jnp.einsum('tkge,ske->tkgs', do_blk, v_wide)
        d_score = (prob_blk * (d_prob - delta_row)).astype(jnp.bfloat16).astype(jnp.float32)
        dq_blk = (jnp.einsum('tkgs,ske->tkge', d_score, k_wide) * score_scale).astype(jnp.bfloat16)
        dk_acc = dk_acc + jnp.einsum('tkgs,tkge->ske', d_score, q_blk) * score_scale
        dv_acc = dv_acc + jnp.einsum('tkgs,tkge->ske', prob_blk, do_blk)
        return (dk_acc, dv_acc), (out_blk.astype(jnp.bfloat16), dq_blk)

    zero_grad = jnp.zeros((SEQ_LEN, KV_HEADS, HEAD_DIM), jnp.float32)
    grad_sums, block_outs = lax.scan(block_step, (zero_grad, zero_grad), jnp.arange(GROUP_DEVS))
    dk_sum, dv_sum = grad_sums
    out_blocks, dq_blocks = block_outs
    out_all = out_blocks.reshape(SEQ_LEN, Q_HEADS * HEAD_DIM)
    dq_all = dq_blocks.reshape(SEQ_LEN, Q_HEADS * HEAD_DIM)
    y_out = jnp.dot(out_all, wo_flat, preferred_element_type=jnp.float32).astype(jnp.bfloat16)
    dk_bf = dk_sum.astype(jnp.bfloat16).reshape(SEQ_LEN, KV_HEADS * HEAD_DIM)
    dv_bf = dv_sum.astype(jnp.bfloat16).reshape(SEQ_LEN, KV_HEADS * HEAD_DIM)
    dx_wide = (jnp.dot(dq_all, wq_flat.T, preferred_element_type=jnp.float32)
               + jnp.dot(dk_bf, wk_flat.T, preferred_element_type=jnp.float32)
               + jnp.dot(dv_bf, wv_flat.T, preferred_element_type=jnp.float32))
    dx_out = dx_wide.astype(jnp.bfloat16)
    return y_out, dx_out
```

```python
import functools

import jax
import jax.numpy as jnp
from jax import lax
from jax.experimental import pallas as pl
from jax.experimental.pallas import tpu as pltpu
from jax.sharding import PartitionSpec as P

MESH = pl.DeviceIdType.MESH
NEG_BIG = -1.0e30
LOG2E = 1.4426950408889634
F32, BF16 = jnp.float32, jnp.bfloat16
NT = (((1,), (1,)), ((), ()))
NN = (((1,), (0,)), ((), ()))
DOC_VALUES = 9


def dot(a, b, dims=NN):
    return lax.dot_general(a, b, dims, preferred_element_type=F32)


def remote(src, dst, send, recv, dev):
    return pltpu.make_async_remote_copy(src_ref=src, dst_ref=dst, send_sem=send, recv_sem=recv,
                                        device_id={'cp': dev}, device_id_type=MESH)


def ring_ids(chips):
    me = lax.axis_index('cp')
    core, chip = lax.rem(me, 2), me // 2
    return core, chip, chip * 2 + 1 - core, lax.rem(chip + 1, chips) * 2 + core, lax.rem(chip + chips - 1, chips) * 2 + core


def entry_barrier(devs):
    barrier = pltpu.get_barrier_semaphore()
    for dev in devs:
        pl.semaphore_signal(barrier, inc=1, device_id={'cp': dev}, device_id_type=MESH)
    pl.semaphore_wait(barrier, len(devs))


def proj_kernel(chips, x, dy, meta, wq, wk, wv, wo, q_o, do_o, kv_o, md_o,
                xb, dyb, mb, kvb, wkb, wvb, wqb, wob, scr, wr, wkv, acc, kvacc,
                loc, wksem, wqsem, wosem, xs, xr, ys, yr, ms, mr, gs, gr, osem):
    half = x.shape[0] // 2
    d_model = x.shape[1]
    tok = 2 * half
    pieces = 2 * chips
    n_ch = xs.shape[1]
    cw = d_model // n_ch
    core, chip, partner, up, down = ring_ids(chips)
    row_off = (pl.multiple_of(half * core, half), pl.multiple_of(3 * half - half * core, half))
    n_q, qd = d_model // wqb.shape[1], wqb.shape[1]
    group = wqb.shape[2]
    head = wqb.shape[3]
    n_o = group * head // wob.shape[1]

    def wq_copy(i, slot):
        return pltpu.make_async_copy(wq.at[pl.ds(i * qd, qd), core], wqb.at[slot], wqsem.at[slot])

    def wo_copy(i, slot):
        rows = wob.shape[1]
        return pltpu.make_async_copy(wo.at[pl.ds(core * group * head + i * rows, rows)], wob.at[slot], wosem.at[slot])

    wk_copies = []
    for ch in range(n_ch):
        rows = pl.ds(ch * 2 * cw, 2 * cw)
        wk_copies.append((pltpu.make_async_copy(wk.at[rows], wkb.at[rows], wksem.at[0, ch]),
                          pltpu.make_async_copy(wv.at[rows], wvb.at[rows], wksem.at[1, ch])))
    x_loc, y_loc, x_rem, y_rem = [], [], [], []
    for ch in range(n_ch):
        cols = pl.ds(ch * cw, cw)
        for pc in range(2):
            src = pl.ds(half * pc, half)
            dst = pl.ds(row_off[pc], half)
            x_loc.append(pltpu.make_async_copy(x.at[src, cols], xb.at[dst, cols], loc.at[0, pc, ch]))
            y_loc.append(pltpu.make_async_copy(dy.at[src, cols], dyb.at[dst, cols], loc.at[1, pc, ch]))
            x_rem.append(remote(x.at[src, cols], xb.at[dst, cols], xs.at[pc, ch], xr.at[pc, ch], partner))
            y_rem.append(remote(dy.at[src, cols], dyb.at[dst, cols], ys.at[pc, ch], yr.at[pc, ch], partner))
    m_loc = pltpu.make_async_copy(meta, mb.at[0], osem.at[0])
    m_rem = remote(meta, mb.at[1], ms, mr, partner)

    for ch in range(n_ch):
        x_loc[2 * ch].start()
        x_loc[2 * ch + 1].start()
        wk_copies[ch][0].start()
        wk_copies[ch][1].start()
    m_loc.start()
    for s in range(wqb.shape[0]):
        wq_copy(s, s).start()
    entry_barrier((partner, up, down))
    for c in x_rem:
        c.start()
    m_rem.start()
    for c in y_rem:
        c.start()
    for c in y_loc:
        c.start()
    for s in range(wob.shape[0]):
        wo_copy(s, s).start()

    for ch in range(n_ch):
        for c in (x_loc[2 * ch], x_loc[2 * ch + 1]):
            c.wait()
        for c in wk_copies[ch]:
            c.wait()
        for part, buf in ((0, wkb), (1, wvb)):
            base = part * 2 * cw
            scr[base:base + 2 * cw, :] = buf[ch * 2 * cw:(ch + 1) * 2 * cw, :].astype(F32)
            wkv[:, part * head:(part + 1) * head] = scr[pl.ds(base + core, cw, stride=2), :].astype(BF16)
        for c in (x_rem[2 * ch], x_rem[2 * ch + 1]):
            c.wait_recv()
        part_sum = dot(xb[:, ch * cw:(ch + 1) * cw], wkv[...])
        if ch == 0:
            kvacc[...] = part_sum
        else:
            kvacc[...] += part_sum
    m_loc.wait()
    m_rem.wait_recv()
    lo, hi = chip, pieces - 1 - chip
    width = md_o.shape[2]
    for pc, idx in ((0, lo), (1, hi)):
        both = (mb[0, pc].astype(F32) + mb[1, pc].astype(F32)).astype(BF16)
        md_o[pc] = both[:, :width]
        kvb[idx, 2 * tok:2 * tok + 16] = both[:, width:]
        kvb[idx, 0:tok] = kvacc[pc * tok:(pc + 1) * tok, 0:head].astype(BF16)
        kvb[idx, tok:2 * tok] = kvacc[pc * tok:(pc + 1) * tok, head:].astype(BF16)

    last = chips // 2 - 1

    def hop(direction, t, pc):
        src = lax.rem(chip + (chips - t if direction == 0 else t), chips)
        idx = src if pc == 0 else pieces - 1 - src
        return remote(kvb.at[idx], kvb.at[idx], gs.at[direction, t, pc], gr.at[direction, t, pc], up if direction == 0 else down)

    def arrived(direction, t, pc):
        src = lax.rem(chip + (chips - t - 1 if direction == 0 else t + 1), chips)
        idx = src if pc == 0 else pieces - 1 - src
        remote(kvb.at[idx], kvb.at[idx], gs.at[direction, t, pc], gr.at[direction, t, pc], up).wait_recv()

    moves = [[(d, pc) for pc in range(2) for d in range(2) if t < last or d == pc] for t in range(last + 1)]

    def advance(t):
        for d, pc in moves[t - 1]:
            arrived(d, t - 1, pc)
            if t <= last and (d, pc) in moves[t]:
                hop(d, t, pc).start()

    for d, pc in moves[0]:
        hop(d, 0, pc).start()

    acc[...] = jnp.zeros_like(acc)
    sub = 128
    n_slot = wqb.shape[0]

    @pl.loop(0, n_q)
    def _(i):
        slot = lax.rem(i, n_slot)
        wq_copy(i, slot).wait()

        @pl.loop(0, qd // sub)
        def _(j):
            rows = pl.ds(pl.multiple_of(j * sub, sub), sub)
            scr[0:sub * group, :] = wqb[slot, rows].astype(F32).reshape(sub * group, head)
            for g in range(group):
                wr[rows, g * head:(g + 1) * head] = scr[pl.ds(g, sub, stride=group), :].astype(BF16)

        @pl.when(i + n_slot < n_q)
        def _():
            wq_copy(i + n_slot, slot).start()

        acc[...] += dot(xb[:, pl.ds(pl.multiple_of(i * qd, qd), qd)], wr[...])

        @pl.when(i == 4)
        def _():
            advance(1)

    for g in range(group):
        for pc in range(2):
            q_o[pc, g * tok:(g + 1) * tok, :] = acc[pc * tok:(pc + 1) * tok, g * head:(g + 1) * head].astype(BF16)
    advance(2)

    for c in y_loc:
        c.wait()
    for c in y_rem:
        c.wait_recv()

    wide = wob.shape[1] // head
    for i in range(n_o):
        slot = i % wob.shape[0]
        wo_copy(i, slot).wait()
        part = dot(dyb[...], wob[slot], NT).astype(BF16)
        for g in range(wide):
            for pc in range(2):
                do_o[pc, (i * wide + g) * tok:(i * wide + g + 1) * tok, :] = part[pc * tok:(pc + 1) * tok, g * head:(g + 1) * head]
        if i + wob.shape[0] < n_o:
            wo_copy(i + wob.shape[0], slot).start()
        if i == 1:
            advance(3)
    for t in range(4, last + 2):
        advance(t)
    out = pltpu.make_async_copy(kvb, kv_o, osem.at[0])
    out.start()
    for c in x_rem + y_rem + [m_rem]:
        c.wait_send()
    for t in range(last + 1):
        for d, pc in moves[t]:
            hop(d, t, pc).wait_send()
    out.wait()


def attn_kernel(chips, scale, q, do, kv, md, q_off, o_ref, dq_ref, dkv, s_scr, p_scr, ds_scr, acc_t, k_t, v_t, row_scr, m_ref, l_ref):
    pieces = 2 * chips
    tok = kv.shape[1] // 2 - 8
    head = kv.shape[2]
    lanes_all = q.shape[1]
    group = lanes_all // tok
    lw = 256
    n_lc = lanes_all // lw
    chip = lax.axis_index('cp') // 2
    dkv[...] = jnp.zeros_like(dkv)

    def prep(j, tot):
        v_t[j] = kv[j, tok:2 * tok].astype(F32).T.astype(BF16)
        k_t[j] = kv[j, 0:tok].astype(F32).T.astype(BF16)
        return tot + kv[j, 2 * tok:2 * tok + 16].astype(F32)

    tot = lax.fori_loop(0, pieces, prep, jnp.zeros((16, head), F32))[0:1]

    for pc in range(2):
        place = chip if pc == 0 else pieces - 1 - chip
        doc_q = md[pc].astype(F32)[0:1]
        start = jnp.zeros((1, lanes_all), F32)
        for v in range(1, DOC_VALUES):
            start = jnp.where(doc_q == float(v), tot[:, v:v + 1], start)
        first = jnp.min(start).astype(jnp.int32) // tok
        pos = q_off[...] + (place * tok).astype(F32)
        m_ref[...] = jnp.full_like(m_ref, NEG_BIG)
        l_ref[...] = jnp.zeros_like(l_ref)

        @pl.loop(first, place + 1)
        def _(kb):
            keys = kv[kb, 0:tok]
            u = (lax.broadcasted_iota(jnp.int32, (tok, lw), 0) + kb * tok).astype(F32)
            for lc in range(n_lc):
                ln = slice(lc * lw, (lc + 1) * lw)
                s = dot(keys, q[pc, ln], NT) * (scale * LOG2E)
                s = jnp.where((u >= start[:, ln]) & (u <= pos[:, ln]), s, NEG_BIG)
                s_scr[kb, :, ln] = s
                m_old = m_ref[:, ln]
                m_new = jnp.maximum(m_old, jnp.max(s, axis=0, keepdims=True))
                l_ref[:, ln] = l_ref[:, ln] * jnp.exp2(m_old - m_new) + jnp.sum(jnp.exp2(s - m_new), axis=0, keepdims=True)
                m_ref[:, ln] = m_new

        log_norm = m_ref[...] + jnp.log2(l_ref[...])
        acc_t[...] = jnp.zeros_like(acc_t)

        @pl.loop(first, place + 1)
        def _(kb):
            for lc in range(n_lc):
                ln = slice(lc * lw, (lc + 1) * lw)
                p = jnp.exp2(s_scr[kb, :, ln] - log_norm[:, ln]).astype(BF16)
                p_scr[kb, :, ln] = p
                acc_t[:, ln] += dot(v_t[kb], p)

        for lc in range(n_lc):
            ln = slice(lc * lw, (lc + 1) * lw)
            o_bf = acc_t[:, ln].astype(BF16).astype(F32)
            do_t = do[pc, ln].astype(F32).T
            l_ref[:, ln] = jnp.sum(do_t * o_bf, axis=0, keepdims=True)
            row_scr[ln, :] = o_bf.T.astype(BF16)
        for g in range(group):
            o_ref[pc * tok:(pc + 1) * tok, g * head:(g + 1) * head] = row_scr[g * tok:(g + 1) * tok, :]
        acc_t[...] = jnp.zeros_like(acc_t)

        @pl.loop(first, place + 1)
        def _(kb):
            vals = kv[kb, tok:2 * tok]
            for lc in range(n_lc):
                ln = slice(lc * lw, (lc + 1) * lw)
                dp = dot(vals, do[pc, ln], NT)
                ds = (p_scr[kb, :, ln].astype(F32) * (dp - l_ref[:, ln])).astype(BF16)
                ds_scr[:, ln] = ds
                acc_t[:, ln] += dot(k_t[kb], ds)
            dkv[kb, tok:2 * tok] += dot(p_scr[kb], do[pc])
            dkv[kb, 0:tok] += dot(ds_scr[...], q[pc]) * scale

        for lc in range(n_lc):
            ln = slice(lc * lw, (lc + 1) * lw)
            row_scr[ln, :] = (acc_t[:, ln] * scale).T.astype(BF16)
        for g in range(group):
            dq_ref[pc * tok:(pc + 1) * tok, g * head:(g + 1) * head] = row_scr[g * tok:(g + 1) * tok, :]


def out_kernel(chips, o, dq, dkv, wo, wq, wk, wv, y, dx,
               ob, dqb, own, ring, fin, a2, b2, wob, wqb, wkb, scr, wr, dacc, yb, xo,
               loc, ex_s, ex_r, rs, rr, fs, fr, wosem, wqsem, wksem, ysem, xsem, ys, yr, xs, xr):
    tok = own.shape[1] // 2
    head = own.shape[2]
    half = tok // 2
    pieces = 2 * chips
    d_half = yb.shape[1]
    core, chip, partner, up, down = ring_ids(chips)
    mine = (pl.multiple_of(half * core, half), pl.multiple_of(3 * half - half * core, half))
    theirs = (pl.multiple_of(half - half * core, half), pl.multiple_of(2 * half + half * core, half))
    hw = o.shape[1]
    col0 = pl.multiple_of(core * d_half, d_half)
    bw = wob.shape[2]
    n_y = d_half // bw
    qd = wqb.shape[1] * head // wr.shape[1]
    n_x = d_half // qd
    n_head = wr.shape[1] // head
    kc = scr.shape[0] // 2

    def wo_copy(i, slot):
        return pltpu.make_async_copy(wo.at[:, pl.ds(pl.multiple_of(col0 + i * bw, bw), bw)], wob.at[slot], wosem.at[slot])

    def wq_copy(i, slot):
        rows = wqb.shape[1]
        return pltpu.make_async_copy(wq.at[pl.ds(pl.multiple_of(col0 * n_head + i * rows, rows), rows)], wqb.at[slot], wqsem.at[slot])

    rows = pl.ds(pl.multiple_of(col0 * 2, 2 * d_half), 2 * d_half)
    wk_copies = [pltpu.make_async_copy(w.at[rows], wkb.at[k], wksem.at[k]) for k, w in enumerate((wk, wv))]
    ocols = pl.ds(pl.multiple_of(core * hw, hw), hw)
    l_own = pltpu.make_async_copy(dkv, own, loc.at[0])
    l_o = pltpu.make_async_copy(o, ob.at[:, ocols], loc.at[1])
    l_dq = pltpu.make_async_copy(dq, dqb.at[:, ocols], loc.at[2])
    r_o = remote(o, ob.at[:, ocols], ex_s.at[0], ex_r.at[0], partner)
    r_dq = remote(dq, dqb.at[:, ocols], ex_s.at[1], ex_r.at[1], partner)

    l_own.start()
    l_o.start()
    l_dq.start()
    for s in range(wob.shape[0]):
        wo_copy(s, s).start()
    entry_barrier((partner, up, down))
    r_o.start()
    r_dq.start()
    for s in range(wqb.shape[0]):
        wq_copy(s, s).start()
    for c in wk_copies:
        c.start()

    steps = chips - 1

    def owner(direction, s):
        chip_w = lax.rem(chip + (2 * chips - 1 - s if direction == 0 else 1 + s), chips)
        return chip_w if direction == 0 else pieces - 1 - chip_w

    def part_rows(kvp):
        return pl.ds(kvp * tok, tok)

    def send(direction, s, kvp):
        src = own.at[owner(direction, 0), part_rows(kvp)] if s == 0 else ring.at[direction, s - 1, kvp]
        return remote(src, ring.at[direction, s, kvp], rs.at[direction, s, kvp], rr.at[direction, s, kvp], up if direction == 0 else down)

    def advance(s):
        for kvp in range(2):
            for d in range(2):
                remote(ring.at[d, s - 1, kvp], ring.at[d, s - 1, kvp], rs.at[d, s - 1, kvp], rr.at[d, s - 1, kvp], up).wait_recv()
                if s <= steps - 1:
                    ring[d, s - 1, kvp] = ring[d, s - 1, kvp] + own[owner(d, s), part_rows(kvp)]
                    send(d, s, kvp).start()
                else:
                    total = ring[d, s - 1, kvp] + own[owner(d, s), part_rows(kvp)]
                    fin[d * tok:(d + 1) * tok, kvp * head:(kvp + 1) * head] = total.astype(BF16)

    l_own.wait()
    for kvp in range(2):
        for d in range(2):
            send(d, 0, kvp).start()

    def out_copies(buf, dst, i, width, lsem, ssem, rsem):
        cols = pl.ds(pl.multiple_of(col0 + i * width, width), width)
        bc = pl.ds(pl.multiple_of(i * width, width), width)
        for pc in range(2):
            pltpu.make_async_copy(buf.at[pl.ds(mine[pc], half), bc], dst.at[pl.ds(half * pc, half), cols], lsem).start()
            remote(buf.at[pl.ds(theirs[pc], half), bc], dst.at[pl.ds(half * pc, half), cols], ssem, rsem, partner).start()

    l_o.wait()
    r_o.wait_recv()
    ns = wob.shape[0]

    @pl.loop(0, n_y)
    def _(i):
        slot = lax.rem(i, ns)
        wo_copy(i, slot).wait()
        yb[:, pl.ds(pl.multiple_of(i * bw, bw), bw)] = dot(ob[...], wob[slot]).astype(BF16)

        @pl.when(i + ns < n_y)
        def _():
            wo_copy(i + ns, slot).start()

        @pl.when(i > 0)
        def _():
            out_copies(yb, y, i - 1, bw, ysem, ys, yr)

        @pl.when(i == 4)
        def _():
            advance(1)

    out_copies(yb, y, n_y - 1, bw, ysem, ys, yr)
    advance(2)

    l_dq.wait()
    r_dq.wait_recv()
    nq = wqb.shape[0]
    sub = 64

    @pl.loop(0, n_x)
    def _(i):
        slot = lax.rem(i, nq)
        wq_copy(i, slot).wait()

        @pl.loop(0, qd // sub)
        def _(j):
            src = pl.ds(pl.multiple_of(j * sub * n_head, sub * n_head), sub * n_head)
            dst = pl.ds(pl.multiple_of(j * sub, sub), sub)
            scr[0:sub * n_head, :] = wqb[slot, src].astype(F32)
            for g in range(n_head):
                wr[dst, g * head:(g + 1) * head] = scr[pl.ds(g, sub, stride=n_head), :].astype(BF16)

        @pl.when(i + nq < n_x)
        def _():
            wq_copy(i + nq, slot).start()

        dacc[:, pl.ds(pl.multiple_of(i * qd, qd), qd)] = dot(dqb[...], wr[...], NT)

        @pl.when(i == 3)
        def _():
            advance(3)

    advance(4)
    for c in wk_copies:
        c.wait()
    for k in range(2):
        for j in range(d_half // kc):
            scr[...] = wkb[k, j * 2 * kc:(j + 1) * 2 * kc].astype(F32)
            for h in range(2):
                b2[j * kc:(j + 1) * kc, (2 * k + h) * head:(2 * k + h + 1) * head] = scr[pl.ds(h, kc, stride=2), :].astype(BF16)
    for s in range(5, steps + 1):
        advance(s)

    r_fin = remote(fin, a2.at[core], fs, fr, partner)
    r_fin.start()
    a2[core] = fin[...]
    r_fin.wait_recv()
    a_all = jnp.concatenate([a2[0][:, :head], a2[1][:, :head], a2[0][:, head:], a2[1][:, head:]], axis=1)
    for i in range(n_y):
        cs = slice(i * bw, (i + 1) * bw)
        xo[:, cs] = (dacc[:, cs] + dot(a_all, b2[cs, :], NT)).astype(BF16)
        if i > 0:
            out_copies(xo, dx, i - 1, bw, xsem, xs, xr)
    out_copies(xo, dx, n_y - 1, bw, xsem, xs, xr)

    for c in (r_o, r_dq, r_fin):
        c.wait_send()
    for s in range(steps):
        for kvp in range(2):
            for d in range(2):
                send(d, s, kvp).wait_send()
    for buf, dst, lsem, ssem, rsem in ((yb, y, ysem, ys, yr), (xo, dx, xsem, xs, xr)):
        cols = pl.ds(col0, d_half)
        pltpu.make_async_copy(buf.at[pl.ds(0, tok)], dst.at[:, cols], lsem).wait()
        both = remote(buf.at[pl.ds(0, tok)], dst.at[:, cols], ssem, rsem, partner)
        both.wait_send()
        both.wait_recv()


def solution(mesh):
    group_devs = mesh.shape['cp']
    chips = group_devs // 2
    row_spec = P(('dp', 'cp'))
    full_spec = P()
    any_spec = pl.BlockSpec(memory_space=pl.ANY)
    vmem_spec = pl.BlockSpec(memory_space=pltpu.VMEM)
    dma = pltpu.SemaphoreType.DMA

    def local_layer(x_in, dy_in, doc_id, w_q, w_k, w_v, w_o):
        tok, d_model = x_in.shape
        q_heads, head = w_q.shape[1], w_q.shape[2]
        kv_heads = w_k.shape[1]
        group = q_heads // kv_heads
        half = tok // 2
        rows2 = 2 * tok
        pieces = 2 * chips
        lanes = group * tok
        d_half = d_model // 2
        scale = head ** -0.5
        core = lax.axis_index('cp') % 2
        docs = doc_id.reshape(2, half)
        slot = jnp.stack([core, 1 - core])[:, None]
        lane = jnp.arange(tok)
        docf = jnp.concatenate([docs, docs], axis=1).astype(F32)
        docf = jnp.where((lane // half)[None, :] == slot, docf, 0.0)
        ids = jnp.tile(docf, (1, group))
        counts = jnp.sum((docs[:, :, None] < jnp.arange(head)[None, None, :]).astype(F32), axis=1)
        meta = jnp.concatenate([ids, counts], axis=1).astype(BF16)
        meta = jnp.broadcast_to(meta[:, None, :], (2, 16, lanes + head))
        q_off = jnp.tile(lane.astype(F32), (group,))[None, :]

        wq4 = w_q.reshape(d_model, kv_heads, group, head)
        wq2 = w_q.reshape(d_model * q_heads, head)
        wk2 = w_k.reshape(d_model * kv_heads, head)
        wv2 = w_v.reshape(d_model * kv_heads, head)
        wo2 = w_o.reshape(q_heads * head, d_model)

        n_ch = 4
        cw = d_model // n_ch
        qd = d_model // 8
        hops = chips // 2
        kv_rows = 2 * tok + 16
        q, do, kv, md = pl.pallas_call(
            functools.partial(proj_kernel, chips),
            name='proj',
            out_shape=(jax.ShapeDtypeStruct((2, lanes, head), BF16), jax.ShapeDtypeStruct((2, lanes, head), BF16),
                       jax.ShapeDtypeStruct((pieces, kv_rows, head), BF16), jax.ShapeDtypeStruct((2, 16, lanes), BF16)),
            in_specs=[any_spec] * 7,
            out_specs=(vmem_spec, vmem_spec, any_spec, vmem_spec),
            scratch_shapes=[
                pltpu.VMEM((rows2, d_model), BF16), pltpu.VMEM((rows2, d_model), BF16), pltpu.VMEM((2, 2, 16, lanes + head), BF16),
                pltpu.VMEM((pieces, kv_rows, head), BF16),
                pltpu.VMEM((2 * d_model, head), BF16), pltpu.VMEM((2 * d_model, head), BF16),
                pltpu.VMEM((3, qd, group, head), BF16), pltpu.VMEM((2, 2 * head, d_model), BF16),
                pltpu.VMEM((4 * cw, head), F32), pltpu.VMEM((qd, group * head), BF16), pltpu.VMEM((cw, 2 * head), BF16),
                pltpu.VMEM((rows2, group * head), F32), pltpu.VMEM((rows2, 2 * head), F32),
                dma((2, 2, n_ch)), dma((2, n_ch)), dma((3,)), dma((2,)),
                dma((2, n_ch)), dma((2, n_ch)), dma((2, n_ch)), dma((2, n_ch)), dma, dma,
                dma((2, hops, 2)), dma((2, hops, 2)), dma((1,)),
            ],
            compiler_params=pltpu.CompilerParams(collective_id=0, has_side_effects=True, vmem_limit_bytes=60 << 20),
        )(x_in, dy_in, meta, wq4, wk2, wv2, wo2)

        o, dq, dkv = pl.pallas_call(
            functools.partial(attn_kernel, chips, scale),
            name='attn',
            out_shape=(jax.ShapeDtypeStruct((rows2, group * head), BF16), jax.ShapeDtypeStruct((rows2, group * head), BF16),
                       jax.ShapeDtypeStruct((pieces, 2 * tok, head), F32)),
            in_specs=[vmem_spec] * 5,
            out_specs=(vmem_spec,) * 3,
            scratch_shapes=[
                pltpu.VMEM((pieces, tok, lanes), F32), pltpu.VMEM((pieces, tok, lanes), BF16), pltpu.VMEM((tok, lanes), BF16),
                pltpu.VMEM((head, lanes), F32), pltpu.VMEM((pieces, head, tok), BF16), pltpu.VMEM((pieces, head, tok), BF16),
                pltpu.VMEM((lanes, head), BF16), pltpu.VMEM((1, lanes), F32), pltpu.VMEM((1, lanes), F32),
            ],
            compiler_params=pltpu.CompilerParams(vmem_limit_bytes=60 << 20),
        )(q, do, kv, md, q_off)

        steps = chips - 1
        bw = d_half // 8
        y, dx = pl.pallas_call(
            functools.partial(out_kernel, chips),
            name='out',
            out_shape=(jax.ShapeDtypeStruct((tok, d_model), BF16), jax.ShapeDtypeStruct((tok, d_model), BF16)),
            in_specs=[any_spec] * 7,
            out_specs=(any_spec, any_spec),
            scratch_shapes=[
                pltpu.VMEM((rows2, q_heads * head), BF16), pltpu.VMEM((rows2, q_heads * head), BF16),
                pltpu.VMEM((pieces, 2 * tok, head), F32), pltpu.VMEM((2, steps, 2, tok, head), F32),
                pltpu.VMEM((rows2, 2 * head), BF16), pltpu.VMEM((2, rows2, 2 * head), BF16), pltpu.VMEM((d_half, 4 * head), BF16),
                pltpu.VMEM((3, q_heads * head, bw), BF16), pltpu.VMEM((3, bw * q_heads, head), BF16),
                pltpu.VMEM((2, 2 * d_half, head), BF16),
                pltpu.VMEM((2 * d_half // 4, head), F32), pltpu.VMEM((bw, q_heads * head), BF16),
                pltpu.VMEM((rows2, d_half), F32), pltpu.VMEM((rows2, d_half), BF16), pltpu.VMEM((rows2, d_half), BF16),
                dma((3,)), dma((2,)), dma((2,)), dma((2, steps, 2)), dma((2, steps, 2)), dma, dma,
                dma((3,)), dma((3,)), dma((2,)), dma, dma, dma, dma, dma, dma,
            ],
            compiler_params=pltpu.CompilerParams(collective_id=1, has_side_effects=True, vmem_limit_bytes=62 << 20),
        )(o, dq, dkv, wo2, wq2, wk2, wv2)
        return y, dx

    return jax.shard_map(local_layer, mesh=mesh,
                         in_specs=(row_spec, row_spec, row_spec, full_spec, full_spec, full_spec, full_spec),
                         out_specs=(row_spec, row_spec), check_vma=False)
```

```python
import functools

import jax
import jax.numpy as jnp
from jax import lax
from jax.experimental import pallas as pl
from jax.experimental.pallas import tpu as pltpu
from jax.sharding import PartitionSpec as P

MESH = pl.DeviceIdType.MESH
NEG_BIG = -1.0e30
LOG2E = 1.4426950408889634
F32, BF16 = jnp.float32, jnp.bfloat16
NT = (((1,), (1,)), ((), ()))
NN = (((1,), (0,)), ((), ()))
DOC_VALUES = 9


def dot(a, b, dims=NN):
    return lax.dot_general(a, b, dims, preferred_element_type=F32)


def remote(src, dst, send, recv, dev):
    return pltpu.make_async_remote_copy(src_ref=src, dst_ref=dst, send_sem=send, recv_sem=recv,
                                        device_id={'cp': dev}, device_id_type=MESH)


def ring_ids(chips):
    me = lax.axis_index('cp')
    core, chip = lax.rem(me, 2), me // 2
    return core, chip, chip * 2 + 1 - core, lax.rem(chip + 1, chips) * 2 + core, lax.rem(chip + chips - 1, chips) * 2 + core


def entry_barrier(devs):
    barrier = pltpu.get_barrier_semaphore()
    for dev in devs:
        pl.semaphore_signal(barrier, inc=1, device_id={'cp': dev}, device_id_type=MESH)
    pl.semaphore_wait(barrier, len(devs))


TILE = 256
PER = 8


def sort_matrix():
    toks = TILE // PER
    r = lax.broadcasted_iota(jnp.int32, (TILE, TILE), 0)
    c = lax.broadcasted_iota(jnp.int32, (TILE, TILE), 1)
    t = r & (toks - 1)
    return jnp.where(c == t * PER + lax.shift_right_logical(r, toks.bit_length() - 1), 1.0, 0.0).astype(BF16)


def split_heads(order, src, dst, count, n_head, head):
    toks = TILE // PER
    for h0 in range(0, n_head, PER):
        for t0 in range(0, count, 4 * toks):
            side = [src[t0 + k * toks:t0 + (k + 1) * toks, h0:h0 + PER, :].reshape(TILE, head) for k in range(4)]
            rows = dot(order, jnp.concatenate(side, axis=1)).astype(BF16)
            for k in range(4):
                for g in range(PER):
                    dst[t0 + k * toks:t0 + (k + 1) * toks, (h0 + g) * head:(h0 + g + 1) * head] = rows[g * toks:(g + 1) * toks, k * head:(k + 1) * head]


def proj_kernel(chips, x, dy, meta, wq, wk, wv, wo, q_o, do_o, kv_o, md_o,
                xb, dyb, mb, kvb, wkb, wvb, wqb, wob, wr, order, pick, wkv, acc, kvacc,
                loc, wksem, wqsem, wosem, xs, xr, ys, yr, ms, mr, gs, gr, osem):
    half = x.shape[0] // 2
    d_model = x.shape[1]
    tok = 2 * half
    pieces = 2 * chips
    n_ch = xs.shape[1]
    cw = d_model // n_ch
    core, chip, partner, up, down = ring_ids(chips)
    row_off = (pl.multiple_of(half * core, half), pl.multiple_of(3 * half - half * core, half))
    n_q, qd = d_model // wqb.shape[1], wqb.shape[1]
    group = wqb.shape[2]
    head = wqb.shape[3]
    n_o = group * head // wob.shape[1]

    def wq_copy(i, slot):
        return pltpu.make_async_copy(wq.at[pl.ds(i * qd, qd), core], wqb.at[slot], wqsem.at[slot])

    def wo_copy(i, slot):
        rows, kw = wob.shape[1], wob.shape[2]
        n, k = i // (d_model // kw), i % (d_model // kw)
        return pltpu.make_async_copy(wo.at[pl.ds(core * group * head + n * rows, rows), pl.ds(k * kw, kw)], wob.at[slot], wosem.at[slot])

    wk_copies = []
    for ch in range(n_ch):
        rows = pl.ds(ch * 2 * cw, 2 * cw)
        wk_copies.append((pltpu.make_async_copy(wk.at[rows], wkb.at[rows], wksem.at[0, ch]),
                          pltpu.make_async_copy(wv.at[rows], wvb.at[rows], wksem.at[1, ch])))
    x_loc, y_loc, x_rem, y_rem = [], [], [], []
    for ch in range(n_ch):
        cols = pl.ds(ch * cw, cw)
        for pc in range(2):
            src = pl.ds(half * pc, half)
            dst = pl.ds(row_off[pc], half)
            x_loc.append(pltpu.make_async_copy(x.at[src, cols], xb.at[dst, cols], loc.at[0, pc, ch]))
            y_loc.append(pltpu.make_async_copy(dy.at[src, cols], dyb.at[dst, cols], loc.at[1, pc, ch]))
            x_rem.append(remote(x.at[src, cols], xb.at[dst, cols], xs.at[pc, ch], xr.at[pc, ch], partner))
            y_rem.append(remote(dy.at[src, cols], dyb.at[dst, cols], ys.at[pc, ch], yr.at[pc, ch], partner))
    m_loc = pltpu.make_async_copy(meta, mb.at[0], osem.at[0])
    m_rem = remote(meta, mb.at[1], ms, mr, partner)

    for ch in range(n_ch):
        x_loc[2 * ch].start()
        x_loc[2 * ch + 1].start()
        wk_copies[ch][0].start()
        wk_copies[ch][1].start()
    m_loc.start()
    for s in range(wqb.shape[0]):
        wq_copy(s, s).start()
    entry_barrier((partner, up, down))
    for c in x_rem:
        c.start()
    m_rem.start()
    for c in y_rem:
        c.start()
    for c in y_loc:
        c.start()
    for s in range(wob.shape[0]):
        wo_copy(s, s).start()

    r = lax.broadcasted_iota(jnp.int32, pick.shape, 0)
    pick[...] = jnp.where(lax.broadcasted_iota(jnp.int32, pick.shape, 1) == 2 * r + core, 1.0, 0.0).astype(BF16)
    order[...] = sort_matrix()
    n_sub = TILE // 2
    for ch in range(n_ch):
        for c in wk_copies[ch]:
            c.wait()
        for j in range(ch * cw // n_sub, (ch + 1) * cw // n_sub, 2):
            side = [buf[t * 2 * n_sub:(t + 1) * 2 * n_sub, :] for t in (j, j + 1) for buf in (wkb, wvb)]
            rows = dot(pick[...], jnp.concatenate(side, axis=1)).astype(BF16)
            wkv[j * n_sub:(j + 1) * n_sub, :] = rows[:, :2 * head]
            wkv[(j + 1) * n_sub:(j + 2) * n_sub, :] = rows[:, 2 * head:]
    quarters = 2
    qs = qd // quarters

    def split_part(slot, dst, k):
        split_heads(order[...], wqb.at[slot, k * qs:(k + 1) * qs], dst.at[k * qs:(k + 1) * qs], qs, group, head)

    wq_copy(0, 0).wait()
    for k in range(quarters):
        split_part(0, wr.at[0], k)
    wq_copy(wqb.shape[0], 0).start()
    for ch in range(n_ch):
        for c in (x_loc[2 * ch], x_loc[2 * ch + 1]):
            c.wait()
        for c in (x_rem[2 * ch], x_rem[2 * ch + 1]):
            c.wait_recv()
        hc = cw // 2
        for k in range(2):
            part_sum = dot(xb[:, ch * cw + k * hc:ch * cw + (k + 1) * hc], wkv[ch * cw + k * hc:ch * cw + (k + 1) * hc])
            if ch == 0:
                kvacc[k] = part_sum
            else:
                kvacc[k] += part_sum
    m_loc.wait()
    m_rem.wait_recv()
    lo, hi = chip, pieces - 1 - chip
    width = md_o.shape[2]
    for pc, idx in ((0, lo), (1, hi)):
        both = (mb[0, pc].astype(F32) + mb[1, pc].astype(F32)).astype(BF16)
        md_o[pc] = both[:, :width]
        kvb[idx, 2 * tok:2 * tok + 16] = both[:, width:]
        kv_sum = (kvacc[0, pc * tok:(pc + 1) * tok, :] + kvacc[1, pc * tok:(pc + 1) * tok, :]).astype(BF16)
        kvb[idx, 0:tok] = kv_sum[:, 0:head]
        kvb[idx, tok:2 * tok] = kv_sum[:, head:]

    last = chips // 2 - 1

    def hop(direction, t, pc):
        src = lax.rem(chip + (chips - t if direction == 0 else t), chips)
        idx = src if pc == 0 else pieces - 1 - src
        return remote(kvb.at[idx], kvb.at[idx], gs.at[direction, t, pc], gr.at[direction, t, pc], up if direction == 0 else down)

    def arrived(direction, t, pc):
        src = lax.rem(chip + (chips - t - 1 if direction == 0 else t + 1), chips)
        idx = src if pc == 0 else pieces - 1 - src
        remote(kvb.at[idx], kvb.at[idx], gs.at[direction, t, pc], gr.at[direction, t, pc], up).wait_recv()

    moves = [[(d, pc) for pc in range(2) for d in range(2) if t < last or d == pc] for t in range(last + 1)]

    def advance(t, only=None):
        for d, pc in moves[t - 1]:
            if only is None or pc == only:
                arrived(d, t - 1, pc)
                if t <= last and (d, pc) in moves[t]:
                    hop(d, t, pc).start()

    for d, pc in moves[0]:
        hop(d, 0, pc).start()

    acc[...] = jnp.zeros_like(acc)
    n_slot = wqb.shape[0]
    nw = group * head // quarters

    def q_step(i, cur, nxt):
        slot = lax.rem(i + 1, n_slot)

        @pl.when(i + 1 < n_q)
        def _():
            wq_copy(i + 1, slot).wait()

        lhs = xb.at[:, pl.ds(pl.multiple_of(i * qd, qd), qd)]
        for k in range(quarters):
            cols = slice(k * nw, (k + 1) * nw)
            acc[:, cols] += dot(lhs[...], cur[:, cols])
            split_part(slot, nxt, k)

        @pl.when(i + 1 + n_slot < n_q)
        def _():
            wq_copy(i + 1 + n_slot, slot).start()

    @pl.loop(0, n_q // 2)
    def _(h):
        q_step(2 * h, wr.at[0], wr.at[1])
        q_step(2 * h + 1, wr.at[1], wr.at[0])

        @pl.when(h == 1)
        def _():
            advance(1, 0)

        @pl.when(h == 2)
        def _():
            advance(1, 1)

        @pl.when(h == 3)
        def _():
            advance(2, 0)

    for g in range(group):
        for pc in range(2):
            q_o[pc, g * tok:(g + 1) * tok, :] = acc[pc * tok:(pc + 1) * tok, g * head:(g + 1) * head].astype(BF16)

    for c in y_loc:
        c.wait()
    for c in y_rem:
        c.wait_recv()

    wide = wob.shape[1] // head
    kw = wob.shape[2]
    n_k = d_model // kw
    for u in range(n_o * n_k):
        n, k = u // n_k, u % n_k
        slot = u % wob.shape[0]
        wo_copy(u, slot).wait()
        part = dot(dyb[:, k * kw:(k + 1) * kw], wob[slot], NT)
        if k == 0:
            acc[:, 0:wide * head] = part
        else:
            acc[:, 0:wide * head] += part
        if u + wob.shape[0] < n_o * n_k:
            wo_copy(u + wob.shape[0], slot).start()
        if k == n_k - 1:
            for g in range(wide):
                for pc in range(2):
                    do_o[pc, (n * wide + g) * tok:(n * wide + g + 1) * tok, :] = acc[pc * tok:(pc + 1) * tok, g * head:(g + 1) * head].astype(BF16)
        if u == 0:
            advance(2, 1)
        elif u == 1:
            advance(3, 0)
        elif u == 2:
            advance(3, 1)
    for t in range(4, last + 2):
        advance(t)
    out = pltpu.make_async_copy(kvb, kv_o, osem.at[0])
    out.start()
    for c in x_rem + y_rem + [m_rem]:
        c.wait_send()
    for t in range(last + 1):
        for d, pc in moves[t]:
            hop(d, t, pc).wait_send()
    out.wait()


def attn_kernel(chips, scale, q, do, kv, md, q_off, o_ref, dq_ref, dkv, s_scr, p_scr, ds_scr, acc_t, k_t, v_t, row_scr, m_ref, l_ref):
    pieces = 2 * chips
    tok = kv.shape[1] // 2 - 8
    head = kv.shape[2]
    lanes_all = q.shape[1]
    group = lanes_all // tok
    lw = 256
    n_lc = lanes_all // lw
    chip = lax.axis_index('cp') // 2
    dkv[...] = jnp.zeros_like(dkv)

    def prep(j, tot):
        v_t[j] = kv[j, tok:2 * tok].astype(F32).T.astype(BF16)
        k_t[j] = kv[j, 0:tok].astype(F32).T.astype(BF16)
        return tot + kv[j, 2 * tok:2 * tok + 16].astype(F32)

    tot = lax.fori_loop(0, pieces, prep, jnp.zeros((16, head), F32))[0:1]

    for pc in range(2):
        place = chip if pc == 0 else pieces - 1 - chip
        doc_q = md[pc].astype(F32)[0:1]
        start = jnp.zeros((1, lanes_all), F32)
        for v in range(1, DOC_VALUES):
            start = jnp.where(doc_q == float(v), tot[:, v:v + 1], start)
        first = jnp.min(start).astype(jnp.int32) // tok
        pos = q_off[...] + (place * tok).astype(F32)
        m_ref[...] = jnp.full_like(m_ref, NEG_BIG)
        l_ref[...] = jnp.zeros_like(l_ref)

        @pl.loop(first, place + 1)
        def _(kb):
            keys = kv[kb, 0:tok]
            u = (lax.broadcasted_iota(jnp.int32, (tok, lw), 0) + kb * tok).astype(F32)
            for lc in range(n_lc):
                ln = slice(lc * lw, (lc + 1) * lw)
                s = dot(keys, q[pc, ln], NT) * (scale * LOG2E)
                s = jnp.where((u >= start[:, ln]) & (u <= pos[:, ln]), s, NEG_BIG)
                s_scr[kb, :, ln] = s
                m_old = m_ref[:, ln]
                m_new = jnp.maximum(m_old, jnp.max(s, axis=0, keepdims=True))
                l_ref[:, ln] = l_ref[:, ln] * jnp.exp2(m_old - m_new) + jnp.sum(jnp.exp2(s - m_new), axis=0, keepdims=True)
                m_ref[:, ln] = m_new

        log_norm = m_ref[...] + jnp.log2(l_ref[...])
        acc_t[...] = jnp.zeros_like(acc_t)

        @pl.loop(first, place + 1)
        def _(kb):
            for lc in range(n_lc):
                ln = slice(lc * lw, (lc + 1) * lw)
                p = jnp.exp2(s_scr[kb, :, ln] - log_norm[:, ln]).astype(BF16)
                p_scr[kb, :, ln] = p
                acc_t[:, ln] += dot(v_t[kb], p)
            dkv[kb, tok:2 * tok] += dot(p_scr[kb], do[pc])

        for lc in range(n_lc):
            ln = slice(lc * lw, (lc + 1) * lw)
            o_bf = acc_t[:, ln].astype(BF16).astype(F32)
            do_t = do[pc, ln].astype(F32).T
            l_ref[:, ln] = jnp.sum(do_t * o_bf, axis=0, keepdims=True)
            row_scr[ln, :] = o_bf.T.astype(BF16)
        for g in range(group):
            o_ref[pc * tok:(pc + 1) * tok, g * head:(g + 1) * head] = row_scr[g * tok:(g + 1) * tok, :]
        acc_t[...] = jnp.zeros_like(acc_t)

        @pl.loop(first, place + 1)
        def _(kb):
            vals = kv[kb, tok:2 * tok]
            for lc in range(n_lc):
                ln = slice(lc * lw, (lc + 1) * lw)
                dp = dot(vals, do[pc, ln], NT)
                ds = (p_scr[kb, :, ln].astype(F32) * (dp - l_ref[:, ln])).astype(BF16)
                ds_scr[:, ln] = ds
                acc_t[:, ln] += dot(k_t[kb], ds)
            dkv[kb, 0:tok] += dot(ds_scr[...], q[pc]) * scale

        for lc in range(n_lc):
            ln = slice(lc * lw, (lc + 1) * lw)
            row_scr[ln, :] = (acc_t[:, ln] * scale).T.astype(BF16)
        for g in range(group):
            dq_ref[pc * tok:(pc + 1) * tok, g * head:(g + 1) * head] = row_scr[g * tok:(g + 1) * tok, :]


def out_kernel(chips, o, dq, dkv, wo, wq, wk, wv, y, dx,
               ob, dqb, own, ring, fin, a2, b2, wob, wqb, wkb, scr, wr, order, dacc, yb, xo,
               loc, ex_s, ex_r, rs, rr, fs, fr, wosem, wqsem, wksem, ysem, xsem, ys, yr, xs, xr):
    tok = own.shape[1] // 2
    head = own.shape[2]
    half = tok // 2
    pieces = 2 * chips
    d_half = yb.shape[1]
    core, chip, partner, up, down = ring_ids(chips)
    mine = (pl.multiple_of(half * core, half), pl.multiple_of(3 * half - half * core, half))
    theirs = (pl.multiple_of(half - half * core, half), pl.multiple_of(2 * half + half * core, half))
    hw = o.shape[1]
    col0 = pl.multiple_of(core * d_half, d_half)
    bw = wob.shape[2]
    n_y = d_half // bw
    qd = wqb.shape[1]
    n_x = d_half // qd
    n_head = wqb.shape[2]
    kc = scr.shape[0] // 2

    def wo_copy(i, slot):
        return pltpu.make_async_copy(wo.at[:, pl.ds(pl.multiple_of(col0 + i * bw, bw), bw)], wob.at[slot], wosem.at[slot])

    def wq_copy(i, slot):
        rows = wqb.shape[1]
        return pltpu.make_async_copy(wq.at[pl.ds(pl.multiple_of(col0 + i * rows, rows), rows)], wqb.at[slot], wqsem.at[slot])

    rows = pl.ds(pl.multiple_of(col0 * 2, 2 * d_half), 2 * d_half)
    wk_copies = [pltpu.make_async_copy(w.at[rows], wkb.at[k], wksem.at[k]) for k, w in enumerate((wk, wv))]
    ocols = pl.ds(pl.multiple_of(core * hw, hw), hw)
    l_own = pltpu.make_async_copy(dkv, own, loc.at[0])
    l_o = pltpu.make_async_copy(o, ob.at[:, ocols], loc.at[1])
    l_dq = pltpu.make_async_copy(dq, dqb.at[:, ocols], loc.at[2])
    r_o = remote(o, ob.at[:, ocols], ex_s.at[0], ex_r.at[0], partner)
    r_dq = remote(dq, dqb.at[:, ocols], ex_s.at[1], ex_r.at[1], partner)

    l_own.start()
    l_o.start()
    l_dq.start()
    for s in range(wob.shape[0]):
        wo_copy(s, s).start()
    entry_barrier((partner, up, down))
    r_o.start()
    r_dq.start()
    for s in range(wqb.shape[0]):
        wq_copy(s, s).start()
    for c in wk_copies:
        c.start()

    steps = chips - 1

    def owner(direction, s):
        chip_w = lax.rem(chip + (2 * chips - 1 - s if direction == 0 else 1 + s), chips)
        return chip_w if direction == 0 else pieces - 1 - chip_w

    def part_rows(row):
        return pl.ds(row, tok)

    def send(direction, s, kvp):
        src = own.at[owner(direction, 0), part_rows(kvp * tok)] if s == 0 else ring.at[direction, s - 1, kvp]
        return remote(src, ring.at[direction, s, kvp], rs.at[direction, s, kvp], rr.at[direction, s, kvp], up if direction == 0 else down)

    def event(e):
        s, kvp = e // 2 + 1, lax.rem(e, 2)
        for d in range(2):
            remote(ring.at[d, s - 1, kvp], ring.at[d, s - 1, kvp], rs.at[d, s - 1, kvp], rr.at[d, s - 1, kvp], up).wait_recv()
            ring[d, s - 1, kvp] = ring[d, s - 1, kvp] + own[owner(d, s), part_rows(pl.multiple_of(kvp * tok, tok))]

        @pl.when(s < steps)
        def _():
            for d in range(2):
                remote(ring.at[d, s - 1, kvp], ring.at[d, s, kvp], rs.at[d, s, kvp], rr.at[d, s, kvp], up if d == 0 else down).start()

    l_own.wait()
    for kvp in range(2):
        for d in range(2):
            send(d, 0, kvp).start()

    def out_copies(buf, dst, i, width, lsem, ssem, rsem):
        cols = pl.ds(pl.multiple_of(col0 + i * width, width), width)
        bc = pl.ds(pl.multiple_of(i * width, width), width)
        for pc in range(2):
            pltpu.make_async_copy(buf.at[pl.ds(mine[pc], half), bc], dst.at[pl.ds(half * pc, half), cols], lsem).start()
            remote(buf.at[pl.ds(theirs[pc], half), bc], dst.at[pl.ds(half * pc, half), cols], ssem, rsem, partner).start()

    l_o.wait()
    r_o.wait_recv()
    ns = wob.shape[0]

    @pl.loop(0, n_y)
    def _(i):
        slot = lax.rem(i, ns)
        wo_copy(i, slot).wait()
        yb[:, pl.ds(pl.multiple_of(i * bw, bw), bw)] = dot(ob[...], wob[slot]).astype(BF16)

        @pl.when(i + ns < n_y)
        def _():
            wo_copy(i + ns, slot).start()

        @pl.when(i > 0)
        def _():
            out_copies(yb, y, i - 1, bw, ysem, ys, yr)

        @pl.when((i >= 3) & (lax.rem(i, 2) == 1))
        def _():
            event((i - 3) // 2)

    out_copies(yb, y, n_y - 1, bw, ysem, ys, yr)

    l_dq.wait()
    r_dq.wait_recv()
    nq = wqb.shape[0]
    quarters = 2
    qs = qd // quarters
    order[...] = sort_matrix()

    def split_part(slot, dst, k):
        split_heads(order[...], wqb.at[slot, k * qs:(k + 1) * qs], dst.at[k * qs:(k + 1) * qs], qs, n_head, head)

    wq_copy(0, 0).wait()
    for k in range(quarters):
        split_part(0, wr.at[0], k)
    wq_copy(nq, 0).start()

    def x_step(i, cur, nxt):
        slot = lax.rem(i + 1, nq)

        @pl.when(i + 1 < n_x)
        def _():
            wq_copy(i + 1, slot).wait()

        dacc[:, pl.ds(pl.multiple_of(i * qd, qd), qd)] = dot(dqb[...], cur[...], NT)
        for k in range(quarters):
            split_part(slot, nxt, k)

        @pl.when(i + 1 + nq < n_x)
        def _():
            wq_copy(i + 1 + nq, slot).start()

    @pl.loop(0, n_x // 2)
    def _(h):
        x_step(2 * h, wr.at[0], wr.at[1])
        event(3 + h)
        x_step(2 * h + 1, wr.at[1], wr.at[0])

    for c in wk_copies:
        c.wait()
    n_e = 2 * steps
    first_e = 3 + n_x // 2

    @pl.loop(first_e, n_e)
    def _(e):
        @pl.when(e < first_e + 4)
        def _():
            j = e - first_e
            rows_b = d_half // 4
            piece = kc // 2
            for k in range(2):
                for m in range(rows_b // piece):
                    r0 = pl.multiple_of(j * rows_b + m * piece, piece)
                    scr[k * kc:(k + 1) * kc, :] = wkb[k, pl.ds(2 * r0, kc), :].astype(F32)
                    for h in range(2):
                        b2[pl.ds(r0, piece), (2 * k + h) * head:(2 * k + h + 1) * head] = scr[pl.ds(k * kc + h, piece, stride=2), :].astype(BF16)

        event(e)

    for kvp in range(2):
        for d in range(2):
            fin[d * tok:(d + 1) * tok, kvp * head:(kvp + 1) * head] = ring[d, steps - 1, kvp].astype(BF16)

    r_fin = remote(fin, a2.at[core], fs, fr, partner)
    r_fin.start()
    a2[core] = fin[...]
    r_fin.wait_recv()
    a_all = jnp.concatenate([a2[0][:, :head], a2[1][:, :head], a2[0][:, head:], a2[1][:, head:]], axis=1)
    for i in range(n_y):
        cs = slice(i * bw, (i + 1) * bw)
        xo[:, cs] = (dacc[:, cs] + dot(a_all, b2[cs, :], NT)).astype(BF16)
        if i > 0:
            out_copies(xo, dx, i - 1, bw, xsem, xs, xr)
    out_copies(xo, dx, n_y - 1, bw, xsem, xs, xr)

    for c in (r_o, r_dq, r_fin):
        c.wait_send()
    for s in range(steps):
        for kvp in range(2):
            for d in range(2):
                send(d, s, kvp).wait_send()
    for buf, dst, lsem, ssem, rsem in ((yb, y, ysem, ys, yr), (xo, dx, xsem, xs, xr)):
        cols = pl.ds(col0, d_half)
        pltpu.make_async_copy(buf.at[pl.ds(0, tok)], dst.at[:, cols], lsem).wait()
        both = remote(buf.at[pl.ds(0, tok)], dst.at[:, cols], ssem, rsem, partner)
        both.wait_send()
        both.wait_recv()


def solution(mesh):
    group_devs = mesh.shape['cp']
    chips = group_devs // 2
    row_spec = P(('dp', 'cp'))
    full_spec = P()
    any_spec = pl.BlockSpec(memory_space=pl.ANY)
    vmem_spec = pl.BlockSpec(memory_space=pltpu.VMEM)
    dma = pltpu.SemaphoreType.DMA

    def local_layer(x_in, dy_in, doc_id, w_q, w_k, w_v, w_o):
        tok, d_model = x_in.shape
        q_heads, head = w_q.shape[1], w_q.shape[2]
        kv_heads = w_k.shape[1]
        group = q_heads // kv_heads
        half = tok // 2
        rows2 = 2 * tok
        pieces = 2 * chips
        lanes = group * tok
        d_half = d_model // 2
        scale = head ** -0.5
        core = lax.axis_index('cp') % 2
        docs = doc_id.reshape(2, half)
        slot = jnp.stack([core, 1 - core])[:, None]
        lane = jnp.arange(tok)
        docf = jnp.concatenate([docs, docs], axis=1).astype(F32)
        docf = jnp.where((lane // half)[None, :] == slot, docf, 0.0)
        ids = jnp.tile(docf, (1, group))
        counts = jnp.sum((docs[:, :, None] < jnp.arange(head)[None, None, :]).astype(F32), axis=1)
        meta = jnp.concatenate([ids, counts], axis=1).astype(BF16)
        meta = jnp.broadcast_to(meta[:, None, :], (2, 16, lanes + head))
        q_off = jnp.tile(lane.astype(F32), (group,))[None, :]

        wq4 = w_q.reshape(d_model, kv_heads, group, head)
        wk2 = w_k.reshape(d_model * kv_heads, head)
        wv2 = w_v.reshape(d_model * kv_heads, head)
        wo2 = w_o.reshape(q_heads * head, d_model)

        n_ch = 4
        cw = d_model // n_ch
        qd = d_model // 8
        hops = chips // 2
        kv_rows = 2 * tok + 16
        q, do, kv, md = pl.pallas_call(
            functools.partial(proj_kernel, chips),
            name='proj',
            out_shape=(jax.ShapeDtypeStruct((2, lanes, head), BF16), jax.ShapeDtypeStruct((2, lanes, head), BF16),
                       jax.ShapeDtypeStruct((pieces, kv_rows, head), BF16), jax.ShapeDtypeStruct((2, 16, lanes), BF16)),
            in_specs=[any_spec] * 7,
            out_specs=(vmem_spec, vmem_spec, any_spec, vmem_spec),
            scratch_shapes=[
                pltpu.VMEM((rows2, d_model), BF16), pltpu.VMEM((rows2, d_model), BF16), pltpu.VMEM((2, 2, 16, lanes + head), BF16),
                pltpu.VMEM((pieces, kv_rows, head), BF16),
                pltpu.VMEM((2 * d_model, head), BF16), pltpu.VMEM((2 * d_model, head), BF16),
                pltpu.VMEM((3, qd, group, head), BF16), pltpu.VMEM((2, 4 * head, d_model // 2), BF16),
                pltpu.VMEM((2, qd, group * head), BF16), pltpu.VMEM((TILE, TILE), BF16), pltpu.VMEM((TILE // 2, TILE), BF16), pltpu.VMEM((d_model, 2 * head), BF16),
                pltpu.VMEM((rows2, group * head), F32), pltpu.VMEM((2, rows2, 2 * head), F32),
                dma((2, 2, n_ch)), dma((2, n_ch)), dma((3,)), dma((2,)),
                dma((2, n_ch)), dma((2, n_ch)), dma((2, n_ch)), dma((2, n_ch)), dma, dma,
                dma((2, hops, 2)), dma((2, hops, 2)), dma((1,)),
            ],
            compiler_params=pltpu.CompilerParams(collective_id=0, has_side_effects=True, vmem_limit_bytes=60 << 20),
        )(x_in, dy_in, meta, wq4, wk2, wv2, wo2)

        o, dq, dkv = pl.pallas_call(
            functools.partial(attn_kernel, chips, scale),
            name='attn',
            out_shape=(jax.ShapeDtypeStruct((rows2, group * head), BF16), jax.ShapeDtypeStruct((rows2, group * head), BF16),
                       jax.ShapeDtypeStruct((pieces, 2 * tok, head), F32)),
            in_specs=[vmem_spec] * 5,
            out_specs=(vmem_spec,) * 3,
            scratch_shapes=[
                pltpu.VMEM((pieces, tok, lanes), F32), pltpu.VMEM((pieces, tok, lanes), BF16), pltpu.VMEM((tok, lanes), BF16),
                pltpu.VMEM((head, lanes), F32), pltpu.VMEM((pieces, head, tok), BF16), pltpu.VMEM((pieces, head, tok), BF16),
                pltpu.VMEM((lanes, head), BF16), pltpu.VMEM((1, lanes), F32), pltpu.VMEM((1, lanes), F32),
            ],
            compiler_params=pltpu.CompilerParams(vmem_limit_bytes=60 << 20),
        )(q, do, kv, md, q_off)

        steps = chips - 1
        bw = d_half // 8
        y, dx = pl.pallas_call(
            functools.partial(out_kernel, chips),
            name='out',
            out_shape=(jax.ShapeDtypeStruct((tok, d_model), BF16), jax.ShapeDtypeStruct((tok, d_model), BF16)),
            in_specs=[any_spec] * 7,
            out_specs=(any_spec, any_spec),
            scratch_shapes=[
                pltpu.VMEM((rows2, q_heads * head), BF16), pltpu.VMEM((rows2, q_heads * head), BF16),
                pltpu.VMEM((pieces, 2 * tok, head), F32), pltpu.VMEM((2, steps, 2, tok, head), F32),
                pltpu.VMEM((rows2, 2 * head), BF16), pltpu.VMEM((2, rows2, 2 * head), BF16), pltpu.VMEM((d_half, 4 * head), BF16),
                pltpu.VMEM((3, q_heads * head, bw), BF16), pltpu.VMEM((3, bw, q_heads, head), BF16),
                pltpu.VMEM((2, 2 * d_half, head), BF16),
                pltpu.VMEM((1024, head), F32), pltpu.VMEM((2, bw, q_heads * head), BF16), pltpu.VMEM((TILE, TILE), BF16),
                pltpu.VMEM((rows2, d_half), F32), pltpu.VMEM((rows2, d_half), BF16), pltpu.VMEM((rows2, d_half), BF16),
                dma((3,)), dma((2,)), dma((2,)), dma((2, steps, 2)), dma((2, steps, 2)), dma, dma,
                dma((3,)), dma((3,)), dma((2,)), dma, dma, dma, dma, dma, dma,
            ],
            compiler_params=pltpu.CompilerParams(collective_id=1, has_side_effects=True, vmem_limit_bytes=62 << 20),
        )(o, dq, dkv, wo2, w_q, wk2, wv2)
        return y, dx

    return jax.shard_map(local_layer, mesh=mesh,
                         in_specs=(row_spec, row_spec, row_spec, full_spec, full_spec, full_spec, full_spec),
                         out_specs=(row_spec, row_spec), check_vma=False)
```

```python
import functools

import jax
import jax.numpy as jnp
from jax import lax
from jax.experimental import pallas as pl
from jax.experimental.pallas import tpu as pltpu
from jax.sharding import PartitionSpec as P

MESH = pl.DeviceIdType.MESH
NEG_BIG = -1.0e30
LOG2E = 1.4426950408889634
F32, BF16 = jnp.float32, jnp.bfloat16
NT = (((1,), (1,)), ((), ()))
NN = (((1,), (0,)), ((), ()))
DOC_VALUES = 9


def dot(a, b, dims=NN):
    return lax.dot_general(a, b, dims, preferred_element_type=F32)


def remote(src, dst, send, recv, dev):
    return pltpu.make_async_remote_copy(src_ref=src, dst_ref=dst, send_sem=send, recv_sem=recv,
                                        device_id={'cp': dev}, device_id_type=MESH)


def ring_ids(chips):
    me = lax.axis_index('cp')
    core, chip = lax.rem(me, 2), me // 2
    return core, chip, chip * 2 + 1 - core, lax.rem(chip + 1, chips) * 2 + core, lax.rem(chip + chips - 1, chips) * 2 + core


def entry_barrier(devs):
    barrier = pltpu.get_barrier_semaphore()
    for dev in devs:
        pl.semaphore_signal(barrier, inc=1, device_id={'cp': dev}, device_id_type=MESH)
    pl.semaphore_wait(barrier, len(devs))


TILE = 256
PER = 8


def sort_matrix():
    toks = TILE // PER
    r = lax.broadcasted_iota(jnp.int32, (TILE, TILE), 0)
    c = lax.broadcasted_iota(jnp.int32, (TILE, TILE), 1)
    t = r & (toks - 1)
    return jnp.where(c == t * PER + lax.shift_right_logical(r, toks.bit_length() - 1), 1.0, 0.0).astype(BF16)


def split_heads(order, src, dst, count, n_head, head):
    toks = TILE // PER
    for h0 in range(0, n_head, PER):
        for t0 in range(0, count, 4 * toks):
            side = [src[t0 + k * toks:t0 + (k + 1) * toks, h0:h0 + PER, :].reshape(TILE, head) for k in range(4)]
            rows = dot(order, jnp.concatenate(side, axis=1)).astype(BF16)
            for k in range(4):
                for g in range(PER):
                    dst[t0 + k * toks:t0 + (k + 1) * toks, (h0 + g) * head:(h0 + g + 1) * head] = rows[g * toks:(g + 1) * toks, k * head:(k + 1) * head]


def proj_kernel(chips, x, dy, meta, wq, wk, wv, wo, q_o, do_o, kv_o, md_o,
                xb, dyb, mb, kvb, wkb, wvb, wqb, wob, wr, order, pick, wkv, acc, kvacc,
                loc, wksem, wqsem, wosem, xs, xr, ys, yr, ms, mr, gs, gr, osem):
    half = x.shape[0] // 2
    d_model = x.shape[1]
    tok = 2 * half
    pieces = 2 * chips
    n_ch = xs.shape[1]
    cw = d_model // n_ch
    core, chip, partner, up, down = ring_ids(chips)
    row_off = (pl.multiple_of(half * core, half), pl.multiple_of(3 * half - half * core, half))
    n_q, qd = d_model // wqb.shape[1], wqb.shape[1]
    group = wqb.shape[2]
    head = wqb.shape[3]
    n_o = group * head // wob.shape[1]

    def wq_copy(i, slot):
        return pltpu.make_async_copy(wq.at[pl.ds(i * qd, qd), core], wqb.at[slot], wqsem.at[slot])

    def wo_copy(i, slot):
        rows, kw = wob.shape[1], wob.shape[2]
        n, k = i // (d_model // kw), i % (d_model // kw)
        return pltpu.make_async_copy(wo.at[pl.ds(core * group * head + n * rows, rows), pl.ds(k * kw, kw)], wob.at[slot], wosem.at[slot])

    wk_copies = []
    for ch in range(n_ch):
        rows = pl.ds(ch * 2 * cw, 2 * cw)
        wk_copies.append((pltpu.make_async_copy(wk.at[rows], wkb.at[rows], wksem.at[0, ch]),
                          pltpu.make_async_copy(wv.at[rows], wvb.at[rows], wksem.at[1, ch])))
    x_loc, y_loc, x_rem, y_rem = [], [], [], []
    for ch in range(n_ch):
        cols = pl.ds(ch * cw, cw)
        for pc in range(2):
            src = pl.ds(half * pc, half)
            dst = pl.ds(row_off[pc], half)
            x_loc.append(pltpu.make_async_copy(x.at[src, cols], xb.at[dst, cols], loc.at[0, pc, ch]))
            y_loc.append(pltpu.make_async_copy(dy.at[src, cols], dyb.at[dst, cols], loc.at[1, pc, ch]))
            x_rem.append(remote(x.at[src, cols], xb.at[dst, cols], xs.at[pc, ch], xr.at[pc, ch], partner))
            y_rem.append(remote(dy.at[src, cols], dyb.at[dst, cols], ys.at[pc, ch], yr.at[pc, ch], partner))
    m_loc = pltpu.make_async_copy(meta, mb.at[0], osem.at[0])
    m_rem = remote(meta, mb.at[1], ms, mr, partner)

    for ch in range(n_ch):
        x_loc[2 * ch].start()
        x_loc[2 * ch + 1].start()
        wk_copies[ch][0].start()
        wk_copies[ch][1].start()
    m_loc.start()
    for s in range(wqb.shape[0]):
        wq_copy(s, s).start()
    entry_barrier((partner, up, down))
    for c in x_rem:
        c.start()
    m_rem.start()
    for c in y_rem:
        c.start()
    for c in y_loc:
        c.start()
    for s in range(wob.shape[0]):
        wo_copy(s, s).start()

    r = lax.broadcasted_iota(jnp.int32, pick.shape, 0)
    pick[...] = jnp.where(lax.broadcasted_iota(jnp.int32, pick.shape, 1) == 2 * r + core, 1.0, 0.0).astype(BF16)
    order[...] = sort_matrix()
    n_sub = TILE // 2
    for ch in range(n_ch):
        for c in wk_copies[ch]:
            c.wait()
        for j in range(ch * cw // n_sub, (ch + 1) * cw // n_sub, 2):
            side = [buf[t * 2 * n_sub:(t + 1) * 2 * n_sub, :] for t in (j, j + 1) for buf in (wkb, wvb)]
            rows = dot(pick[...], jnp.concatenate(side, axis=1)).astype(BF16)
            wkv[j * n_sub:(j + 1) * n_sub, :] = rows[:, :2 * head]
            wkv[(j + 1) * n_sub:(j + 2) * n_sub, :] = rows[:, 2 * head:]
    quarters = 2
    qs = qd // quarters

    def split_part(slot, dst, k):
        split_heads(order[...], wqb.at[slot, k * qs:(k + 1) * qs], dst.at[k * qs:(k + 1) * qs], qs, group, head)

    wq_copy(0, 0).wait()
    for k in range(quarters):
        split_part(0, wr.at[0], k)
    wq_copy(wqb.shape[0], 0).start()
    for ch in range(n_ch):
        for c in (x_loc[2 * ch], x_loc[2 * ch + 1]):
            c.wait()
        for c in (x_rem[2 * ch], x_rem[2 * ch + 1]):
            c.wait_recv()
        hc = cw // 2
        for k in range(2):
            part_sum = dot(xb[:, ch * cw + k * hc:ch * cw + (k + 1) * hc], wkv[ch * cw + k * hc:ch * cw + (k + 1) * hc])
            if ch == 0:
                kvacc[k] = part_sum
            else:
                kvacc[k] += part_sum
    m_loc.wait()
    m_rem.wait_recv()
    lo, hi = chip, pieces - 1 - chip
    width = md_o.shape[2]
    for pc, idx in ((0, lo), (1, hi)):
        both = (mb[0, pc].astype(F32) + mb[1, pc].astype(F32)).astype(BF16)
        md_o[pc] = both[:, :width]
        kvb[idx, 2 * tok:2 * tok + 16] = both[:, width:]
        kv_sum = (kvacc[0, pc * tok:(pc + 1) * tok, :] + kvacc[1, pc * tok:(pc + 1) * tok, :]).astype(BF16)
        kvb[idx, 0:tok] = kv_sum[:, 0:head]
        kvb[idx, tok:2 * tok] = kv_sum[:, head:]

    last = chips // 2 - 1

    def hop(direction, t, pc):
        src = lax.rem(chip + (chips - t if direction == 0 else t), chips)
        idx = src if pc == 0 else pieces - 1 - src
        return remote(kvb.at[idx], kvb.at[idx], gs.at[direction, t, pc], gr.at[direction, t, pc], up if direction == 0 else down)

    def arrived(direction, t, pc):
        src = lax.rem(chip + (chips - t - 1 if direction == 0 else t + 1), chips)
        idx = src if pc == 0 else pieces - 1 - src
        remote(kvb.at[idx], kvb.at[idx], gs.at[direction, t, pc], gr.at[direction, t, pc], up).wait_recv()

    moves = [[(d, pc) for pc in range(2) for d in range(2) if t < last or d == pc] for t in range(last + 1)]

    def advance(t, only=None):
        for d, pc in moves[t - 1]:
            if only is None or pc == only:
                arrived(d, t - 1, pc)
                if t <= last and (d, pc) in moves[t]:
                    hop(d, t, pc).start()

    for d, pc in moves[0]:
        hop(d, 0, pc).start()

    acc[...] = jnp.zeros_like(acc)
    n_slot = wqb.shape[0]
    nw = group * head // quarters

    def q_step(i, cur, nxt):
        slot = lax.rem(i + 1, n_slot)

        @pl.when(i + 1 < n_q)
        def _():
            wq_copy(i + 1, slot).wait()

        lhs = xb.at[:, pl.ds(pl.multiple_of(i * qd, qd), qd)]
        for k in range(quarters):
            cols = slice(k * nw, (k + 1) * nw)
            acc[:, cols] += dot(lhs[...], cur[:, cols])
            split_part(slot, nxt, k)

        @pl.when(i + 1 + n_slot < n_q)
        def _():
            wq_copy(i + 1 + n_slot, slot).start()

    @pl.loop(0, n_q // 2)
    def _(h):
        q_step(2 * h, wr.at[0], wr.at[1])
        q_step(2 * h + 1, wr.at[1], wr.at[0])

        @pl.when(h == 1)
        def _():
            advance(1, 0)

        @pl.when(h == 2)
        def _():
            advance(1, 1)

        @pl.when(h == 3)
        def _():
            advance(2, 0)

    for g in range(group):
        for pc in range(2):
            q_o[pc, g * tok:(g + 1) * tok, :] = acc[pc * tok:(pc + 1) * tok, g * head:(g + 1) * head].astype(BF16)

    for c in y_loc:
        c.wait()
    for c in y_rem:
        c.wait_recv()

    wide = wob.shape[1] // head
    kw = wob.shape[2]
    n_k = d_model // kw
    for u in range(n_o * n_k):
        n, k = u // n_k, u % n_k
        slot = u % wob.shape[0]
        wo_copy(u, slot).wait()
        part = dot(dyb[:, k * kw:(k + 1) * kw], wob[slot], NT)
        if k == 0:
            acc[:, 0:wide * head] = part
        else:
            acc[:, 0:wide * head] += part
        if u + wob.shape[0] < n_o * n_k:
            wo_copy(u + wob.shape[0], slot).start()
        if k == n_k - 1:
            for g in range(wide):
                for pc in range(2):
                    do_o[pc, (n * wide + g) * tok:(n * wide + g + 1) * tok, :] = acc[pc * tok:(pc + 1) * tok, g * head:(g + 1) * head].astype(BF16)
        if u == 0:
            advance(2, 1)
        elif u == 1:
            advance(3, 0)
        elif u == 2:
            advance(3, 1)
    for t in range(4, last + 2):
        advance(t)
    out = pltpu.make_async_copy(kvb, kv_o, osem.at[0])
    out.start()
    for c in x_rem + y_rem + [m_rem]:
        c.wait_send()
    for t in range(last + 1):
        for d, pc in moves[t]:
            hop(d, t, pc).wait_send()
    out.wait()


def attn_kernel(chips, scale, q, do, kv, md, q_off, o_ref, dq_ref, dkv, s_scr, p_scr, acc_t, row_scr, m_ref, l_ref):
    pieces = 2 * chips
    tok = kv.shape[1] // 2 - 8
    head = kv.shape[2]
    lanes_all = q.shape[1]
    group = lanes_all // tok
    lw = 256
    lanes = [slice(a, a + lw) for a in range(0, lanes_all, lw)]
    chip = lax.axis_index('cp') // 2
    dkv[...] = jnp.zeros_like(dkv)
    tot = lax.fori_loop(0, pieces, lambda j, a: a + kv[j, 2 * tok:2 * tok + 16].astype(F32), jnp.zeros((16, head), F32))[0:1]

    @pl.loop(0, 2)
    def _(pc):
        place = jnp.where(pc == 0, chip, pieces - 1 - chip)
        doc_q = md[pc].astype(F32)[0:1]
        start = jnp.zeros((1, lanes_all), F32)
        for v in range(1, DOC_VALUES):
            start = jnp.where(doc_q == float(v), tot[:, v:v + 1], start)
        first = jnp.min(start).astype(jnp.int32) // tok
        pos = q_off[...] + (place * tok).astype(F32)
        n_pair = (place - first + 2) // 2
        m_ref[...] = jnp.full_like(m_ref, NEG_BIG)
        l_ref[...] = jnp.zeros_like(l_ref)

        def rows_of(t, base):
            kb = place - 2 * t
            return jnp.concatenate([kv[jnp.maximum(kb - 1, 0), base:base + tok], kv[kb, base:base + tok]], axis=0)

        def add_rows(t, base, val):
            kb = place - 2 * t
            dkv[kb, base:base + tok] += val[tok:]
            dkv[jnp.maximum(kb - 1, 0), base:base + tok] += val[:tok]

        def score(t, masked):
            keys = rows_of(t, 0)
            u = (lax.broadcasted_iota(jnp.int32, (2 * tok, lw), 0) + (place - 2 * t - 1) * tok).astype(F32)
            scales = []
            for ln in lanes:
                s = dot(keys, q[pc, ln], NT) * (scale * LOG2E)
                if masked:
                    s = jnp.where((u >= start[:, ln]) & (u <= pos[:, ln]), s, NEG_BIG)
                s_scr[t, :, ln] = s
                m_old = m_ref[:, ln]
                m_new = jnp.maximum(m_old, jnp.max(s, axis=0, keepdims=True))
                m_ref[:, ln] = m_new
                scales.append((m_new, jnp.exp2(m_old - m_new)))
            for ln, (m_new, shrink) in zip(lanes, scales):
                l_ref[:, ln] = l_ref[:, ln] * shrink + jnp.sum(jnp.exp2(s_scr[t, :, ln] - m_new), axis=0, keepdims=True)

        last_start = (jnp.max(start).astype(jnp.int32) + tok - 1) // tok
        n_full = jnp.maximum((place - last_start - 1) // 2, 0)

        @pl.loop(0, n_pair)
        def _(t):
            inside = (t >= 1) & (t <= n_full)

            @pl.when(inside)
            def _():
                score(t, False)

            @pl.when(jnp.logical_not(inside))
            def _():
                score(t, True)

        log_norm = m_ref[...] + jnp.log2(l_ref[...])
        acc_t[...] = jnp.zeros_like(acc_t)

        @pl.loop(0, n_pair)
        def _(t):
            v_t = rows_of(t, tok).astype(F32).T.astype(BF16)
            dv = jnp.zeros((2 * tok, head), F32)
            for ln in lanes:
                p = jnp.exp2(s_scr[t, :, ln] - log_norm[:, ln]).astype(BF16)
                p_scr[t, :, ln] = p
                acc_t[:, ln] += dot(v_t, p)
                dv = dv + dot(p, do[pc, ln])
            add_rows(t, tok, dv)

        for ln in lanes:
            o_bf = acc_t[:, ln].astype(BF16).astype(F32)
            do_t = do[pc, ln].astype(F32).T
            l_ref[:, ln] = jnp.sum(do_t * o_bf, axis=0, keepdims=True)
            row_scr[ln, :] = o_bf.T.astype(BF16)
        out_rows = pl.ds(pl.multiple_of(pc * tok, tok), tok)
        for g in range(group):
            o_ref[out_rows, g * head:(g + 1) * head] = row_scr[g * tok:(g + 1) * tok, :]
        acc_t[...] = jnp.zeros_like(acc_t)

        @pl.loop(0, n_pair)
        def _(t):
            vals = rows_of(t, tok)
            k_t = rows_of(t, 0).astype(F32).T.astype(BF16)
            dk = jnp.zeros((2 * tok, head), F32)
            nxt = dot(vals, do[pc, lanes[0]], NT)
            for i, ln in enumerate(lanes):
                dp = nxt
                if i + 1 < len(lanes):
                    nxt = dot(vals, do[pc, lanes[i + 1]], NT)
                ds = (p_scr[t, :, ln].astype(F32) * (dp - l_ref[:, ln])).astype(BF16)
                acc_t[:, ln] += dot(k_t, ds)
                dk = dk + dot(ds, q[pc, ln])
            add_rows(t, 0, dk * scale)

        for ln in lanes:
            row_scr[ln, :] = (acc_t[:, ln] * scale).T.astype(BF16)
        for g in range(group):
            dq_ref[out_rows, g * head:(g + 1) * head] = row_scr[g * tok:(g + 1) * tok, :]


def out_kernel(chips, o, dq, dkv, wo, wq, wk, wv, y, dx,
               ob, dqb, own, ring, fin, a2, b2, wob, wqb, wkb, scr, wr, order, dacc, yb, xo,
               loc, ex_s, ex_r, rs, rr, fs, fr, wosem, wqsem, wksem, ysem, xsem, ys, yr, xs, xr):
    tok = own.shape[1] // 2
    head = own.shape[2]
    half = tok // 2
    pieces = 2 * chips
    d_half = yb.shape[1]
    core, chip, partner, up, down = ring_ids(chips)
    mine = (pl.multiple_of(half * core, half), pl.multiple_of(3 * half - half * core, half))
    theirs = (pl.multiple_of(half - half * core, half), pl.multiple_of(2 * half + half * core, half))
    hw = o.shape[1]
    col0 = pl.multiple_of(core * d_half, d_half)
    bw = wob.shape[2]
    n_y = d_half // bw
    qd = wqb.shape[1]
    n_x = d_half // qd
    n_head = wqb.shape[2]
    kc = scr.shape[0] // 2

    def wo_copy(i, slot):
        return pltpu.make_async_copy(wo.at[:, pl.ds(pl.multiple_of(col0 + i * bw, bw), bw)], wob.at[slot], wosem.at[slot])

    def wq_copy(i, slot):
        rows = wqb.shape[1]
        return pltpu.make_async_copy(wq.at[pl.ds(pl.multiple_of(col0 + i * rows, rows), rows)], wqb.at[slot], wqsem.at[slot])

    rows = pl.ds(pl.multiple_of(col0 * 2, 2 * d_half), 2 * d_half)
    wk_copies = [pltpu.make_async_copy(w.at[rows], wkb.at[k], wksem.at[k]) for k, w in enumerate((wk, wv))]
    ocols = pl.ds(pl.multiple_of(core * hw, hw), hw)
    l_own = pltpu.make_async_copy(dkv, own, loc.at[0])
    l_o = pltpu.make_async_copy(o, ob.at[:, ocols], loc.at[1])
    l_dq = pltpu.make_async_copy(dq, dqb.at[:, ocols], loc.at[2])
    r_o = remote(o, ob.at[:, ocols], ex_s.at[0], ex_r.at[0], partner)
    r_dq = remote(dq, dqb.at[:, ocols], ex_s.at[1], ex_r.at[1], partner)

    l_own.start()
    l_o.start()
    l_dq.start()
    for s in range(wob.shape[0]):
        wo_copy(s, s).start()
    entry_barrier((partner, up, down))
    r_o.start()
    r_dq.start()
    for s in range(wqb.shape[0]):
        wq_copy(s, s).start()
    for c in wk_copies:
        c.start()

    steps = chips - 1

    def owner(direction, s):
        chip_w = lax.rem(chip + (2 * chips - 1 - s if direction == 0 else 1 + s), chips)
        return chip_w if direction == 0 else pieces - 1 - chip_w

    def part_rows(row):
        return pl.ds(row, tok)

    def send(direction, s, kvp):
        src = own.at[owner(direction, 0), part_rows(kvp * tok)] if s == 0 else ring.at[direction, s - 1, kvp]
        return remote(src, ring.at[direction, s, kvp], rs.at[direction, s, kvp], rr.at[direction, s, kvp], up if direction == 0 else down)

    def event(e):
        s, kvp = e // 2 + 1, lax.rem(e, 2)
        for d in range(2):
            remote(ring.at[d, s - 1, kvp], ring.at[d, s - 1, kvp], rs.at[d, s - 1, kvp], rr.at[d, s - 1, kvp], up).wait_recv()
            ring[d, s - 1, kvp] = ring[d, s - 1, kvp] + own[owner(d, s), part_rows(pl.multiple_of(kvp * tok, tok))]

        @pl.when(s < steps)
        def _():
            for d in range(2):
                remote(ring.at[d, s - 1, kvp], ring.at[d, s, kvp], rs.at[d, s, kvp], rr.at[d, s, kvp], up if d == 0 else down).start()

    l_own.wait()
    for kvp in range(2):
        for d in range(2):
            send(d, 0, kvp).start()

    def out_copies(buf, dst, i, width, lsem, ssem, rsem):
        cols = pl.ds(pl.multiple_of(col0 + i * width, width), width)
        bc = pl.ds(pl.multiple_of(i * width, width), width)
        for pc in range(2):
            pltpu.make_async_copy(buf.at[pl.ds(mine[pc], half), bc], dst.at[pl.ds(half * pc, half), cols], lsem).start()
            remote(buf.at[pl.ds(theirs[pc], half), bc], dst.at[pl.ds(half * pc, half), cols], ssem, rsem, partner).start()

    l_o.wait()
    r_o.wait_recv()
    ns = wob.shape[0]

    @pl.loop(0, n_y)
    def _(i):
        slot = lax.rem(i, ns)
        wo_copy(i, slot).wait()
        yb[:, pl.ds(pl.multiple_of(i * bw, bw), bw)] = dot(ob[...], wob[slot]).astype(BF16)

        @pl.when(i + ns < n_y)
        def _():
            wo_copy(i + ns, slot).start()

        @pl.when(i > 0)
        def _():
            out_copies(yb, y, i - 1, bw, ysem, ys, yr)

        @pl.when((i >= 3) & (lax.rem(i, 2) == 1))
        def _():
            event((i - 3) // 2)

    out_copies(yb, y, n_y - 1, bw, ysem, ys, yr)

    l_dq.wait()
    r_dq.wait_recv()
    nq = wqb.shape[0]
    quarters = 2
    qs = qd // quarters
    order[...] = sort_matrix()

    def split_part(slot, dst, k):
        split_heads(order[...], wqb.at[slot, k * qs:(k + 1) * qs], dst.at[k * qs:(k + 1) * qs], qs, n_head, head)

    wq_copy(0, 0).wait()
    for k in range(quarters):
        split_part(0, wr.at[0], k)
    wq_copy(nq, 0).start()

    def x_step(i, cur, nxt):
        slot = lax.rem(i + 1, nq)

        @pl.when(i + 1 < n_x)
        def _():
            wq_copy(i + 1, slot).wait()

        dacc[:, pl.ds(pl.multiple_of(i * qd, qd), qd)] = dot(dqb[...], cur[...], NT)
        for k in range(quarters):
            split_part(slot, nxt, k)

        @pl.when(i + 1 + nq < n_x)
        def _():
            wq_copy(i + 1 + nq, slot).start()

    @pl.loop(0, n_x // 2)
    def _(h):
        x_step(2 * h, wr.at[0], wr.at[1])
        event(3 + 2 * h)
        x_step(2 * h + 1, wr.at[1], wr.at[0])
        event(4 + 2 * h)

    for c in wk_copies:
        c.wait()
    n_e = 2 * steps
    first_e = 3 + n_x

    @pl.loop(first_e, n_e)
    def _(e):
        @pl.when(e < first_e + 2)
        def _():
            j = e - first_e
            rows_b = d_half // 2
            piece = kc // 2
            for k in range(2):
                for m in range(rows_b // piece):
                    r0 = pl.multiple_of(j * rows_b + m * piece, piece)
                    scr[k * kc:(k + 1) * kc, :] = wkb[k, pl.ds(2 * r0, kc), :].astype(F32)
                    for h in range(2):
                        b2[pl.ds(r0, piece), (2 * k + h) * head:(2 * k + h + 1) * head] = scr[pl.ds(k * kc + h, piece, stride=2), :].astype(BF16)

        event(e)

    for kvp in range(2):
        for d in range(2):
            fin[d * tok:(d + 1) * tok, kvp * head:(kvp + 1) * head] = ring[d, steps - 1, kvp].astype(BF16)

    r_fin = remote(fin, a2.at[core], fs, fr, partner)
    r_fin.start()
    a2[core] = fin[...]
    r_fin.wait_recv()
    a_all = jnp.concatenate([a2[0][:, :head], a2[1][:, :head], a2[0][:, head:], a2[1][:, head:]], axis=1)
    for i in range(n_y):
        cs = slice(i * bw, (i + 1) * bw)
        xo[:, cs] = (dacc[:, cs] + dot(a_all, b2[cs, :], NT)).astype(BF16)
        if i > 0:
            out_copies(xo, dx, i - 1, bw, xsem, xs, xr)
    out_copies(xo, dx, n_y - 1, bw, xsem, xs, xr)

    for c in (r_o, r_dq, r_fin):
        c.wait_send()
    for s in range(steps):
        for kvp in range(2):
            for d in range(2):
                send(d, s, kvp).wait_send()
    for buf, dst, lsem, ssem, rsem in ((yb, y, ysem, ys, yr), (xo, dx, xsem, xs, xr)):
        cols = pl.ds(col0, d_half)
        pltpu.make_async_copy(buf.at[pl.ds(0, tok)], dst.at[:, cols], lsem).wait()
        both = remote(buf.at[pl.ds(0, tok)], dst.at[:, cols], ssem, rsem, partner)
        both.wait_send()
        both.wait_recv()


def solution(mesh):
    group_devs = mesh.shape['cp']
    chips = group_devs // 2
    row_spec = P(('dp', 'cp'))
    full_spec = P()
    any_spec = pl.BlockSpec(memory_space=pl.ANY)
    vmem_spec = pl.BlockSpec(memory_space=pltpu.VMEM)
    dma = pltpu.SemaphoreType.DMA

    def local_layer(x_in, dy_in, doc_id, w_q, w_k, w_v, w_o):
        tok, d_model = x_in.shape
        q_heads, head = w_q.shape[1], w_q.shape[2]
        kv_heads = w_k.shape[1]
        group = q_heads // kv_heads
        half = tok // 2
        rows2 = 2 * tok
        pieces = 2 * chips
        lanes = group * tok
        d_half = d_model // 2
        scale = head ** -0.5
        core = lax.axis_index('cp') % 2
        docs = doc_id.reshape(2, half)
        slot = jnp.stack([core, 1 - core])[:, None]
        lane = jnp.arange(tok)
        docf = jnp.concatenate([docs, docs], axis=1).astype(F32)
        docf = jnp.where((lane // half)[None, :] == slot, docf, 0.0)
        ids = jnp.tile(docf, (1, group))
        counts = jnp.sum((docs[:, :, None] < jnp.arange(head)[None, None, :]).astype(F32), axis=1)
        meta = jnp.concatenate([ids, counts], axis=1).astype(BF16)
        meta = jnp.broadcast_to(meta[:, None, :], (2, 16, lanes + head))
        q_off = jnp.tile(lane.astype(F32), (group,))[None, :]

        wq4 = w_q.reshape(d_model, kv_heads, group, head)
        wk2 = w_k.reshape(d_model * kv_heads, head)
        wv2 = w_v.reshape(d_model * kv_heads, head)
        wo2 = w_o.reshape(q_heads * head, d_model)

        n_ch = 4
        cw = d_model // n_ch
        qd = d_model // 8
        hops = chips // 2
        kv_rows = 2 * tok + 16
        q, do, kv, md = pl.pallas_call(
            functools.partial(proj_kernel, chips),
            name='proj',
            out_shape=(jax.ShapeDtypeStruct((2, lanes, head), BF16), jax.ShapeDtypeStruct((2, lanes, head), BF16),
                       jax.ShapeDtypeStruct((pieces, kv_rows, head), BF16), jax.ShapeDtypeStruct((2, 16, lanes), BF16)),
            in_specs=[any_spec] * 7,
            out_specs=(vmem_spec, vmem_spec, any_spec, vmem_spec),
            scratch_shapes=[
                pltpu.VMEM((rows2, d_model), BF16), pltpu.VMEM((rows2, d_model), BF16), pltpu.VMEM((2, 2, 16, lanes + head), BF16),
                pltpu.VMEM((pieces, kv_rows, head), BF16),
                pltpu.VMEM((2 * d_model, head), BF16), pltpu.VMEM((2 * d_model, head), BF16),
                pltpu.VMEM((3, qd, group, head), BF16), pltpu.VMEM((2, 4 * head, d_model // 2), BF16),
                pltpu.VMEM((2, qd, group * head), BF16), pltpu.VMEM((TILE, TILE), BF16), pltpu.VMEM((TILE // 2, TILE), BF16), pltpu.VMEM((d_model, 2 * head), BF16),
                pltpu.VMEM((rows2, group * head), F32), pltpu.VMEM((2, rows2, 2 * head), F32),
                dma((2, 2, n_ch)), dma((2, n_ch)), dma((3,)), dma((2,)),
                dma((2, n_ch)), dma((2, n_ch)), dma((2, n_ch)), dma((2, n_ch)), dma, dma,
                dma((2, hops, 2)), dma((2, hops, 2)), dma((1,)),
            ],
            compiler_params=pltpu.CompilerParams(collective_id=0, has_side_effects=True, vmem_limit_bytes=60 << 20),
        )(x_in, dy_in, meta, wq4, wk2, wv2, wo2)

        o, dq, dkv = pl.pallas_call(
            functools.partial(attn_kernel, chips, scale),
            name='attn',
            out_shape=(jax.ShapeDtypeStruct((rows2, group * head), BF16), jax.ShapeDtypeStruct((rows2, group * head), BF16),
                       jax.ShapeDtypeStruct((pieces, 2 * tok, head), F32)),
            in_specs=[vmem_spec] * 5,
            out_specs=(vmem_spec,) * 3,
            scratch_shapes=[
                pltpu.VMEM((chips, rows2, lanes), F32), pltpu.VMEM((chips, rows2, lanes), BF16), pltpu.VMEM((head, lanes), F32),
                pltpu.VMEM((lanes, head), BF16), pltpu.VMEM((1, lanes), F32), pltpu.VMEM((1, lanes), F32),
            ],
            compiler_params=pltpu.CompilerParams(vmem_limit_bytes=60 << 20),
        )(q, do, kv, md, q_off)

        steps = chips - 1
        bw = d_half // 8
        y, dx = pl.pallas_call(
            functools.partial(out_kernel, chips),
            name='out',
            out_shape=(jax.ShapeDtypeStruct((tok, d_model), BF16), jax.ShapeDtypeStruct((tok, d_model), BF16)),
            in_specs=[any_spec] * 7,
            out_specs=(any_spec, any_spec),
            scratch_shapes=[
                pltpu.VMEM((rows2, q_heads * head), BF16), pltpu.VMEM((rows2, q_heads * head), BF16),
                pltpu.VMEM((pieces, 2 * tok, head), F32), pltpu.VMEM((2, steps, 2, tok, head), F32),
                pltpu.VMEM((rows2, 2 * head), BF16), pltpu.VMEM((2, rows2, 2 * head), BF16), pltpu.VMEM((d_half, 4 * head), BF16),
                pltpu.VMEM((3, q_heads * head, bw), BF16), pltpu.VMEM((3, bw, q_heads, head), BF16),
                pltpu.VMEM((2, 2 * d_half, head), BF16),
                pltpu.VMEM((1024, head), F32), pltpu.VMEM((2, bw, q_heads * head), BF16), pltpu.VMEM((TILE, TILE), BF16),
                pltpu.VMEM((rows2, d_half), F32), pltpu.VMEM((rows2, d_half), BF16), pltpu.VMEM((rows2, d_half), BF16),
                dma((3,)), dma((2,)), dma((2,)), dma((2, steps, 2)), dma((2, steps, 2)), dma, dma,
                dma((3,)), dma((3,)), dma((2,)), dma, dma, dma, dma, dma, dma,
            ],
            compiler_params=pltpu.CompilerParams(collective_id=1, has_side_effects=True, vmem_limit_bytes=62 << 20),
        )(o, dq, dkv, wo2, w_q, wk2, wv2)
        return y, dx

    return jax.shard_map(local_layer, mesh=mesh,
                         in_specs=(row_spec, row_spec, row_spec, full_spec, full_spec, full_spec, full_spec),
                         out_specs=(row_spec, row_spec), check_vma=False)
```

```python
import functools

import jax
import jax.numpy as jnp
from jax import lax
from jax.experimental import pallas as pl
from jax.experimental.pallas import tpu as pltpu
from jax.sharding import PartitionSpec as P

MESH = pl.DeviceIdType.MESH
NEG_BIG = -1.0e30
LOG2E = 1.4426950408889634
F32, BF16 = jnp.float32, jnp.bfloat16
NT = (((1,), (1,)), ((), ()))
NN = (((1,), (0,)), ((), ()))
DOC_VALUES = 9


def dot(a, b, dims=NN):
    return lax.dot_general(a, b, dims, preferred_element_type=F32)


def remote(src, dst, send, recv, dev):
    return pltpu.make_async_remote_copy(src_ref=src, dst_ref=dst, send_sem=send, recv_sem=recv,
                                        device_id={'cp': dev}, device_id_type=MESH)


def ring_ids(chips):
    me = lax.axis_index('cp')
    core, chip = lax.rem(me, 2), me // 2
    return core, chip, chip * 2 + 1 - core, lax.rem(chip + 1, chips) * 2 + core, lax.rem(chip + chips - 1, chips) * 2 + core


def entry_barrier(devs):
    barrier = pltpu.get_barrier_semaphore()
    for dev in devs:
        pl.semaphore_signal(barrier, inc=1, device_id={'cp': dev}, device_id_type=MESH)
    pl.semaphore_wait(barrier, len(devs))


TILE = 256
PER = 8


def sort_matrix():
    toks = TILE // PER
    r = lax.broadcasted_iota(jnp.int32, (TILE, TILE), 0)
    c = lax.broadcasted_iota(jnp.int32, (TILE, TILE), 1)
    t = r & (toks - 1)
    return jnp.where(c == t * PER + lax.shift_right_logical(r, toks.bit_length() - 1), 1.0, 0.0).astype(BF16)


def split_heads(order, src, dst, count, n_head, head):
    toks = TILE // PER
    for h0 in range(0, n_head, PER):
        for t0 in range(0, count, 4 * toks):
            side = [src[t0 + k * toks:t0 + (k + 1) * toks, h0:h0 + PER, :].reshape(TILE, head) for k in range(4)]
            rows = dot(order, jnp.concatenate(side, axis=1)).astype(BF16)
            for k in range(4):
                for g in range(PER):
                    dst[t0 + k * toks:t0 + (k + 1) * toks, (h0 + g) * head:(h0 + g + 1) * head] = rows[g * toks:(g + 1) * toks, k * head:(k + 1) * head]


def proj_kernel(chips, x, dy, meta, wq, wk, wv, wo, q_o, do_o, kv_o, md_o,
                xb, dyb, mb, kvb, wkb, wvb, wqb, wob, wr, order, pick, wkv, acc, kvacc,
                loc, wksem, wqsem, wosem, xs, xr, ys, yr, ms, mr, gs, gr, osem):
    half = x.shape[0] // 2
    d_model = x.shape[1]
    tok = 2 * half
    pieces = 2 * chips
    n_ch = xs.shape[1]
    cw = d_model // n_ch
    core, chip, partner, up, down = ring_ids(chips)
    row_off = (pl.multiple_of(half * core, half), pl.multiple_of(3 * half - half * core, half))
    n_q, qd = d_model // wqb.shape[1], wqb.shape[1]
    group = wqb.shape[2]
    head = wqb.shape[3]
    n_o = group * head // wob.shape[1]

    def wq_copy(i, slot):
        return pltpu.make_async_copy(wq.at[pl.ds(i * qd, qd), core], wqb.at[slot], wqsem.at[slot])

    def wo_copy(i, slot):
        rows, kw = wob.shape[1], wob.shape[2]
        n, k = i // (d_model // kw), i % (d_model // kw)
        return pltpu.make_async_copy(wo.at[pl.ds(core * group * head + n * rows, rows), pl.ds(k * kw, kw)], wob.at[slot], wosem.at[slot])

    wk_copies = []
    for ch in range(n_ch):
        rows = pl.ds(ch * 2 * cw, 2 * cw)
        wk_copies.append((pltpu.make_async_copy(wk.at[rows], wkb.at[rows], wksem.at[0, ch]),
                          pltpu.make_async_copy(wv.at[rows], wvb.at[rows], wksem.at[1, ch])))
    x_loc, y_loc, x_rem, y_rem = [], [], [], []
    for ch in range(n_ch):
        cols = pl.ds(ch * cw, cw)
        for pc in range(2):
            src = pl.ds(half * pc, half)
            dst = pl.ds(row_off[pc], half)
            x_loc.append(pltpu.make_async_copy(x.at[src, cols], xb.at[dst, cols], loc.at[0, pc, ch]))
            y_loc.append(pltpu.make_async_copy(dy.at[src, cols], dyb.at[dst, cols], loc.at[1, pc, ch]))
            x_rem.append(remote(x.at[src, cols], xb.at[dst, cols], xs.at[pc, ch], xr.at[pc, ch], partner))
            y_rem.append(remote(dy.at[src, cols], dyb.at[dst, cols], ys.at[pc, ch], yr.at[pc, ch], partner))
    m_loc = pltpu.make_async_copy(meta, mb.at[0], osem.at[0])
    m_rem = remote(meta, mb.at[1], ms, mr, partner)

    for ch in range(n_ch):
        x_loc[2 * ch].start()
        x_loc[2 * ch + 1].start()
        wk_copies[ch][0].start()
        wk_copies[ch][1].start()
    m_loc.start()
    for s in range(wqb.shape[0]):
        wq_copy(s, s).start()
    entry_barrier((partner, up, down))
    for c in x_rem:
        c.start()
    m_rem.start()

    r = lax.broadcasted_iota(jnp.int32, pick.shape, 0)
    pick[...] = jnp.where(lax.broadcasted_iota(jnp.int32, pick.shape, 1) == 2 * r + core, 1.0, 0.0).astype(BF16)
    order[...] = sort_matrix()
    n_sub = TILE // 2
    for ch in range(n_ch):
        for c in wk_copies[ch]:
            c.wait()
        for j in range(ch * cw // n_sub, (ch + 1) * cw // n_sub, 2):
            side = [buf[t * 2 * n_sub:(t + 1) * 2 * n_sub, :] for t in (j, j + 1) for buf in (wkb, wvb)]
            rows = dot(pick[...], jnp.concatenate(side, axis=1)).astype(BF16)
            wkv[j * n_sub:(j + 1) * n_sub, :] = rows[:, :2 * head]
            wkv[(j + 1) * n_sub:(j + 2) * n_sub, :] = rows[:, 2 * head:]
    quarters = 2
    qs = qd // quarters

    def split_part(slot, dst, k):
        split_heads(order[...], wqb.at[slot, k * qs:(k + 1) * qs], dst.at[k * qs:(k + 1) * qs], qs, group, head)

    n_slot = wqb.shape[0]

    def sort_block(i):
        slot = lax.rem(i, n_slot)
        wq_copy(i, slot).wait()
        for k in range(quarters):
            split_part(slot, wr.at[i], k)

        @pl.when(i + n_slot < n_q)
        def _():
            wq_copy(i + n_slot, slot).start()

    early = n_q // 2
    pl.loop(0, early)(sort_block)
    for ch in range(n_ch):
        for c in (x_loc[2 * ch], x_loc[2 * ch + 1]):
            c.wait()
        for c in (x_rem[2 * ch], x_rem[2 * ch + 1]):
            c.wait_recv()
        hc = cw // 2
        for k in range(2):
            part_sum = dot(xb[:, ch * cw + k * hc:ch * cw + (k + 1) * hc], wkv[ch * cw + k * hc:ch * cw + (k + 1) * hc])
            if ch == 0:
                kvacc[k] = part_sum
            else:
                kvacc[k] += part_sum
    m_loc.wait()
    m_rem.wait_recv()
    lo, hi = chip, pieces - 1 - chip
    width = md_o.shape[2]
    for pc, idx in ((0, lo), (1, hi)):
        both = (mb[0, pc].astype(F32) + mb[1, pc].astype(F32)).astype(BF16)
        md_o[pc] = both[:, :width]
        kvb[idx, 2 * tok:2 * tok + 16] = both[:, width:]
        kv_sum = (kvacc[0, pc * tok:(pc + 1) * tok, :] + kvacc[1, pc * tok:(pc + 1) * tok, :]).astype(BF16)
        kvb[idx, 0:tok] = kv_sum[:, 0:head]
        kvb[idx, tok:2 * tok] = kv_sum[:, head:]

    last = chips // 2 - 1

    def hop(direction, t, pc):
        src = lax.rem(chip + (chips - t if direction == 0 else t), chips)
        idx = src if pc == 0 else pieces - 1 - src
        return remote(kvb.at[idx], kvb.at[idx], gs.at[direction, t, pc], gr.at[direction, t, pc], up if direction == 0 else down)

    def arrived(direction, t, pc):
        src = lax.rem(chip + (chips - t - 1 if direction == 0 else t + 1), chips)
        idx = src if pc == 0 else pieces - 1 - src
        remote(kvb.at[idx], kvb.at[idx], gs.at[direction, t, pc], gr.at[direction, t, pc], up).wait_recv()

    moves = [[(d, pc) for pc in range(2) for d in range(2) if t < last or d == pc] for t in range(last + 1)]

    def advance(t, only=None):
        for d, pc in moves[t - 1]:
            if only is None or pc == only:
                arrived(d, t - 1, pc)
                if t <= last and (d, pc) in moves[t]:
                    hop(d, t, pc).start()

    for d, pc in moves[0]:
        hop(d, 0, pc).start()

    for c in y_rem:
        c.start()
    for c in y_loc:
        c.start()
    for k in range(wob.shape[0]):
        wo_copy(k, k).start()

    pl.loop(early, n_q)(sort_block)
    acc[...] = jnp.zeros_like(acc)

    @pl.loop(0, n_q)
    def _(i):
        acc[...] += dot(xb[:, pl.ds(pl.multiple_of(i * qd, qd), qd)], wr[i])

        for at, step in ((1, (1, 0)), (3, (1, 1)), (5, (2, 0)), (7, (2, 1))):
            @pl.when(i == at)
            def _():
                advance(*step)

    for g in range(group):
        for pc in range(2):
            q_o[pc, g * tok:(g + 1) * tok, :] = acc[pc * tok:(pc + 1) * tok, g * head:(g + 1) * head].astype(BF16)

    for c in y_loc:
        c.wait()
    for c in y_rem:
        c.wait_recv()

    plan = {2: (3, 0), 4: (3, 1)}
    wide = wob.shape[1] // head
    kw = wob.shape[2]
    n_k = d_model // kw
    for u in range(n_o * n_k):
        n, k = u // n_k, u % n_k
        slot = u % wob.shape[0]
        wo_copy(u, slot).wait()
        part = dot(dyb[:, k * kw:(k + 1) * kw], wob[slot], NT)
        if k == 0:
            acc[:, 0:wide * head] = part
        else:
            acc[:, 0:wide * head] += part
        if u + wob.shape[0] < n_o * n_k:
            wo_copy(u + wob.shape[0], slot).start()
        if k == n_k - 1:
            for g in range(wide):
                for pc in range(2):
                    do_o[pc, (n * wide + g) * tok:(n * wide + g + 1) * tok, :] = acc[pc * tok:(pc + 1) * tok, g * head:(g + 1) * head].astype(BF16)
        if u in plan:
            advance(*plan[u])
    for t in range(4, last + 2):
        advance(t)
    out = pltpu.make_async_copy(kvb, kv_o, osem.at[0])
    out.start()
    for c in x_rem + y_rem + [m_rem]:
        c.wait_send()
    for t in range(last + 1):
        for d, pc in moves[t]:
            hop(d, t, pc).wait_send()
    out.wait()


def attn_kernel(chips, scale, q, do, kv, md, o_ref, dq_ref, dkv, s_scr, p_scr, acc_t, row_scr, m_ref, l_ref):
    pieces = 2 * chips
    tok = kv.shape[1] // 2 - 8
    head = kv.shape[2]
    lanes_all = q.shape[1]
    group = lanes_all // tok
    lw = 256
    lanes = [slice(a, a + lw) for a in range(0, lanes_all, lw)]
    chip = lax.axis_index('cp') // 2
    dkv[...] = jnp.zeros_like(dkv)
    lane = lax.broadcasted_iota(jnp.int32, (1, lanes_all), 1)
    for g in range(1, group):
        lane = jnp.where(lane >= tok, lane - tok, lane)
    q_off = lane.astype(F32)
    tot = lax.fori_loop(0, pieces, lambda j, a: a + kv[j, 2 * tok:2 * tok + 16].astype(F32), jnp.zeros((16, head), F32))[0:1]

    @pl.loop(0, 2)
    def _(pc):
        place = jnp.where(pc == 0, chip, pieces - 1 - chip)
        doc_q = md[pc].astype(F32)[0:1]
        start = jnp.zeros((1, lanes_all), F32)
        for v in range(1, DOC_VALUES):
            start = jnp.where(doc_q == float(v), tot[:, v:v + 1], start)
        first = jnp.min(start).astype(jnp.int32) // tok
        pos = q_off + (place * tok).astype(F32)
        n_pair = (place - first + 2) // 2
        m_ref[...] = jnp.full_like(m_ref, NEG_BIG)
        l_ref[...] = jnp.zeros_like(l_ref)

        def rows_of(t, base):
            kb = place - 2 * t
            return jnp.concatenate([kv[jnp.maximum(kb - 1, 0), base:base + tok], kv[kb, base:base + tok]], axis=0)

        def add_rows(t, base, val):
            kb = place - 2 * t
            dkv[kb, base:base + tok] += val[tok:]
            dkv[jnp.maximum(kb - 1, 0), base:base + tok] += val[:tok]

        def score(t, masked):
            keys = rows_of(t, 0)
            u = (lax.broadcasted_iota(jnp.int32, (2 * tok, lw), 0) + (place - 2 * t - 1) * tok).astype(F32)
            scales = []
            for ln in lanes:
                m_old = m_ref[:, ln]
                m_new = m_old
                for a in (0, tok):
                    s = dot(keys[a:a + tok], q[pc, ln], NT) * (scale * LOG2E)
                    if masked:
                        s = jnp.where((u[a:a + tok] >= start[:, ln]) & (u[a:a + tok] <= pos[:, ln]), s, NEG_BIG)
                    s_scr[t, a:a + tok, ln] = s
                    m_new = jnp.maximum(m_new, jnp.max(s, axis=0, keepdims=True))
                m_ref[:, ln] = m_new
                scales.append((m_new, jnp.exp2(m_old - m_new)))
            for ln, (m_new, shrink) in zip(lanes, scales):
                l_ref[:, ln] = l_ref[:, ln] * shrink + jnp.sum(jnp.exp2(s_scr[t, :, ln] - m_new), axis=0, keepdims=True)

        last_start = (jnp.max(start).astype(jnp.int32) + tok - 1) // tok
        n_full = jnp.maximum((place - last_start - 1) // 2, 0)

        @pl.loop(0, n_pair)
        def _(t):
            inside = (t >= 1) & (t <= n_full)

            @pl.when(inside)
            def _():
                score(t, False)

            @pl.when(jnp.logical_not(inside))
            def _():
                score(t, True)

        log_norm = m_ref[...] + jnp.log2(l_ref[...])
        acc_t[...] = jnp.zeros_like(acc_t)

        @pl.loop(0, n_pair)
        def _(t):
            v_t = rows_of(t, tok).astype(F32).T.astype(BF16)
            dv = jnp.zeros((2 * tok, head), F32)
            for ln in lanes:
                p = jnp.exp2(s_scr[t, :, ln] - log_norm[:, ln]).astype(BF16)
                p_scr[t, :, ln] = p
                acc_t[:, ln] += dot(v_t, p)
                dv = dv + dot(p, do[pc, ln])
            add_rows(t, tok, dv)

        for ln in lanes:
            o_bf = acc_t[:, ln].astype(BF16).astype(F32)
            do_t = do[pc, ln].astype(F32).T
            l_ref[:, ln] = jnp.sum(do_t * o_bf, axis=0, keepdims=True)
            row_scr[ln, :] = o_bf.T.astype(BF16)
        out_rows = pl.ds(pl.multiple_of(pc * tok, tok), tok)
        for g in range(group):
            o_ref[out_rows, g * head:(g + 1) * head] = row_scr[g * tok:(g + 1) * tok, :]
        acc_t[...] = jnp.zeros_like(acc_t)

        @pl.loop(0, n_pair)
        def _(t):
            vals = rows_of(t, tok)
            k_t = rows_of(t, 0).astype(F32).T.astype(BF16)
            dk = jnp.zeros((2 * tok, head), F32)
            nxt = dot(vals, do[pc, lanes[0]], NT)
            for i, ln in enumerate(lanes):
                dp = nxt
                if i + 1 < len(lanes):
                    nxt = dot(vals, do[pc, lanes[i + 1]], NT)
                ds = (p_scr[t, :, ln].astype(F32) * (dp - l_ref[:, ln])).astype(BF16)
                acc_t[:, ln] += dot(k_t, ds)
                dk = dk + dot(ds, q[pc, ln])
            add_rows(t, 0, dk * scale)

        for ln in lanes:
            row_scr[ln, :] = (acc_t[:, ln] * scale).T.astype(BF16)
        for g in range(group):
            dq_ref[out_rows, g * head:(g + 1) * head] = row_scr[g * tok:(g + 1) * tok, :]


def out_kernel(chips, o, dq, dkv, wo, wq, wk, wv, y, dx,
               ob, dqb, own, ring, fin, a2, b2, wob, wqb, wkb, scr, wr, order, dacc, yb, xo,
               loc, ex_s, ex_r, rs, rr, fs, fr, wosem, wqsem, wksem, ysem, xsem, ys, yr, xs, xr):
    tok = own.shape[1] // 2
    head = own.shape[2]
    half = tok // 2
    pieces = 2 * chips
    d_half = yb.shape[1]
    core, chip, partner, up, down = ring_ids(chips)
    mine = (pl.multiple_of(half * core, half), pl.multiple_of(3 * half - half * core, half))
    theirs = (pl.multiple_of(half - half * core, half), pl.multiple_of(2 * half + half * core, half))
    hw = o.shape[1]
    col0 = pl.multiple_of(core * d_half, d_half)
    bw = wob.shape[2]
    n_y = d_half // bw
    qd = wqb.shape[1]
    n_x = d_half // qd
    n_head = wqb.shape[2]
    kc = scr.shape[0] // 2

    def wo_copy(i, slot):
        return pltpu.make_async_copy(wo.at[:, pl.ds(pl.multiple_of(col0 + i * bw, bw), bw)], wob.at[slot], wosem.at[slot])

    def wq_copy(i, slot):
        rows = wqb.shape[1]
        return pltpu.make_async_copy(wq.at[pl.ds(pl.multiple_of(col0 + i * rows, rows), rows)], wqb.at[slot], wqsem.at[slot])

    rows = pl.ds(pl.multiple_of(col0 * 2, 2 * d_half), 2 * d_half)
    wk_copies = [pltpu.make_async_copy(w.at[rows], wkb.at[k], wksem.at[k]) for k, w in enumerate((wk, wv))]
    ocols = pl.ds(pl.multiple_of(core * hw, hw), hw)
    l_own = pltpu.make_async_copy(dkv, own, loc.at[0])
    l_o = pltpu.make_async_copy(o, ob.at[:, ocols], loc.at[1])
    l_dq = pltpu.make_async_copy(dq, dqb.at[:, ocols], loc.at[2])
    r_o = remote(o, ob.at[:, ocols], ex_s.at[0], ex_r.at[0], partner)
    r_dq = remote(dq, dqb.at[:, ocols], ex_s.at[1], ex_r.at[1], partner)

    l_own.start()
    l_o.start()
    l_dq.start()
    for s in range(wob.shape[0]):
        wo_copy(s, s).start()
    entry_barrier((partner, up, down))
    r_o.start()
    r_dq.start()
    for s in range(wqb.shape[0]):
        wq_copy(s, s).start()
    for c in wk_copies:
        c.start()

    steps = chips - 1

    def owner(direction, s):
        chip_w = lax.rem(chip + (2 * chips - 1 - s if direction == 0 else 1 + s), chips)
        return chip_w if direction == 0 else pieces - 1 - chip_w

    def part_rows(row):
        return pl.ds(row, tok)

    def send(direction, s, kvp):
        src = own.at[owner(direction, 0), part_rows(kvp * tok)] if s == 0 else ring.at[direction, s - 1, kvp]
        return remote(src, ring.at[direction, s, kvp], rs.at[direction, s, kvp], rr.at[direction, s, kvp], up if direction == 0 else down)

    def event(e):
        s, kvp = e // 2 + 1, lax.rem(e, 2)
        for d in range(2):
            remote(ring.at[d, s - 1, kvp], ring.at[d, s - 1, kvp], rs.at[d, s - 1, kvp], rr.at[d, s - 1, kvp], up).wait_recv()
            ring[d, s - 1, kvp] = ring[d, s - 1, kvp] + own[owner(d, s), part_rows(pl.multiple_of(kvp * tok, tok))]

        @pl.when(s < steps)
        def _():
            for d in range(2):
                remote(ring.at[d, s - 1, kvp], ring.at[d, s, kvp], rs.at[d, s, kvp], rr.at[d, s, kvp], up if d == 0 else down).start()

    l_own.wait()
    for kvp in range(2):
        for d in range(2):
            send(d, 0, kvp).start()

    def out_copies(buf, dst, i, width, lsem, ssem, rsem):
        cols = pl.ds(pl.multiple_of(col0 + i * width, width), width)
        bc = pl.ds(pl.multiple_of(i * width, width), width)
        for pc in range(2):
            pltpu.make_async_copy(buf.at[pl.ds(mine[pc], half), bc], dst.at[pl.ds(half * pc, half), cols], lsem).start()
            remote(buf.at[pl.ds(theirs[pc], half), bc], dst.at[pl.ds(half * pc, half), cols], ssem, rsem, partner).start()

    l_o.wait()
    r_o.wait_recv()
    ns = wob.shape[0]

    @pl.loop(0, n_y)
    def _(i):
        slot = lax.rem(i, ns)
        wo_copy(i, slot).wait()
        yb[:, pl.ds(pl.multiple_of(i * bw, bw), bw)] = dot(ob[...], wob[slot]).astype(BF16)

        @pl.when(i + ns < n_y)
        def _():
            wo_copy(i + ns, slot).start()

        @pl.when(i > 0)
        def _():
            out_copies(yb, y, i - 1, bw, ysem, ys, yr)

        @pl.when((i >= 3) & (lax.rem(i, 2) == 1))
        def _():
            event((i - 3) // 2)

    out_copies(yb, y, n_y - 1, bw, ysem, ys, yr)

    l_dq.wait()
    r_dq.wait_recv()
    nq = wqb.shape[0]
    quarters = 2
    qs = qd // quarters
    order[...] = sort_matrix()

    def split_part(slot, dst, k):
        split_heads(order[...], wqb.at[slot, k * qs:(k + 1) * qs], dst.at[k * qs:(k + 1) * qs], qs, n_head, head)

    wq_copy(0, 0).wait()
    for k in range(quarters):
        split_part(0, wr.at[0], k)
    wq_copy(nq, 0).start()

    def x_step(i, cur, nxt):
        slot = lax.rem(i + 1, nq)

        @pl.when(i + 1 < n_x)
        def _():
            wq_copy(i + 1, slot).wait()

        dacc[:, pl.ds(pl.multiple_of(i * qd, qd), qd)] = dot(dqb[...], cur[...], NT)
        for k in range(quarters):
            split_part(slot, nxt, k)

        @pl.when(i + 1 + nq < n_x)
        def _():
            wq_copy(i + 1 + nq, slot).start()

    @pl.loop(0, n_x // 2)
    def _(h):
        x_step(2 * h, wr.at[0], wr.at[1])
        event(3 + 2 * h)
        x_step(2 * h + 1, wr.at[1], wr.at[0])
        event(4 + 2 * h)

    for c in wk_copies:
        c.wait()
    n_e = 2 * steps
    first_e = 3 + n_x

    @pl.loop(first_e, n_e - 1)
    def _(e):
        @pl.when(e < first_e + 2)
        def _():
            j = e - first_e
            rows_b = d_half // 2
            piece = kc // 2
            for k in range(2):
                for m in range(rows_b // piece):
                    r0 = pl.multiple_of(j * rows_b + m * piece, piece)
                    scr[k * kc:(k + 1) * kc, :] = wkb[k, pl.ds(2 * r0, kc), :].astype(F32)
                    for h in range(2):
                        b2[pl.ds(r0, piece), (2 * k + h) * head:(2 * k + h + 1) * head] = scr[pl.ds(k * kc + h, piece, stride=2), :].astype(BF16)

        event(e)

    r_fin = [remote(fin.at[kvp], a2.at[core, kvp], fs.at[kvp], fr.at[kvp], partner) for kvp in range(2)]
    for kvp in range(2):
        if kvp == 1:
            event(n_e - 1)
        for d in range(2):
            fin[kvp, d * tok:(d + 1) * tok] = ring[d, steps - 1, kvp].astype(BF16)
        r_fin[kvp].start()
        a2[core, kvp] = fin[kvp]
        r_fin[kvp].wait_recv()
        a_all = jnp.concatenate([a2[0, kvp], a2[1, kvp]], axis=1)
        for i in range(n_y):
            cs = slice(i * bw, (i + 1) * bw)
            part = dacc[:, cs] + dot(a_all, b2[cs, 2 * kvp * head:2 * (kvp + 1) * head], NT)
            if kvp == 0:
                dacc[:, cs] = part
            else:
                xo[:, cs] = part.astype(BF16)
                if i > 0:
                    out_copies(xo, dx, i - 1, bw, xsem, xs, xr)
    out_copies(xo, dx, n_y - 1, bw, xsem, xs, xr)

    for c in (r_o, r_dq, *r_fin):
        c.wait_send()
    for s in range(steps):
        for kvp in range(2):
            for d in range(2):
                send(d, s, kvp).wait_send()
    for buf, dst, lsem, ssem, rsem in ((yb, y, ysem, ys, yr), (xo, dx, xsem, xs, xr)):
        cols = pl.ds(col0, d_half)
        pltpu.make_async_copy(buf.at[pl.ds(0, tok)], dst.at[:, cols], lsem).wait()
        both = remote(buf.at[pl.ds(0, tok)], dst.at[:, cols], ssem, rsem, partner)
        both.wait_send()
        both.wait_recv()


def solution(mesh):
    group_devs = mesh.shape['cp']
    chips = group_devs // 2
    row_spec = P(('dp', 'cp'))
    full_spec = P()
    any_spec = pl.BlockSpec(memory_space=pl.ANY)
    vmem_spec = pl.BlockSpec(memory_space=pltpu.VMEM)
    dma = pltpu.SemaphoreType.DMA

    def local_layer(x_in, dy_in, doc_id, w_q, w_k, w_v, w_o):
        tok, d_model = x_in.shape
        q_heads, head = w_q.shape[1], w_q.shape[2]
        kv_heads = w_k.shape[1]
        group = q_heads // kv_heads
        half = tok // 2
        rows2 = 2 * tok
        pieces = 2 * chips
        lanes = group * tok
        d_half = d_model // 2
        scale = head ** -0.5
        core = lax.axis_index('cp') % 2
        docs = doc_id.reshape(2, half)
        slot = jnp.stack([core, 1 - core])[:, None]
        lane = jnp.arange(tok)
        docf = jnp.concatenate([docs, docs], axis=1).astype(F32)
        docf = jnp.where((lane // half)[None, :] == slot, docf, 0.0)
        ids = jnp.tile(docf, (1, group))
        counts = jnp.sum((docs[:, :, None] < jnp.arange(head)[None, None, :]).astype(F32), axis=1)
        meta = jnp.concatenate([ids, counts], axis=1).astype(BF16)
        meta = jnp.broadcast_to(meta[:, None, :], (2, 16, lanes + head))

        wq4 = w_q.reshape(d_model, kv_heads, group, head)
        wk2 = w_k.reshape(d_model * kv_heads, head)
        wv2 = w_v.reshape(d_model * kv_heads, head)
        wo2 = w_o.reshape(q_heads * head, d_model)

        n_ch = 4
        cw = d_model // n_ch
        qd = d_model // 8
        hops = chips // 2
        kv_rows = 2 * tok + 16
        q, do, kv, md = pl.pallas_call(
            functools.partial(proj_kernel, chips),
            name='proj',
            out_shape=(jax.ShapeDtypeStruct((2, lanes, head), BF16), jax.ShapeDtypeStruct((2, lanes, head), BF16),
                       jax.ShapeDtypeStruct((pieces, kv_rows, head), BF16), jax.ShapeDtypeStruct((2, 16, lanes), BF16)),
            in_specs=[any_spec] * 7,
            out_specs=(vmem_spec, vmem_spec, any_spec, vmem_spec),
            scratch_shapes=[
                pltpu.VMEM((rows2, d_model), BF16), pltpu.VMEM((rows2, d_model), BF16), pltpu.VMEM((2, 2, 16, lanes + head), BF16),
                pltpu.VMEM((pieces, kv_rows, head), BF16),
                pltpu.VMEM((2 * d_model, head), BF16), pltpu.VMEM((2 * d_model, head), BF16),
                pltpu.VMEM((2, qd, group, head), BF16), pltpu.VMEM((3, 4 * head, d_model // 4), BF16),
                pltpu.VMEM((8, qd, group * head), BF16), pltpu.VMEM((TILE, TILE), BF16), pltpu.VMEM((TILE // 2, TILE), BF16), pltpu.VMEM((d_model, 2 * head), BF16),
                pltpu.VMEM((rows2, group * head), F32), pltpu.VMEM((2, rows2, 2 * head), F32),
                dma((2, 2, n_ch)), dma((2, n_ch)), dma((2,)), dma((3,)),
                dma((2, n_ch)), dma((2, n_ch)), dma((2, n_ch)), dma((2, n_ch)), dma, dma,
                dma((2, hops, 2)), dma((2, hops, 2)), dma((1,)),
            ],
            compiler_params=pltpu.CompilerParams(collective_id=0, has_side_effects=True, vmem_limit_bytes=63 << 20),
        )(x_in, dy_in, meta, wq4, wk2, wv2, wo2)

        o, dq, dkv = pl.pallas_call(
            functools.partial(attn_kernel, chips, scale),
            name='attn',
            out_shape=(jax.ShapeDtypeStruct((rows2, group * head), BF16), jax.ShapeDtypeStruct((rows2, group * head), BF16),
                       jax.ShapeDtypeStruct((pieces, 2 * tok, head), F32)),
            in_specs=[vmem_spec] * 4,
            out_specs=(vmem_spec,) * 3,
            scratch_shapes=[
                pltpu.VMEM((chips, rows2, lanes), F32), pltpu.VMEM((chips, rows2, lanes), BF16), pltpu.VMEM((head, lanes), F32),
                pltpu.VMEM((lanes, head), BF16), pltpu.VMEM((1, lanes), F32), pltpu.VMEM((1, lanes), F32),
            ],
            compiler_params=pltpu.CompilerParams(vmem_limit_bytes=60 << 20),
        )(q, do, kv, md)

        steps = chips - 1
        bw = d_half // 8
        y, dx = pl.pallas_call(
            functools.partial(out_kernel, chips),
            name='out',
            out_shape=(jax.ShapeDtypeStruct((tok, d_model), BF16), jax.ShapeDtypeStruct((tok, d_model), BF16)),
            in_specs=[any_spec] * 7,
            out_specs=(any_spec, any_spec),
            scratch_shapes=[
                pltpu.VMEM((rows2, q_heads * head), BF16), pltpu.VMEM((rows2, q_heads * head), BF16),
                pltpu.VMEM((pieces, 2 * tok, head), F32), pltpu.VMEM((2, steps, 2, tok, head), F32),
                pltpu.VMEM((2, rows2, head), BF16), pltpu.VMEM((2, 2, rows2, head), BF16), pltpu.VMEM((d_half, 4 * head), BF16),
                pltpu.VMEM((3, q_heads * head, bw), BF16), pltpu.VMEM((3, bw, q_heads, head), BF16),
                pltpu.VMEM((2, 2 * d_half, head), BF16),
                pltpu.VMEM((1024, head), F32), pltpu.VMEM((2, bw, q_heads * head), BF16), pltpu.VMEM((TILE, TILE), BF16),
                pltpu.VMEM((rows2, d_half), F32), pltpu.VMEM((rows2, d_half), BF16), pltpu.VMEM((rows2, d_half), BF16),
                dma((3,)), dma((2,)), dma((2,)), dma((2, steps, 2)), dma((2, steps, 2)), dma((2,)), dma((2,)),
                dma((3,)), dma((3,)), dma((2,)), dma, dma, dma, dma, dma, dma,
            ],
            compiler_params=pltpu.CompilerParams(collective_id=1, has_side_effects=True, vmem_limit_bytes=62 << 20),
        )(o, dq, dkv, wo2, w_q, wk2, wv2)
        return y, dx

    return jax.shard_map(local_layer, mesh=mesh,
                         in_specs=(row_spec, row_spec, row_spec, full_spec, full_spec, full_spec, full_spec),
                         out_specs=(row_spec, row_spec), check_vma=False)
```

```python
import functools

import jax
import jax.numpy as jnp
from jax import lax
from jax.experimental import pallas as pl
from jax.experimental.pallas import tpu as pltpu
from jax.sharding import PartitionSpec as P

MESH = pl.DeviceIdType.MESH
NEG_BIG = -1.0e30
LOG2E = 1.4426950408889634
F32, BF16 = jnp.float32, jnp.bfloat16
NT = (((1,), (1,)), ((), ()))
NN = (((1,), (0,)), ((), ()))
DOC_VALUES = 9


def dot(a, b, dims=NN):
    return lax.dot_general(a, b, dims, preferred_element_type=F32)


def remote(src, dst, send, recv, dev):
    return pltpu.make_async_remote_copy(src_ref=src, dst_ref=dst, send_sem=send, recv_sem=recv,
                                        device_id={'cp': dev}, device_id_type=MESH)


def ring_ids(chips):
    me = lax.axis_index('cp')
    core, chip = lax.rem(me, 2), me // 2
    return core, chip, chip * 2 + 1 - core, lax.rem(chip + 1, chips) * 2 + core, lax.rem(chip + chips - 1, chips) * 2 + core


def entry_barrier(devs):
    barrier = pltpu.get_barrier_semaphore()
    for dev in devs:
        pl.semaphore_signal(barrier, inc=1, device_id={'cp': dev}, device_id_type=MESH)
    pl.semaphore_wait(barrier, len(devs))


TILE = 256
PER = 8


def sort_matrix():
    toks = TILE // PER
    r = lax.broadcasted_iota(jnp.int32, (TILE, TILE), 0)
    c = lax.broadcasted_iota(jnp.int32, (TILE, TILE), 1)
    t = r & (toks - 1)
    return jnp.where(c == t * PER + lax.shift_right_logical(r, toks.bit_length() - 1), 1.0, 0.0).astype(BF16)


def split_heads(order, src, dst, count, n_head, head):
    toks = TILE // PER
    for h0 in range(0, n_head, PER):
        for t0 in range(0, count, 4 * toks):
            side = [src[t0 + k * toks:t0 + (k + 1) * toks, h0:h0 + PER, :].reshape(TILE, head) for k in range(4)]
            rows = dot(order, jnp.concatenate(side, axis=1)).astype(BF16)
            for k in range(4):
                for g in range(PER):
                    dst[t0 + k * toks:t0 + (k + 1) * toks, (h0 + g) * head:(h0 + g + 1) * head] = rows[g * toks:(g + 1) * toks, k * head:(k + 1) * head]


def proj_kernel(chips, x, dy, meta, wq, wk, wv, wo, q_o, do_o, kv_o, md_o,
                xb, dyb, mb, kvb, wkb, wvb, wqb, wob, wr, order, pick, wkv, acc, kvacc, kvx,
                loc, wksem, wqsem, wosem, xs, xr, ys, yr, ms, mr, ks, kr, gs, gr, osem):
    half = x.shape[0] // 2
    d_model = x.shape[1]
    tok = 2 * half
    pieces = 2 * chips
    n_ch = xs.shape[1]
    cw = d_model // n_ch
    core, chip, partner, up, down = ring_ids(chips)
    row_off = (pl.multiple_of(half * core, half), pl.multiple_of(3 * half - half * core, half))
    n_q, qd = d_model // wqb.shape[1], wqb.shape[1]
    group = wqb.shape[2]
    head = wqb.shape[3]
    n_o = group * head // wob.shape[1]

    def wq_copy(i, slot):
        return pltpu.make_async_copy(wq.at[pl.ds(i * qd, qd), core], wqb.at[slot], wqsem.at[slot])

    def wo_copy(i, slot):
        rows, kw = wob.shape[1], wob.shape[2]
        n, k = i // (d_model // kw), i % (d_model // kw)
        return pltpu.make_async_copy(wo.at[pl.ds(core * group * head + n * rows, rows), pl.ds(k * kw, kw)], wob.at[slot], wosem.at[slot])

    wk_copies = []
    for ch in range(n_ch):
        rows = pl.ds(ch * 2 * cw, 2 * cw)
        wk_copies.append((pltpu.make_async_copy(wk.at[rows], wkb.at[rows], wksem.at[0, ch]),
                          pltpu.make_async_copy(wv.at[rows], wvb.at[rows], wksem.at[1, ch])))
    x_loc, y_loc, x_rem, y_rem = [], [], [], []
    for ch in range(n_ch):
        cols = pl.ds(ch * cw, cw)
        for pc in range(2):
            src = pl.ds(half * pc, half)
            dst = pl.ds(row_off[pc], half)
            x_loc.append(pltpu.make_async_copy(x.at[src, cols], xb.at[dst, cols], loc.at[0, pc, ch]))
            y_loc.append(pltpu.make_async_copy(dy.at[src, cols], dyb.at[dst, cols], loc.at[1, pc, ch]))
            x_rem.append(remote(x.at[src, cols], xb.at[dst, cols], xs.at[pc, ch], xr.at[pc, ch], partner))
            y_rem.append(remote(dy.at[src, cols], dyb.at[dst, cols], ys.at[pc, ch], yr.at[pc, ch], partner))
    m_loc = pltpu.make_async_copy(meta, mb.at[0], osem.at[0])
    m_rem = remote(meta, mb.at[1], ms, mr, partner)

    for ch in range(n_ch):
        x_loc[2 * ch].start()
        x_loc[2 * ch + 1].start()
        wk_copies[ch][0].start()
        wk_copies[ch][1].start()
    m_loc.start()
    for s in range(wqb.shape[0]):
        wq_copy(s, s).start()
    entry_barrier((partner, up, down))
    m_rem.start()
    for c in x_rem[:n_ch]:
        c.start()

    n_sub = TILE // 2
    r = lax.broadcasted_iota(jnp.int32, pick.shape, 0)
    t = r & (n_sub - 1)
    pick[...] = jnp.where(lax.broadcasted_iota(jnp.int32, pick.shape, 1) == 2 * t + jnp.where(r >= n_sub, 1, 0), 1.0, 0.0).astype(BF16)
    order[...] = sort_matrix()
    for ch in range(n_ch):
        for c in wk_copies[ch]:
            c.wait()
        for j in range(cw // n_sub):
            src = slice((ch * cw + j * n_sub) * 2, (ch * cw + (j + 1) * n_sub) * 2)
            rows = dot(pick[...], jnp.concatenate([wkb[src, :], wvb[src, :]], axis=1)).astype(BF16)
            for h in range(2):
                wkv[j * n_sub:(j + 1) * n_sub, h * 2 * head:(h + 1) * 2 * head] = rows[h * n_sub:(h + 1) * n_sub]
        for c in (x_loc[2 * ch], x_loc[2 * ch + 1]):
            c.wait()
        part_sum = dot(jnp.concatenate([xb[pl.ds(row_off[pc], half), ch * cw:(ch + 1) * cw] for pc in range(2)], axis=0), wkv[...])
        if ch == 0:
            kvacc[...] = part_sum
        else:
            kvacc[...] += part_sum
    both_heads = [kvacc[:, h * 2 * head:(h + 1) * 2 * head] for h in range(2)]
    kvx[0] = jnp.where(core == 0, both_heads[1], both_heads[0]).astype(BF16)
    kvx[1] = jnp.where(core == 0, both_heads[0], both_heads[1]).astype(BF16)
    k_rem = remote(kvx.at[0], kvx.at[2], ks, kr, partner)
    k_rem.start()
    for c in x_rem[n_ch:]:
        c.start()
    m_loc.wait()
    m_rem.wait_recv()
    lo, hi = chip, pieces - 1 - chip
    width = md_o.shape[2]
    own_off = (pl.multiple_of(half * core, half), pl.multiple_of(half - half * core, half))
    for pc, idx in ((0, lo), (1, hi)):
        both = (mb[0, pc].astype(F32) + mb[1, pc].astype(F32)).astype(BF16)
        md_o[pc] = both[:, :width]
        kvb[idx, 2 * tok:2 * tok + 16] = both[:, width:]
        for k in range(2):
            kvb[idx, pl.ds(k * tok + own_off[pc], half)] = kvx[1, pc * half:(pc + 1) * half, k * head:(k + 1) * head]
    k_rem.wait_recv()
    for pc, idx in ((0, lo), (1, hi)):
        for k in range(2):
            kvb[idx, pl.ds(k * tok + own_off[1 - pc], half)] = kvx[2, pc * half:(pc + 1) * half, k * head:(k + 1) * head]

    last = chips // 2 - 1

    def hop(direction, t, pc):
        src = lax.rem(chip + (chips - t if direction == 0 else t), chips)
        idx = src if pc == 0 else pieces - 1 - src
        return remote(kvb.at[idx], kvb.at[idx], gs.at[direction, t, pc], gr.at[direction, t, pc], up if direction == 0 else down)

    def arrived(direction, t, pc):
        src = lax.rem(chip + (chips - t - 1 if direction == 0 else t + 1), chips)
        idx = src if pc == 0 else pieces - 1 - src
        remote(kvb.at[idx], kvb.at[idx], gs.at[direction, t, pc], gr.at[direction, t, pc], up).wait_recv()

    moves = [[(d, pc) for pc in range(2) for d in range(2) if t < last or d == pc] for t in range(last + 1)]

    def advance(t, only=None):
        for d, pc in moves[t - 1]:
            if only is None or pc == only:
                arrived(d, t - 1, pc)
                if t <= last and (d, pc) in moves[t]:
                    hop(d, t, pc).start()

    for d, pc in moves[0]:
        hop(d, 0, pc).start()

    for c in y_rem:
        c.start()
    for c in y_loc:
        c.start()
    for k in range(wob.shape[0]):
        wo_copy(k, k).start()
    quarters = 2
    qs = qd // quarters

    def split_part(slot, dst, k):
        split_heads(order[...], wqb.at[slot, k * qs:(k + 1) * qs], dst.at[k * qs:(k + 1) * qs], qs, group, head)

    wq_copy(0, 0).wait()
    for k in range(quarters):
        split_part(0, wr.at[0], k)
    wq_copy(wqb.shape[0], 0).start()

    acc[...] = jnp.zeros_like(acc)
    n_slot = wqb.shape[0]
    nw = group * head // quarters

    def q_step(i, cur, nxt):
        slot = lax.rem(i + 1, n_slot)

        @pl.when(i + 1 < n_q)
        def _():
            wq_copy(i + 1, slot).wait()

        lhs = xb.at[:, pl.ds(pl.multiple_of(i * qd, qd), qd)]
        for k in range(quarters):
            cols = slice(k * nw, (k + 1) * nw)
            acc[:, cols] += dot(lhs[...], cur[:, cols])
            split_part(slot, nxt, k)

        @pl.when(i + 1 + n_slot < n_q)
        def _():
            wq_copy(i + 1 + n_slot, slot).start()

    plan = {1: (1, 0), 3: (1, 1), 4: (2, 0), 6: (2, 1), 7: (3, 0)}

    @pl.loop(0, n_q // 2)
    def _(h):
        cols = pl.ds(pl.multiple_of(h * 2 * qd, 2 * qd), 2 * qd)
        for pc in range(2):
            rows = xb.at[pl.ds(row_off[pc], half), cols]
            remote(rows, rows, xs.at[pc, h], xr.at[pc, h], partner).wait_recv()
        for k in range(2):
            q_step(2 * h + k, wr.at[k], wr.at[1 - k])
            for at, step in plan.items():
                if at % 2 == k:
                    @pl.when(h == at // 2)
                    def _():
                        advance(*step)

    for g in range(group):
        for pc in range(2):
            q_o[pc, g * tok:(g + 1) * tok, :] = acc[pc * tok:(pc + 1) * tok, g * head:(g + 1) * head].astype(BF16)

    for c in y_loc:
        c.wait()
    for c in y_rem:
        c.wait_recv()

    wide = wob.shape[1] // head
    kw = wob.shape[2]
    n_k = d_model // kw
    for u in range(n_o * n_k):
        n, k = u // n_k, u % n_k
        slot = u % wob.shape[0]
        wo_copy(u, slot).wait()
        part = dot(dyb[:, k * kw:(k + 1) * kw], wob[slot], NT)
        if k == 0:
            acc[:, 0:wide * head] = part
        else:
            acc[:, 0:wide * head] += part
        if u + wob.shape[0] < n_o * n_k:
            wo_copy(u + wob.shape[0], slot).start()
        if k == n_k - 1:
            for g in range(wide):
                for pc in range(2):
                    do_o[pc, (n * wide + g) * tok:(n * wide + g + 1) * tok, :] = acc[pc * tok:(pc + 1) * tok, g * head:(g + 1) * head].astype(BF16)
        if u == 0:
            advance(3, 1)
    for t in range(4, last + 2):
        advance(t)
    out = pltpu.make_async_copy(kvb, kv_o, osem.at[0])
    out.start()
    for c in x_rem + y_rem + [m_rem, k_rem]:
        c.wait_send()
    for t in range(last + 1):
        for d, pc in moves[t]:
            hop(d, t, pc).wait_send()
    out.wait()


def attn_kernel(chips, scale, q, do, kv, md, o_ref, dq_ref, dkv, s_scr, p_scr, acc_t, row_scr, m_ref, l_ref):
    pieces = 2 * chips
    tok = kv.shape[1] // 2 - 8
    head = kv.shape[2]
    lanes_all = q.shape[1]
    group = lanes_all // tok
    lw = 256
    lanes = [slice(a, a + lw) for a in range(0, lanes_all, lw)]
    chip = lax.axis_index('cp') // 2
    dkv[...] = jnp.zeros_like(dkv)
    lane = lax.broadcasted_iota(jnp.int32, (1, lanes_all), 1)
    for g in range(1, group):
        lane = jnp.where(lane >= tok, lane - tok, lane)
    q_off = lane.astype(F32)
    tot = lax.fori_loop(0, pieces, lambda j, a: a + kv[j, 2 * tok:2 * tok + 16].astype(F32), jnp.zeros((16, head), F32))[0:1]

    @pl.loop(0, 2)
    def _(pc):
        place = jnp.where(pc == 0, chip, pieces - 1 - chip)
        doc_q = md[pc].astype(F32)[0:1]
        start = jnp.zeros((1, lanes_all), F32)
        for v in range(1, DOC_VALUES):
            start = jnp.where(doc_q == float(v), tot[:, v:v + 1], start)
        first = jnp.min(start).astype(jnp.int32) // tok
        pos = q_off + (place * tok).astype(F32)
        n_pair = (place - first + 2) // 2
        m_ref[...] = jnp.full_like(m_ref, NEG_BIG)
        l_ref[...] = jnp.zeros_like(l_ref)

        def rows_of(t, base):
            kb = place - 2 * t
            return jnp.concatenate([kv[jnp.maximum(kb - 1, 0), base:base + tok], kv[kb, base:base + tok]], axis=0)

        def add_rows(t, base, val):
            kb = place - 2 * t
            dkv[kb, base:base + tok] += val[tok:]
            dkv[jnp.maximum(kb - 1, 0), base:base + tok] += val[:tok]

        def score(t, masked):
            keys = rows_of(t, 0)
            u = (lax.broadcasted_iota(jnp.int32, (2 * tok, lw), 0) + (place - 2 * t - 1) * tok).astype(F32)
            scales = []
            for ln in lanes:
                s = dot(keys, q[pc, ln], NT) * (scale * LOG2E)
                if masked:
                    s = jnp.where((u >= start[:, ln]) & (u <= pos[:, ln]), s, NEG_BIG)
                s_scr[t, :, ln] = s
                m_old = m_ref[:, ln]
                m_new = jnp.maximum(m_old, jnp.max(s, axis=0, keepdims=True))
                m_ref[:, ln] = m_new
                scales.append((m_new, jnp.exp2(m_old - m_new)))
            for ln, (m_new, shrink) in zip(lanes, scales):
                l_ref[:, ln] = l_ref[:, ln] * shrink + jnp.sum(jnp.exp2(s_scr[t, :, ln] - m_new), axis=0, keepdims=True)

        last_start = (jnp.max(start).astype(jnp.int32) + tok - 1) // tok
        n_full = jnp.maximum((place - last_start - 1) // 2, 0)

        @pl.loop(0, n_pair)
        def _(t):
            inside = (t >= 1) & (t <= n_full)

            @pl.when(inside)
            def _():
                score(t, False)

            @pl.when(jnp.logical_not(inside))
            def _():
                score(t, True)

        log_norm = m_ref[...] + jnp.log2(l_ref[...])
        acc_t[...] = jnp.zeros_like(acc_t)

        @pl.loop(0, n_pair)
        def _(t):
            v_t = rows_of(t, tok).astype(F32).T.astype(BF16)
            dv = jnp.zeros((2 * tok, head), F32)
            for ln in lanes:
                p = jnp.exp2(s_scr[t, :, ln] - log_norm[:, ln]).astype(BF16)
                p_scr[t, :, ln] = p
                acc_t[:, ln] += dot(v_t, p)
                dv = dv + dot(p, do[pc, ln])
            add_rows(t, tok, dv)

        for ln in lanes:
            o_bf = acc_t[:, ln].astype(BF16).astype(F32)
            do_t = do[pc, ln].astype(F32).T
            l_ref[:, ln] = jnp.sum(do_t * o_bf, axis=0, keepdims=True)
            row_scr[ln, :] = o_bf.T.astype(BF16)
        out_rows = pl.ds(pl.multiple_of(pc * tok, tok), tok)
        for g in range(group):
            o_ref[out_rows, g * head:(g + 1) * head] = row_scr[g * tok:(g + 1) * tok, :]
        acc_t[...] = jnp.zeros_like(acc_t)

        @pl.loop(0, n_pair)
        def _(t):
            vals = rows_of(t, tok)
            k_t = rows_of(t, 0).astype(F32).T.astype(BF16)
            dk = jnp.zeros((2 * tok, head), F32)
            nxt = dot(vals, do[pc, lanes[0]], NT)
            for i, ln in enumerate(lanes):
                dp = nxt
                if i + 1 < len(lanes):
                    nxt = dot(vals, do[pc, lanes[i + 1]], NT)
                ds = (p_scr[t, :, ln].astype(F32) * (dp - l_ref[:, ln])).astype(BF16)
                acc_t[:, ln] += dot(k_t, ds)
                dk = dk + dot(ds, q[pc, ln])
            add_rows(t, 0, dk * scale)

        for ln in lanes:
            row_scr[ln, :] = (acc_t[:, ln] * scale).T.astype(BF16)
        for g in range(group):
            dq_ref[out_rows, g * head:(g + 1) * head] = row_scr[g * tok:(g + 1) * tok, :]


def out_kernel(chips, o, dq, dkv, wo, wq, wk, wv, y, dx,
               ob, dqb, own, ring, fin, a2, b2, wob, wqb, wkb, scr, wr, order, dacc, yb, xo,
               loc, ex_s, ex_r, rs, rr, fs, fr, wosem, wqsem, wksem, ysem, xsem, ys, yr, xs, xr):
    tok = own.shape[1] // 2
    head = own.shape[2]
    half = tok // 2
    pieces = 2 * chips
    d_half = yb.shape[1]
    core, chip, partner, up, down = ring_ids(chips)
    mine = (pl.multiple_of(half * core, half), pl.multiple_of(3 * half - half * core, half))
    theirs = (pl.multiple_of(half - half * core, half), pl.multiple_of(2 * half + half * core, half))
    hw = o.shape[1]
    col0 = pl.multiple_of(core * d_half, d_half)
    bw = wob.shape[2]
    n_y = d_half // bw
    qd = wqb.shape[1]
    n_x = d_half // qd
    n_head = wqb.shape[2]
    kc = scr.shape[0] // 2

    def wo_copy(i, slot):
        return pltpu.make_async_copy(wo.at[:, pl.ds(pl.multiple_of(col0 + i * bw, bw), bw)], wob.at[slot], wosem.at[slot])

    def wq_copy(i, slot):
        rows = wqb.shape[1]
        return pltpu.make_async_copy(wq.at[pl.ds(pl.multiple_of(col0 + i * rows, rows), rows)], wqb.at[slot], wqsem.at[slot])

    rows = pl.ds(pl.multiple_of(col0 * 2, 2 * d_half), 2 * d_half)
    wk_copies = [pltpu.make_async_copy(w.at[rows], wkb.at[k], wksem.at[k]) for k, w in enumerate((wk, wv))]
    ocols = pl.ds(pl.multiple_of(core * hw, hw), hw)
    l_own = pltpu.make_async_copy(dkv, own, loc.at[0])
    l_o = pltpu.make_async_copy(o, ob.at[:, ocols], loc.at[1])
    l_dq = pltpu.make_async_copy(dq, dqb.at[:, ocols], loc.at[2])
    r_o = remote(o, ob.at[:, ocols], ex_s.at[0], ex_r.at[0], partner)
    r_dq = remote(dq, dqb.at[:, ocols], ex_s.at[1], ex_r.at[1], partner)

    l_own.start()
    l_o.start()
    l_dq.start()
    for s in range(wob.shape[0]):
        wo_copy(s, s).start()
    entry_barrier((partner, up, down))
    r_o.start()
    r_dq.start()
    for s in range(wqb.shape[0]):
        wq_copy(s, s).start()
    for c in wk_copies:
        c.start()

    steps = chips - 1

    def owner(direction, s):
        chip_w = lax.rem(chip + (2 * chips - 1 - s if direction == 0 else 1 + s), chips)
        return chip_w if direction == 0 else pieces - 1 - chip_w

    def part_rows(row):
        return pl.ds(row, tok)

    def send(direction, s, kvp):
        src = own.at[owner(direction, 0), part_rows(kvp * tok)] if s == 0 else ring.at[direction, s - 1, kvp]
        return remote(src, ring.at[direction, s, kvp], rs.at[direction, s, kvp], rr.at[direction, s, kvp], up if direction == 0 else down)

    def event(e):
        s, kvp = e // 2 + 1, lax.rem(e, 2)
        for d in range(2):
            remote(ring.at[d, s - 1, kvp], ring.at[d, s - 1, kvp], rs.at[d, s - 1, kvp], rr.at[d, s - 1, kvp], up).wait_recv()
            ring[d, s - 1, kvp] = ring[d, s - 1, kvp] + own[owner(d, s), part_rows(pl.multiple_of(kvp * tok, tok))]

        @pl.when(s < steps)
        def _():
            for d in range(2):
                remote(ring.at[d, s - 1, kvp], ring.at[d, s, kvp], rs.at[d, s, kvp], rr.at[d, s, kvp], up if d == 0 else down).start()

    l_own.wait()
    for kvp in range(2):
        for d in range(2):
            send(d, 0, kvp).start()

    def out_copies(buf, dst, i, width, lsem, ssem, rsem):
        cols = pl.ds(pl.multiple_of(col0 + i * width, width), width)
        bc = pl.ds(pl.multiple_of(i * width, width), width)
        for pc in range(2):
            pltpu.make_async_copy(buf.at[pl.ds(mine[pc], half), bc], dst.at[pl.ds(half * pc, half), cols], lsem).start()
            remote(buf.at[pl.ds(theirs[pc], half), bc], dst.at[pl.ds(half * pc, half), cols], ssem, rsem, partner).start()

    l_o.wait()
    r_o.wait_recv()
    ns = wob.shape[0]

    @pl.loop(0, n_y)
    def _(i):
        slot = lax.rem(i, ns)
        wo_copy(i, slot).wait()
        yb[:, pl.ds(pl.multiple_of(i * bw, bw), bw)] = dot(ob[...], wob[slot]).astype(BF16)

        @pl.when(i + ns < n_y)
        def _():
            wo_copy(i + ns, slot).start()

        @pl.when(i > 0)
        def _():
            out_copies(yb, y, i - 1, bw, ysem, ys, yr)

        @pl.when((i >= 3) & (lax.rem(i, 2) == 1))
        def _():
            event((i - 3) // 2)

    out_copies(yb, y, n_y - 1, bw, ysem, ys, yr)

    l_dq.wait()
    r_dq.wait_recv()
    nq = wqb.shape[0]
    quarters = 2
    qs = qd // quarters
    order[...] = sort_matrix()

    def split_part(slot, dst, k):
        split_heads(order[...], wqb.at[slot, k * qs:(k + 1) * qs], dst.at[k * qs:(k + 1) * qs], qs, n_head, head)

    wq_copy(0, 0).wait()
    for k in range(quarters):
        split_part(0, wr.at[0], k)
    wq_copy(nq, 0).start()

    def x_step(i, cur, nxt):
        slot = lax.rem(i + 1, nq)

        @pl.when(i + 1 < n_x)
        def _():
            wq_copy(i + 1, slot).wait()

        dacc[:, pl.ds(pl.multiple_of(i * qd, qd), qd)] = dot(dqb[...], cur[...], NT)
        for k in range(quarters):
            split_part(slot, nxt, k)

        @pl.when(i + 1 + nq < n_x)
        def _():
            wq_copy(i + 1 + nq, slot).start()

    @pl.loop(0, n_x // 2)
    def _(h):
        x_step(2 * h, wr.at[0], wr.at[1])
        event(3 + 2 * h)
        x_step(2 * h + 1, wr.at[1], wr.at[0])
        event(4 + 2 * h)

    for c in wk_copies:
        c.wait()
    n_e = 2 * steps
    first_e = 3 + n_x

    @pl.loop(first_e, n_e)
    def _(e):
        @pl.when(e < first_e + 2)
        def _():
            j = e - first_e
            rows_b = d_half // 2
            piece = kc // 2
            for k in range(2):
                for m in range(rows_b // piece):
                    r0 = pl.multiple_of(j * rows_b + m * piece, piece)
                    scr[k * kc:(k + 1) * kc, :] = wkb[k, pl.ds(2 * r0, kc), :].astype(F32)
                    for h in range(2):
                        b2[pl.ds(r0, piece), (2 * k + h) * head:(2 * k + h + 1) * head] = scr[pl.ds(k * kc + h, piece, stride=2), :].astype(BF16)

        event(e)

    for kvp in range(2):
        for d in range(2):
            fin[d * tok:(d + 1) * tok, kvp * head:(kvp + 1) * head] = ring[d, steps - 1, kvp].astype(BF16)

    r_fin = remote(fin, a2.at[core], fs, fr, partner)
    r_fin.start()
    a2[core] = fin[...]
    r_fin.wait_recv()
    a_all = jnp.concatenate([a2[0][:, :head], a2[1][:, :head], a2[0][:, head:], a2[1][:, head:]], axis=1)
    for i in range(n_y):
        cs = slice(i * bw, (i + 1) * bw)
        xo[:, cs] = (dacc[:, cs] + dot(a_all, b2[cs, :], NT)).astype(BF16)
        if i > 0:
            out_copies(xo, dx, i - 1, bw, xsem, xs, xr)
    out_copies(xo, dx, n_y - 1, bw, xsem, xs, xr)

    for c in (r_o, r_dq, r_fin):
        c.wait_send()
    for s in range(steps):
        for kvp in range(2):
            for d in range(2):
                send(d, s, kvp).wait_send()
    for buf, dst, lsem, ssem, rsem in ((yb, y, ysem, ys, yr), (xo, dx, xsem, xs, xr)):
        cols = pl.ds(col0, d_half)
        pltpu.make_async_copy(buf.at[pl.ds(0, tok)], dst.at[:, cols], lsem).wait()
        both = remote(buf.at[pl.ds(0, tok)], dst.at[:, cols], ssem, rsem, partner)
        both.wait_send()
        both.wait_recv()


def solution(mesh):
    group_devs = mesh.shape['cp']
    chips = group_devs // 2
    row_spec = P(('dp', 'cp'))
    full_spec = P()
    any_spec = pl.BlockSpec(memory_space=pl.ANY)
    vmem_spec = pl.BlockSpec(memory_space=pltpu.VMEM)
    dma = pltpu.SemaphoreType.DMA

    def local_layer(x_in, dy_in, doc_id, w_q, w_k, w_v, w_o):
        tok, d_model = x_in.shape
        q_heads, head = w_q.shape[1], w_q.shape[2]
        kv_heads = w_k.shape[1]
        group = q_heads // kv_heads
        half = tok // 2
        rows2 = 2 * tok
        pieces = 2 * chips
        lanes = group * tok
        d_half = d_model // 2
        scale = head ** -0.5
        core = lax.axis_index('cp') % 2
        docs = doc_id.reshape(2, half)
        slot = jnp.stack([core, 1 - core])[:, None]
        lane = jnp.arange(tok)
        docf = jnp.concatenate([docs, docs], axis=1).astype(F32)
        docf = jnp.where((lane // half)[None, :] == slot, docf, 0.0)
        ids = jnp.tile(docf, (1, group))
        counts = jnp.sum((docs[:, :, None] < jnp.arange(head)[None, None, :]).astype(F32), axis=1)
        meta = jnp.concatenate([ids, counts], axis=1).astype(BF16)
        meta = jnp.broadcast_to(meta[:, None, :], (2, 16, lanes + head))

        wq4 = w_q.reshape(d_model, kv_heads, group, head)
        wk2 = w_k.reshape(d_model * kv_heads, head)
        wv2 = w_v.reshape(d_model * kv_heads, head)
        wo2 = w_o.reshape(q_heads * head, d_model)

        n_ch = 4
        cw = d_model // n_ch
        qd = d_model // 8
        hops = chips // 2
        kv_rows = 2 * tok + 16
        q, do, kv, md = pl.pallas_call(
            functools.partial(proj_kernel, chips),
            name='proj',
            out_shape=(jax.ShapeDtypeStruct((2, lanes, head), BF16), jax.ShapeDtypeStruct((2, lanes, head), BF16),
                       jax.ShapeDtypeStruct((pieces, kv_rows, head), BF16), jax.ShapeDtypeStruct((2, 16, lanes), BF16)),
            in_specs=[any_spec] * 7,
            out_specs=(vmem_spec, vmem_spec, any_spec, vmem_spec),
            scratch_shapes=[
                pltpu.VMEM((rows2, d_model), BF16), pltpu.VMEM((rows2, d_model), BF16), pltpu.VMEM((2, 2, 16, lanes + head), BF16),
                pltpu.VMEM((pieces, kv_rows, head), BF16),
                pltpu.VMEM((2 * d_model, head), BF16), pltpu.VMEM((2 * d_model, head), BF16),
                pltpu.VMEM((3, qd, group, head), BF16), pltpu.VMEM((2, 4 * head, d_model // 2), BF16),
                pltpu.VMEM((2, qd, group * head), BF16), pltpu.VMEM((TILE, TILE), BF16), pltpu.VMEM((TILE, TILE), BF16), pltpu.VMEM((cw, 4 * head), BF16),
                pltpu.VMEM((rows2, group * head), F32), pltpu.VMEM((tok, 4 * head), F32), pltpu.VMEM((3, tok, 2 * head), BF16),
                dma((2, 2, n_ch)), dma((2, n_ch)), dma((3,)), dma((2,)),
                dma((2, n_ch)), dma((2, n_ch)), dma((2, n_ch)), dma((2, n_ch)), dma, dma, dma, dma,
                dma((2, hops, 2)), dma((2, hops, 2)), dma((1,)),
            ],
            compiler_params=pltpu.CompilerParams(collective_id=0, has_side_effects=True, vmem_limit_bytes=60 << 20),
        )(x_in, dy_in, meta, wq4, wk2, wv2, wo2)

        o, dq, dkv = pl.pallas_call(
            functools.partial(attn_kernel, chips, scale),
            name='attn',
            out_shape=(jax.ShapeDtypeStruct((rows2, group * head), BF16), jax.ShapeDtypeStruct((rows2, group * head), BF16),
                       jax.ShapeDtypeStruct((pieces, 2 * tok, head), F32)),
            in_specs=[vmem_spec] * 4,
            out_specs=(vmem_spec,) * 3,
            scratch_shapes=[
                pltpu.VMEM((chips, rows2, lanes), F32), pltpu.VMEM((chips, rows2, lanes), BF16), pltpu.VMEM((head, lanes), F32),
                pltpu.VMEM((lanes, head), BF16), pltpu.VMEM((1, lanes), F32), pltpu.VMEM((1, lanes), F32),
            ],
            compiler_params=pltpu.CompilerParams(vmem_limit_bytes=60 << 20),
        )(q, do, kv, md)

        steps = chips - 1
        bw = d_half // 8
        y, dx = pl.pallas_call(
            functools.partial(out_kernel, chips),
            name='out',
            out_shape=(jax.ShapeDtypeStruct((tok, d_model), BF16), jax.ShapeDtypeStruct((tok, d_model), BF16)),
            in_specs=[any_spec] * 7,
            out_specs=(any_spec, any_spec),
            scratch_shapes=[
                pltpu.VMEM((rows2, q_heads * head), BF16), pltpu.VMEM((rows2, q_heads * head), BF16),
                pltpu.VMEM((pieces, 2 * tok, head), F32), pltpu.VMEM((2, steps, 2, tok, head), F32),
                pltpu.VMEM((rows2, 2 * head), BF16), pltpu.VMEM((2, rows2, 2 * head), BF16), pltpu.VMEM((d_half, 4 * head), BF16),
                pltpu.VMEM((3, q_heads * head, bw), BF16), pltpu.VMEM((3, bw, q_heads, head), BF16),
                pltpu.VMEM((2, 2 * d_half, head), BF16),
                pltpu.VMEM((1024, head), F32), pltpu.VMEM((2, bw, q_heads * head), BF16), pltpu.VMEM((TILE, TILE), BF16),
                pltpu.VMEM((rows2, d_half), F32), pltpu.VMEM((rows2, d_half), BF16), pltpu.VMEM((rows2, d_half), BF16),
                dma((3,)), dma((2,)), dma((2,)), dma((2, steps, 2)), dma((2, steps, 2)), dma, dma,
                dma((3,)), dma((3,)), dma((2,)), dma, dma, dma, dma, dma, dma,
            ],
            compiler_params=pltpu.CompilerParams(collective_id=1, has_side_effects=True, vmem_limit_bytes=62 << 20),
        )(o, dq, dkv, wo2, w_q, wk2, wv2)
        return y, dx

    return jax.shard_map(local_layer, mesh=mesh,
                         in_specs=(row_spec, row_spec, row_spec, full_spec, full_spec, full_spec, full_spec),
                         out_specs=(row_spec, row_spec), check_vma=False)
```

```python
import functools

import jax
import jax.numpy as jnp
from jax import lax
from jax.experimental import pallas as pl
from jax.experimental.pallas import tpu as pltpu
from jax.sharding import PartitionSpec as P

MESH = pl.DeviceIdType.MESH
NEG_BIG = -1.0e30
LOG2E = 1.4426950408889634
F32, BF16 = jnp.float32, jnp.bfloat16
NT = (((1,), (1,)), ((), ()))
NN = (((1,), (0,)), ((), ()))
DOC_VALUES = 9


def dot(a, b, dims=NN):
    return lax.dot_general(a, b, dims, preferred_element_type=F32)


def remote(src, dst, send, recv, dev):
    return pltpu.make_async_remote_copy(src_ref=src, dst_ref=dst, send_sem=send, recv_sem=recv,
                                        device_id={'cp': dev}, device_id_type=MESH)


def ring_ids(chips):
    me = lax.axis_index('cp')
    core, chip = lax.rem(me, 2), me // 2
    return core, chip, chip * 2 + 1 - core, lax.rem(chip + 1, chips) * 2 + core, lax.rem(chip + chips - 1, chips) * 2 + core


def entry_barrier(devs):
    barrier = pltpu.get_barrier_semaphore()
    for dev in devs:
        pl.semaphore_signal(barrier, inc=1, device_id={'cp': dev}, device_id_type=MESH)
    pl.semaphore_wait(barrier, len(devs))


TILE = 256
PER = 8


def sort_matrix():
    toks = TILE // PER
    r = lax.broadcasted_iota(jnp.int32, (TILE, TILE), 0)
    c = lax.broadcasted_iota(jnp.int32, (TILE, TILE), 1)
    t = r & (toks - 1)
    return jnp.where(c == t * PER + lax.shift_right_logical(r, toks.bit_length() - 1), 1.0, 0.0).astype(BF16)


def split_heads(order, src, dst, count, n_head, head):
    toks = TILE // PER
    for h0 in range(0, n_head, PER):
        for t0 in range(0, count, 4 * toks):
            side = [src[t0 + k * toks:t0 + (k + 1) * toks, h0:h0 + PER, :].reshape(TILE, head) for k in range(4)]
            rows = dot(order, jnp.concatenate(side, axis=1)).astype(BF16)
            for k in range(4):
                for g in range(PER):
                    dst[t0 + k * toks:t0 + (k + 1) * toks, (h0 + g) * head:(h0 + g + 1) * head] = rows[g * toks:(g + 1) * toks, k * head:(k + 1) * head]


def proj_kernel(chips, x, dy, meta, wq, wk, wv, wo, q_o, do_o, kv_o, md_o,
                xb, dyb, mb, kvb, wkb, wvb, wqb, wob, wr, order, pick, wkv, acc, kvacc, kvx,
                loc, wksem, wqsem, wosem, xs, xr, ys, yr, ms, mr, ks, kr, gs, gr, osem):
    half = x.shape[0] // 2
    d_model = x.shape[1]
    tok = 2 * half
    pieces = 2 * chips
    n_ch = xs.shape[1]
    cw = d_model // n_ch
    core, chip, partner, up, down = ring_ids(chips)
    row_off = (pl.multiple_of(half * core, half), pl.multiple_of(3 * half - half * core, half))
    n_q, qd = d_model // wqb.shape[1], wqb.shape[1]
    group = wqb.shape[2]
    head = wqb.shape[3]
    n_o = group * head // wob.shape[1]

    def wq_copy(i, slot):
        return pltpu.make_async_copy(wq.at[pl.ds(i * qd, qd), core], wqb.at[slot], wqsem.at[slot])

    def wo_copy(i, slot):
        rows, kw = wob.shape[1], wob.shape[2]
        n, k = i // (d_model // kw), i % (d_model // kw)
        return pltpu.make_async_copy(wo.at[pl.ds(core * group * head + n * rows, rows), pl.ds(k * kw, kw)], wob.at[slot], wosem.at[slot])

    wk_copies = []
    for ch in range(n_ch):
        rows = pl.ds(ch * 2 * cw, 2 * cw)
        wk_copies.append((pltpu.make_async_copy(wk.at[rows], wkb.at[rows], wksem.at[0, ch]),
                          pltpu.make_async_copy(wv.at[rows], wvb.at[rows], wksem.at[1, ch])))
    x_loc, y_loc, x_rem, y_rem = [], [], [], []
    for ch in range(n_ch):
        cols = pl.ds(ch * cw, cw)
        for pc in range(2):
            src = pl.ds(half * pc, half)
            dst = pl.ds(row_off[pc], half)
            x_loc.append(pltpu.make_async_copy(x.at[src, cols], xb.at[dst, cols], loc.at[0, pc, ch]))
            y_loc.append(pltpu.make_async_copy(dy.at[src, cols], dyb.at[dst, cols], loc.at[1, pc, ch]))
            x_rem.append(remote(x.at[src, cols], xb.at[dst, cols], xs.at[pc, ch], xr.at[pc, ch], partner))
            y_rem.append(remote(dy.at[src, cols], dyb.at[dst, cols], ys.at[pc, ch], yr.at[pc, ch], partner))
    m_loc = pltpu.make_async_copy(meta, mb.at[0], osem.at[0])
    m_rem = remote(meta, mb.at[1], ms, mr, partner)

    for ch in range(n_ch):
        x_loc[2 * ch].start()
        x_loc[2 * ch + 1].start()
        wk_copies[ch][0].start()
        wk_copies[ch][1].start()
    m_loc.start()
    for s in range(wqb.shape[0]):
        wq_copy(s, s).start()
    entry_barrier((partner, up, down))
    m_rem.start()
    for c in x_rem[:n_ch]:
        c.start()

    n_sub = TILE // 2
    r = lax.broadcasted_iota(jnp.int32, pick.shape, 0)
    t = r & (n_sub - 1)
    pick[...] = jnp.where(lax.broadcasted_iota(jnp.int32, pick.shape, 1) == 2 * t + jnp.where(r >= n_sub, 1, 0), 1.0, 0.0).astype(BF16)
    order[...] = sort_matrix()
    for ch in range(n_ch):
        for c in wk_copies[ch]:
            c.wait()
        for j in range(cw // n_sub):
            src = slice((ch * cw + j * n_sub) * 2, (ch * cw + (j + 1) * n_sub) * 2)
            rows = dot(pick[...], jnp.concatenate([wkb[src, :], wvb[src, :]], axis=1)).astype(BF16)
            for h in range(2):
                wkv[j * n_sub:(j + 1) * n_sub, h * 2 * head:(h + 1) * 2 * head] = rows[h * n_sub:(h + 1) * n_sub]
        for c in (x_loc[2 * ch], x_loc[2 * ch + 1]):
            c.wait()
        part_sum = dot(jnp.concatenate([xb[pl.ds(row_off[pc], half), ch * cw:(ch + 1) * cw] for pc in range(2)], axis=0), wkv[...])
        if ch == 0:
            kvacc[...] = part_sum
        else:
            kvacc[...] += part_sum
    both_heads = [kvacc[:, h * 2 * head:(h + 1) * 2 * head] for h in range(2)]
    kvx[0] = jnp.where(core == 0, both_heads[1], both_heads[0]).astype(BF16)
    kvx[1] = jnp.where(core == 0, both_heads[0], both_heads[1]).astype(BF16)
    k_rem = remote(kvx.at[0], kvx.at[2], ks, kr, partner)
    k_rem.start()
    for c in x_rem[n_ch:]:
        c.start()
    quarters = 2
    qs = qd // quarters

    def split_part(slot, dst, k):
        split_heads(order[...], wqb.at[slot, k * qs:(k + 1) * qs], dst.at[k * qs:(k + 1) * qs], qs, group, head)

    wq_copy(0, 0).wait()
    for k in range(quarters):
        split_part(0, wr.at[0], k)
    wq_copy(wqb.shape[0], 0).start()

    m_loc.wait()
    m_rem.wait_recv()
    lo, hi = chip, pieces - 1 - chip
    width = md_o.shape[2]
    own_off = (pl.multiple_of(half * core, half), pl.multiple_of(half - half * core, half))
    for pc, idx in ((0, lo), (1, hi)):
        both = (mb[0, pc].astype(F32) + mb[1, pc].astype(F32)).astype(BF16)
        md_o[pc] = both[:, :width]
        kvb[idx, 2 * tok:2 * tok + 16] = both[:, width:]
        for k in range(2):
            kvb[idx, pl.ds(k * tok + own_off[pc], half)] = kvx[1, pc * half:(pc + 1) * half, k * head:(k + 1) * head]
    k_rem.wait_recv()
    for pc, idx in ((0, lo), (1, hi)):
        for k in range(2):
            kvb[idx, pl.ds(k * tok + own_off[1 - pc], half)] = kvx[2, pc * half:(pc + 1) * half, k * head:(k + 1) * head]

    last = chips // 2 - 1

    def hop(direction, t, pc):
        src = lax.rem(chip + (chips - t if direction == 0 else t), chips)
        idx = src if pc == 0 else pieces - 1 - src
        return remote(kvb.at[idx], kvb.at[idx], gs.at[direction, t, pc], gr.at[direction, t, pc], up if direction == 0 else down)

    def arrived(direction, t, pc):
        src = lax.rem(chip + (chips - t - 1 if direction == 0 else t + 1), chips)
        idx = src if pc == 0 else pieces - 1 - src
        remote(kvb.at[idx], kvb.at[idx], gs.at[direction, t, pc], gr.at[direction, t, pc], up).wait_recv()

    moves = [[(d, pc) for pc in range(2) for d in range(2) if t < last or d == pc] for t in range(last + 1)]

    def advance(t, only=None):
        for d, pc in moves[t - 1]:
            if only is None or pc == only:
                arrived(d, t - 1, pc)
                if t <= last and (d, pc) in moves[t]:
                    hop(d, t, pc).start()

    for d, pc in moves[0]:
        hop(d, 0, pc).start()

    for c in y_rem:
        c.start()
    for c in y_loc:
        c.start()
    for k in range(wob.shape[0]):
        wo_copy(k, k).start()

    acc[...] = jnp.zeros_like(acc)
    n_slot = wqb.shape[0]
    nw = group * head // quarters

    def q_step(i, cur, nxt):
        slot = lax.rem(i + 1, n_slot)

        @pl.when(i + 1 < n_q)
        def _():
            wq_copy(i + 1, slot).wait()

        lhs = xb.at[:, pl.ds(pl.multiple_of(i * qd, qd), qd)]
        for k in range(quarters):
            cols = slice(k * nw, (k + 1) * nw)
            acc[:, cols] += dot(lhs[...], cur[:, cols])
            split_part(slot, nxt, k)

        @pl.when(i + 1 + n_slot < n_q)
        def _():
            wq_copy(i + 1 + n_slot, slot).start()

    plan = {1: (1, 0), 3: (1, 1), 4: (2, 0), 6: (2, 1), 7: (3, 0)}

    @pl.loop(0, n_q // 2)
    def _(h):
        cols = pl.ds(pl.multiple_of(h * 2 * qd, 2 * qd), 2 * qd)
        for pc in range(2):
            rows = xb.at[pl.ds(row_off[pc], half), cols]
            remote(rows, rows, xs.at[pc, h], xr.at[pc, h], partner).wait_recv()
        for k in range(2):
            q_step(2 * h + k, wr.at[k], wr.at[1 - k])
            for at, step in plan.items():
                if at % 2 == k:
                    @pl.when(h == at // 2)
                    def _():
                        advance(*step)

    for g in range(group):
        for pc in range(2):
            q_o[pc, g * tok:(g + 1) * tok, :] = acc[pc * tok:(pc + 1) * tok, g * head:(g + 1) * head].astype(BF16)

    for c in y_loc:
        c.wait()
    for c in y_rem:
        c.wait_recv()

    wide = wob.shape[1] // head
    kw = wob.shape[2]
    n_k = d_model // kw
    for u in range(n_o * n_k):
        n, k = u // n_k, u % n_k
        slot = u % wob.shape[0]
        wo_copy(u, slot).wait()
        part = dot(dyb[:, k * kw:(k + 1) * kw], wob[slot], NT)
        if k == 0:
            acc[:, 0:wide * head] = part
        else:
            acc[:, 0:wide * head] += part
        if u + wob.shape[0] < n_o * n_k:
            wo_copy(u + wob.shape[0], slot).start()
        if k == n_k - 1:
            for g in range(wide):
                for pc in range(2):
                    do_o[pc, (n * wide + g) * tok:(n * wide + g + 1) * tok, :] = acc[pc * tok:(pc + 1) * tok, g * head:(g + 1) * head].astype(BF16)
        if u == 0:
            advance(3, 1)
    for t in range(4, last + 2):
        advance(t)
    out = pltpu.make_async_copy(kvb, kv_o, osem.at[0])
    out.start()
    for c in x_rem + y_rem + [m_rem, k_rem]:
        c.wait_send()
    for t in range(last + 1):
        for d, pc in moves[t]:
            hop(d, t, pc).wait_send()
    out.wait()


def attn_kernel(chips, scale, q, do, kv, md, o_ref, dq_ref, dkv, s_scr, p_scr, acc_t, row_scr, m_ref, l_ref):
    pieces = 2 * chips
    tok = kv.shape[1] // 2 - 8
    head = kv.shape[2]
    lanes_all = q.shape[1]
    group = lanes_all // tok
    lw = 256
    lanes = [slice(a, a + lw) for a in range(0, lanes_all, lw)]
    chip = lax.axis_index('cp') // 2
    dkv[...] = jnp.zeros_like(dkv)
    lane = lax.broadcasted_iota(jnp.int32, (1, lanes_all), 1)
    for g in range(1, group):
        lane = jnp.where(lane >= tok, lane - tok, lane)
    q_off = lane.astype(F32)
    tot = lax.fori_loop(0, pieces, lambda j, a: a + kv[j, 2 * tok:2 * tok + 16].astype(F32), jnp.zeros((16, head), F32))[0:1]

    @pl.loop(0, 2)
    def _(pc):
        place = jnp.where(pc == 0, chip, pieces - 1 - chip)
        doc_q = md[pc].astype(F32)[0:1]
        start = jnp.zeros((1, lanes_all), F32)
        for v in range(1, DOC_VALUES):
            start = jnp.where(doc_q == float(v), tot[:, v:v + 1], start)
        first = jnp.min(start).astype(jnp.int32) // tok
        pos = q_off + (place * tok).astype(F32)
        n_pair = (place - first + 2) // 2
        m_ref[...] = jnp.full_like(m_ref, NEG_BIG)
        l_ref[...] = jnp.zeros_like(l_ref)

        def rows_of(t, base):
            kb = place - 2 * t
            return jnp.concatenate([kv[jnp.maximum(kb - 1, 0), base:base + tok], kv[kb, base:base + tok]], axis=0)

        def add_rows(t, base, val):
            kb = place - 2 * t
            dkv[kb, base:base + tok] += val[tok:]
            dkv[jnp.maximum(kb - 1, 0), base:base + tok] += val[:tok]

        def score(t, masked):
            keys = rows_of(t, 0)
            u = (lax.broadcasted_iota(jnp.int32, (2 * tok, lw), 0) + (place - 2 * t - 1) * tok).astype(F32)
            scales = []
            for ln in lanes:
                s = dot(keys, q[pc, ln], NT) * (scale * LOG2E)
                if masked:
                    s = jnp.where((u >= start[:, ln]) & (u <= pos[:, ln]), s, NEG_BIG)
                s_scr[t, :, ln] = s
                m_old = m_ref[:, ln]
                m_new = jnp.maximum(m_old, jnp.max(s, axis=0, keepdims=True))
                m_ref[:, ln] = m_new
                scales.append((m_new, jnp.exp2(m_old - m_new)))
            for ln, (m_new, shrink) in zip(lanes, scales):
                l_ref[:, ln] = l_ref[:, ln] * shrink + jnp.sum(jnp.exp2(s_scr[t, :, ln] - m_new), axis=0, keepdims=True)

        last_start = (jnp.max(start).astype(jnp.int32) + tok - 1) // tok
        n_full = jnp.maximum((place - last_start - 1) // 2, 0)

        @pl.loop(0, n_pair)
        def _(t):
            inside = (t >= 1) & (t <= n_full)

            @pl.when(inside)
            def _():
                score(t, False)

            @pl.when(jnp.logical_not(inside))
            def _():
                score(t, True)

        log_norm = m_ref[...] + jnp.log2(l_ref[...])
        acc_t[...] = jnp.zeros_like(acc_t)

        @pl.loop(0, n_pair)
        def _(t):
            v_t = rows_of(t, tok).astype(F32).T.astype(BF16)
            dv = jnp.zeros((2 * tok, head), F32)
            for ln in lanes:
                p = jnp.exp2(s_scr[t, :, ln] - log_norm[:, ln]).astype(BF16)
                p_scr[t, :, ln] = p
                acc_t[:, ln] += dot(v_t, p)
                dv = dv + dot(p, do[pc, ln])
            add_rows(t, tok, dv)

        for ln in lanes:
            o_bf = acc_t[:, ln].astype(BF16).astype(F32)
            do_t = do[pc, ln].astype(F32).T
            l_ref[:, ln] = jnp.sum(do_t * o_bf, axis=0, keepdims=True)
            row_scr[ln, :] = o_bf.T.astype(BF16)
        out_rows = pl.ds(pl.multiple_of(pc * tok, tok), tok)
        for g in range(group):
            o_ref[out_rows, g * head:(g + 1) * head] = row_scr[g * tok:(g + 1) * tok, :]
        acc_t[...] = jnp.zeros_like(acc_t)

        @pl.loop(0, n_pair)
        def _(t):
            vals = rows_of(t, tok)
            k_t = rows_of(t, 0).astype(F32).T.astype(BF16)
            dk = jnp.zeros((2 * tok, head), F32)
            nxt = dot(vals, do[pc, lanes[0]], NT)
            for i, ln in enumerate(lanes):
                dp = nxt
                if i + 1 < len(lanes):
                    nxt = dot(vals, do[pc, lanes[i + 1]], NT)
                ds = (p_scr[t, :, ln].astype(F32) * (dp - l_ref[:, ln])).astype(BF16)
                acc_t[:, ln] += dot(k_t, ds)
                dk = dk + dot(ds, q[pc, ln])
            add_rows(t, 0, dk * scale)

        for ln in lanes:
            row_scr[ln, :] = (acc_t[:, ln] * scale).T.astype(BF16)
        for g in range(group):
            dq_ref[out_rows, g * head:(g + 1) * head] = row_scr[g * tok:(g + 1) * tok, :]


def out_kernel(chips, o, dq, dkv, wo, wq, wk, wv, y, dx,
               ob, dqb, own, ring, fin, a2, b2, wob, wqb, wkb, scr, wr, order, dacc, yb, xo,
               loc, ex_s, ex_r, rs, rr, fs, fr, wosem, wqsem, wksem, ysem, xsem, ys, yr, xs, xr):
    tok = own.shape[1] // 2
    head = own.shape[2]
    half = tok // 2
    pieces = 2 * chips
    d_half = yb.shape[1]
    core, chip, partner, up, down = ring_ids(chips)
    mine = (pl.multiple_of(half * core, half), pl.multiple_of(3 * half - half * core, half))
    theirs = (pl.multiple_of(half - half * core, half), pl.multiple_of(2 * half + half * core, half))
    hw = o.shape[1]
    col0 = pl.multiple_of(core * d_half, d_half)
    bw = wob.shape[2]
    n_y = d_half // bw
    qd = wqb.shape[1]
    n_x = d_half // qd
    n_head = wqb.shape[2]
    kc = scr.shape[0] // 2

    def wo_copy(i, slot):
        return pltpu.make_async_copy(wo.at[:, pl.ds(pl.multiple_of(col0 + i * bw, bw), bw)], wob.at[slot], wosem.at[slot])

    def wq_copy(i, slot):
        rows = wqb.shape[1]
        return pltpu.make_async_copy(wq.at[pl.ds(pl.multiple_of(col0 + i * rows, rows), rows)], wqb.at[slot], wqsem.at[slot])

    rows = pl.ds(pl.multiple_of(col0 * 2, 2 * d_half), 2 * d_half)
    wk_copies = [pltpu.make_async_copy(w.at[rows], wkb.at[k], wksem.at[k]) for k, w in enumerate((wk, wv))]
    ocols = pl.ds(pl.multiple_of(core * hw, hw), hw)
    l_own = pltpu.make_async_copy(dkv, own, loc.at[0])
    l_o = pltpu.make_async_copy(o, ob.at[:, ocols], loc.at[1])
    l_dq = pltpu.make_async_copy(dq, dqb.at[:, ocols], loc.at[2])
    r_o = remote(o, ob.at[:, ocols], ex_s.at[0], ex_r.at[0], partner)
    r_dq = remote(dq, dqb.at[:, ocols], ex_s.at[1], ex_r.at[1], partner)

    l_own.start()
    l_o.start()
    l_dq.start()
    for s in range(wob.shape[0]):
        wo_copy(s, s).start()
    entry_barrier((partner, up, down))
    r_o.start()
    r_dq.start()
    for s in range(wqb.shape[0]):
        wq_copy(s, s).start()
    for c in wk_copies:
        c.start()

    steps = chips - 1

    def owner(direction, s):
        chip_w = lax.rem(chip + (2 * chips - 1 - s if direction == 0 else 1 + s), chips)
        return chip_w if direction == 0 else pieces - 1 - chip_w

    def part_rows(row):
        return pl.ds(row, tok)

    def send(direction, s, kvp):
        src = own.at[owner(direction, 0), part_rows(kvp * tok)] if s == 0 else ring.at[direction, s - 1, kvp]
        return remote(src, ring.at[direction, s, kvp], rs.at[direction, s, kvp], rr.at[direction, s, kvp], up if direction == 0 else down)

    def event(e):
        s, kvp = e // 2 + 1, e % 2 if isinstance(e, int) else lax.rem(e, 2)
        for d in range(2):
            remote(ring.at[d, s - 1, kvp], ring.at[d, s - 1, kvp], rs.at[d, s - 1, kvp], rr.at[d, s - 1, kvp], up).wait_recv()
            ring[d, s - 1, kvp] = ring[d, s - 1, kvp] + own[owner(d, s), part_rows(kvp * tok if isinstance(e, int) else pl.multiple_of(kvp * tok, tok))]

        @pl.when(s < steps)
        def _():
            for d in range(2):
                remote(ring.at[d, s - 1, kvp], ring.at[d, s, kvp], rs.at[d, s, kvp], rr.at[d, s, kvp], up if d == 0 else down).start()

    l_own.wait()
    for kvp in range(2):
        for d in range(2):
            send(d, 0, kvp).start()

    def out_copies(buf, dst, i, width, lsem, ssem, rsem):
        cols = pl.ds(pl.multiple_of(col0 + i * width, width), width)
        bc = pl.ds(pl.multiple_of(i * width, width), width)
        for pc in range(2):
            pltpu.make_async_copy(buf.at[pl.ds(mine[pc], half), bc], dst.at[pl.ds(half * pc, half), cols], lsem).start()
            remote(buf.at[pl.ds(theirs[pc], half), bc], dst.at[pl.ds(half * pc, half), cols], ssem, rsem, partner).start()

    nq = wqb.shape[0]
    quarters = 2
    qs = qd // quarters
    order[...] = sort_matrix()

    def split_part(slot, dst, k):
        split_heads(order[...], wqb.at[slot, k * qs:(k + 1) * qs], dst.at[k * qs:(k + 1) * qs], qs, n_head, head)

    wq_copy(0, 0).wait()
    for k in range(quarters):
        split_part(0, wr.at[0], k)
    wq_copy(nq, 0).start()

    l_o.wait()
    r_o.wait_recv()
    event(0)
    ns = wob.shape[0]

    @pl.loop(0, n_y)
    def _(i):
        slot = lax.rem(i, ns)
        wo_copy(i, slot).wait()
        yb[:, pl.ds(pl.multiple_of(i * bw, bw), bw)] = dot(ob[...], wob[slot]).astype(BF16)

        @pl.when(i + ns < n_y)
        def _():
            wo_copy(i + ns, slot).start()

        @pl.when(i > 0)
        def _():
            out_copies(yb, y, i - 1, bw, ysem, ys, yr)

        @pl.when(lax.rem(i, 2) == 1)
        def _():
            event((i + 1) // 2)

    out_copies(yb, y, n_y - 1, bw, ysem, ys, yr)

    l_dq.wait()
    r_dq.wait_recv()
    def x_step(i, cur, nxt):
        slot = lax.rem(i + 1, nq)

        @pl.when(i + 1 < n_x)
        def _():
            wq_copy(i + 1, slot).wait()

        dacc[:, pl.ds(pl.multiple_of(i * qd, qd), qd)] = dot(dqb[...], cur[...], NT)
        for k in range(quarters):
            split_part(slot, nxt, k)

        @pl.when(i + 1 + nq < n_x)
        def _():
            wq_copy(i + 1 + nq, slot).start()

    @pl.loop(0, n_x // 2)
    def _(h):
        x_step(2 * h, wr.at[0], wr.at[1])
        event(5 + 2 * h)
        x_step(2 * h + 1, wr.at[1], wr.at[0])
        event(6 + 2 * h)

    for c in wk_copies:
        c.wait()
    n_e = 2 * steps

    @pl.loop(0, 2)
    def _(j):
        rows_b = d_half // 2
        piece = kc // 2
        for k in range(2):
            for m in range(rows_b // piece):
                r0 = pl.multiple_of(j * rows_b + m * piece, piece)
                scr[k * kc:(k + 1) * kc, :] = wkb[k, pl.ds(2 * r0, kc), :].astype(F32)
                for h in range(2):
                    b2[pl.ds(r0, piece), (2 * k + h) * head:(2 * k + h + 1) * head] = scr[pl.ds(k * kc + h, piece, stride=2), :].astype(BF16)

    for e in range(5 + n_x, n_e):
        event(e)

    for kvp in range(2):
        for d in range(2):
            fin[d * tok:(d + 1) * tok, kvp * head:(kvp + 1) * head] = ring[d, steps - 1, kvp].astype(BF16)

    r_fin = remote(fin, a2.at[core], fs, fr, partner)
    r_fin.start()
    a2[core] = fin[...]
    r_fin.wait_recv()
    a_all = jnp.concatenate([a2[0][:, :head], a2[1][:, :head], a2[0][:, head:], a2[1][:, head:]], axis=1)
    for i in range(n_y):
        cs = slice(i * bw, (i + 1) * bw)
        xo[:, cs] = (dacc[:, cs] + dot(a_all, b2[cs, :], NT)).astype(BF16)
        if i > 0:
            out_copies(xo, dx, i - 1, bw, xsem, xs, xr)
    out_copies(xo, dx, n_y - 1, bw, xsem, xs, xr)

    for c in (r_o, r_dq, r_fin):
        c.wait_send()
    for s in range(steps):
        for kvp in range(2):
            for d in range(2):
                send(d, s, kvp).wait_send()
    for buf, dst, lsem, ssem, rsem in ((yb, y, ysem, ys, yr), (xo, dx, xsem, xs, xr)):
        cols = pl.ds(col0, d_half)
        pltpu.make_async_copy(buf.at[pl.ds(0, tok)], dst.at[:, cols], lsem).wait()
        both = remote(buf.at[pl.ds(0, tok)], dst.at[:, cols], ssem, rsem, partner)
        both.wait_send()
        both.wait_recv()


def solution(mesh):
    group_devs = mesh.shape['cp']
    chips = group_devs // 2
    row_spec = P(('dp', 'cp'))
    full_spec = P()
    any_spec = pl.BlockSpec(memory_space=pl.ANY)
    vmem_spec = pl.BlockSpec(memory_space=pltpu.VMEM)
    dma = pltpu.SemaphoreType.DMA

    def local_layer(x_in, dy_in, doc_id, w_q, w_k, w_v, w_o):
        tok, d_model = x_in.shape
        q_heads, head = w_q.shape[1], w_q.shape[2]
        kv_heads = w_k.shape[1]
        group = q_heads // kv_heads
        half = tok // 2
        rows2 = 2 * tok
        pieces = 2 * chips
        lanes = group * tok
        d_half = d_model // 2
        scale = head ** -0.5
        core = lax.axis_index('cp') % 2
        docs = doc_id.reshape(2, half)
        slot = jnp.stack([core, 1 - core])[:, None]
        lane = jnp.arange(tok)
        docf = jnp.concatenate([docs, docs], axis=1).astype(F32)
        docf = jnp.where((lane // half)[None, :] == slot, docf, 0.0)
        ids = jnp.tile(docf, (1, group))
        counts = jnp.sum((docs[:, :, None] < jnp.arange(head)[None, None, :]).astype(F32), axis=1)
        meta = jnp.concatenate([ids, counts], axis=1).astype(BF16)
        meta = jnp.broadcast_to(meta[:, None, :], (2, 16, lanes + head))

        wq4 = w_q.reshape(d_model, kv_heads, group, head)
        wk2 = w_k.reshape(d_model * kv_heads, head)
        wv2 = w_v.reshape(d_model * kv_heads, head)
        wo2 = w_o.reshape(q_heads * head, d_model)

        n_ch = 4
        cw = d_model // n_ch
        qd = d_model // 8
        hops = chips // 2
        kv_rows = 2 * tok + 16
        q, do, kv, md = pl.pallas_call(
            functools.partial(proj_kernel, chips),
            name='proj',
            out_shape=(jax.ShapeDtypeStruct((2, lanes, head), BF16), jax.ShapeDtypeStruct((2, lanes, head), BF16),
                       jax.ShapeDtypeStruct((pieces, kv_rows, head), BF16), jax.ShapeDtypeStruct((2, 16, lanes), BF16)),
            in_specs=[any_spec] * 7,
            out_specs=(vmem_spec, vmem_spec, any_spec, vmem_spec),
            scratch_shapes=[
                pltpu.VMEM((rows2, d_model), BF16), pltpu.VMEM((rows2, d_model), BF16), pltpu.VMEM((2, 2, 16, lanes + head), BF16),
                pltpu.VMEM((pieces, kv_rows, head), BF16),
                pltpu.VMEM((2 * d_model, head), BF16), pltpu.VMEM((2 * d_model, head), BF16),
                pltpu.VMEM((3, qd, group, head), BF16), pltpu.VMEM((2, 4 * head, d_model // 2), BF16),
                pltpu.VMEM((2, qd, group * head), BF16), pltpu.VMEM((TILE, TILE), BF16), pltpu.VMEM((TILE, TILE), BF16), pltpu.VMEM((cw, 4 * head), BF16),
                pltpu.VMEM((rows2, group * head), F32), pltpu.VMEM((tok, 4 * head), F32), pltpu.VMEM((3, tok, 2 * head), BF16),
                dma((2, 2, n_ch)), dma((2, n_ch)), dma((3,)), dma((2,)),
                dma((2, n_ch)), dma((2, n_ch)), dma((2, n_ch)), dma((2, n_ch)), dma, dma, dma, dma,
                dma((2, hops, 2)), dma((2, hops, 2)), dma((1,)),
            ],
            compiler_params=pltpu.CompilerParams(collective_id=0, has_side_effects=True, vmem_limit_bytes=60 << 20),
        )(x_in, dy_in, meta, wq4, wk2, wv2, wo2)

        o, dq, dkv = pl.pallas_call(
            functools.partial(attn_kernel, chips, scale),
            name='attn',
            out_shape=(jax.ShapeDtypeStruct((rows2, group * head), BF16), jax.ShapeDtypeStruct((rows2, group * head), BF16),
                       jax.ShapeDtypeStruct((pieces, 2 * tok, head), F32)),
            in_specs=[vmem_spec] * 4,
            out_specs=(vmem_spec,) * 3,
            scratch_shapes=[
                pltpu.VMEM((chips, rows2, lanes), F32), pltpu.VMEM((chips, rows2, lanes), BF16), pltpu.VMEM((head, lanes), F32),
                pltpu.VMEM((lanes, head), BF16), pltpu.VMEM((1, lanes), F32), pltpu.VMEM((1, lanes), F32),
            ],
            compiler_params=pltpu.CompilerParams(vmem_limit_bytes=60 << 20),
        )(q, do, kv, md)

        steps = chips - 1
        bw = d_half // 8
        y, dx = pl.pallas_call(
            functools.partial(out_kernel, chips),
            name='out',
            out_shape=(jax.ShapeDtypeStruct((tok, d_model), BF16), jax.ShapeDtypeStruct((tok, d_model), BF16)),
            in_specs=[any_spec] * 7,
            out_specs=(any_spec, any_spec),
            scratch_shapes=[
                pltpu.VMEM((rows2, q_heads * head), BF16), pltpu.VMEM((rows2, q_heads * head), BF16),
                pltpu.VMEM((pieces, 2 * tok, head), F32), pltpu.VMEM((2, steps, 2, tok, head), F32),
                pltpu.VMEM((rows2, 2 * head), BF16), pltpu.VMEM((2, rows2, 2 * head), BF16), pltpu.VMEM((d_half, 4 * head), BF16),
                pltpu.VMEM((3, q_heads * head, bw), BF16), pltpu.VMEM((3, bw, q_heads, head), BF16),
                pltpu.VMEM((2, 2 * d_half, head), BF16),
                pltpu.VMEM((1024, head), F32), pltpu.VMEM((2, bw, q_heads * head), BF16), pltpu.VMEM((TILE, TILE), BF16),
                pltpu.VMEM((rows2, d_half), F32), pltpu.VMEM((rows2, d_half), BF16), pltpu.VMEM((rows2, d_half), BF16),
                dma((3,)), dma((2,)), dma((2,)), dma((2, steps, 2)), dma((2, steps, 2)), dma, dma,
                dma((3,)), dma((3,)), dma((2,)), dma, dma, dma, dma, dma, dma,
            ],
            compiler_params=pltpu.CompilerParams(collective_id=1, has_side_effects=True, vmem_limit_bytes=62 << 20),
        )(o, dq, dkv, wo2, w_q, wk2, wv2)
        return y, dx

    return jax.shard_map(local_layer, mesh=mesh,
                         in_specs=(row_spec, row_spec, row_spec, full_spec, full_spec, full_spec, full_spec),
                         out_specs=(row_spec, row_spec), check_vma=False)
```
